32 devices in a mesh: dp: 8 (over z, y), tp: 4 (over x, core).
Axes of the slice: x: 2, y: 2, z: 4, core: 2. Of those that a mesh axis runs over, the one named last changes fastest.
Arguments:
- activations: bfloat16 [16, 256, 768], P('dp', 'tp'), may hold values from -6 to 6
- pair_rep: bfloat16 [16, 256, 256, 256], P('dp', 'tp'), may hold values from -6 to 6
- noise_times: float32 [16], P('dp'), may hold values from 0 to 1
- class_ids: int32 [16], P('dp'), may hold values from 0 to 40
- chain_lengths: int32 [16], P('dp'), may hold values from 64 to 256, as said below
- ada_weight: bfloat16 [256, 4608], replicated, may hold values from -0.375 to 0.375
- class_table: bfloat16 [41, 256], replicated, may hold values from -4 to 4
- pair_weight: bfloat16 [12, 256], replicated, may hold values from -0.375 to 0.375
- attn_in: bfloat16 [4, 768, 768], P(None, None, 'tp'), may hold values from -0.21875 to 0.21875
- attn_out: bfloat16 [768, 768], P('tp'), may hold values from -2.5 to 2.5
- ff_in: bfloat16 [2, 768, 3072], P(None, None, 'tp'), may hold values from -0.21875 to 0.21875
- ff_out: bfloat16 [3072, 768], P('tp'), may hold values from -0.109375 to 0.109375
- cotangent: bfloat16 [16, 256, 768], P('dp', 'tp'), may hold values from -6 to 6
Outputs:
- result: bfloat16 [16, 256, 768], P('dp', 'tp')
- grad_inputs: bfloat16 [16, 256, 768], P('dp', 'tp')
- grad_pair: bfloat16 [16, 256, 256, 256], P('dp', 'tp')
- grad_attn_in: float32 [4, 768, 768], P(None, 'dp', 'tp')
- grad_attn_out: float32 [768, 768], P('tp', 'dp')
- grad_ff_in: float32 [2, 768, 3072], P(None, 'dp', 'tp')
- grad_ff_out: float32 [3072, 768], P('tp', 'dp')
- grad_ada: float32 [256, 4608], P(None, 'dp')
- grad_table: float32 [41, 256], P(None, 'dp')
- grad_pair_weight: float32 [12, 256], P(None, 'dp')
The draws below stay inside these ranges and needn't reach their ends.
Inputs may be any that keep to these rules, and one draw needn't show every extreme that they name: `chain_lengths`: every chain has at least a quarter of its 256 slots valid, and in each draw some chain has all 256.
All inputs are finite; a program needn't handle non-finite values.
Results may differ from the reference program's by a relative error of at most 0.02.
The reference program's roundings to bfloat16 on the way count: a program that leaves them out, or rounds other values in their place, can miss the bound.
Values may be sent and summed in bfloat16 or wider, within the bound.
A program may use at most 128 MiB of HBM per device.

```python
import math
import jax
import jax.numpy as jnp
from jax import lax

D = 768
H = 12
HD = 64
P_SIZE = 256
FF = 3072
COND = 256
NCLASS = 41
L = 256
CH_DEV = 2
CHAINS = 16
N_DP = 8


def draw_chain_lengths(key, part):
    first_key, second_key = jax.random.split(jax.random.fold_in(key, 17))
    drawn = jax.random.randint(first_key, (CHAINS,), L // 4, L + 1)
    full_spot = jax.random.randint(second_key, (), 0, CHAINS)
    return jnp.where(jnp.arange(CHAINS) == full_spot, L, drawn).astype(jnp.int32)


def touch_ends(result, own_key, smallest, high):
    shape = result.shape
    place = [jax.random.randint(jax.random.fold_in(own_key, axis), (), 0, shape[axis]) for axis in range(len(shape))]
    result = result.at[tuple(place)].set(smallest)
    longest = shape.index(max(shape))
    place[longest] = (place[longest] + 1) % shape[longest]
    return result.at[tuple(place)].set(high)


def spiked(values, key, source, target, parts, factor):
    owner, partner = [(jnp.arange(values.shape[dim]) // (values.shape[dim] // parts)).reshape([-1 if axis == dim else 1 for axis in range(values.ndim)]) for dim in (source, target)]
    chosen = jax.random.permutation(key, parts)[partner]
    strong = (owner == chosen) | (owner == (partner + parts // 2) % parts)
    return jnp.where(strong, factor * values, values)


def block_levels(rng, extent, shards, low, largest):
    level, own = 1.0, jax.random.fold_in(rng, 6)
    for position, shards_of in shards:
        steps = jnp.exp(jax.random.uniform(jax.random.fold_in(own, position), (shards_of,), jnp.float32, low / len(shards), largest / len(shards)))
        level = level * jnp.repeat(steps, extent[position] // shards_of).reshape([-1 if axis == position else 1 for axis in range(len(extent))])
    return level


def bell_draw(stream_key, extent, deviation, limit, cuts=(), held_as=jnp.bfloat16):
    entries = jax.random.normal(stream_key, extent, jnp.float32) * deviation
    if len(cuts) > 0:
        entries = block_levels(stream_key, extent, cuts, -0.22, 0.18) * entries
    return jnp.clip(entries, min=-limit, max=limit).astype(held_as)


def bell_draw_with(rng, extent, width, most, cuts, heavy, kind=jnp.bfloat16):
    values = width * jax.random.normal(rng, extent, jnp.float32)
    if cuts:
        values = values * block_levels(rng, extent, cuts, -0.22, 0.18)
    return jnp.clip(spiked(values, jax.random.fold_in(rng, 3), *heavy), -most, most).astype(kind)


def setup_inputs(seed: int = 0) -> dict:
    seeds = jax.random.split(jax.random.key(seed), 14)
    return {
        "activations": bell_draw(seeds[0], (CHAINS, L, D), 1.0, 6.0, ((0, 8), (1, 4))),
        "pair_rep": bell_draw(seeds[1], (CHAINS, L, L, P_SIZE), 1.0, 6.0, ((0, 8), (1, 4))),
        "noise_times": jnp.clip(1.0 * jax.random.uniform(seeds[2], (CHAINS,), jnp.float32) ** block_levels(seeds[2], (CHAINS,), ((0, 8),), -0.2, 0.2), 0.0, 1.0),
        "class_ids": touch_ends(jax.random.randint(seeds[3], (CHAINS,), 0, NCLASS), jax.random.fold_in(seeds[3], 1), 0, NCLASS - 1).astype(jnp.int32),
        "chain_lengths": draw_chain_lengths(jax.random.fold_in(seeds[13], 71), 0),
        "ada_weight": bell_draw(seeds[5], (COND, 6 * D), COND ** -0.5, 0.375),
        "class_table": bell_draw(seeds[6], (NCLASS, COND), 0.5, 4.0),
        "pair_weight": bell_draw(seeds[7], (H, P_SIZE), P_SIZE ** -0.5, 0.375),
        "attn_in": bell_draw(seeds[8], (4, D, D), D ** -0.5, 0.21875, ((2, 4),)),
        "attn_out": bell_draw(seeds[9], (D, D), (D // 128) ** -0.5, 2.5, ((0, 4),)),
        "ff_in": bell_draw(seeds[10], (2, D, FF), D ** -0.5, 0.21875, ((2, 4),)),
        "ff_out": bell_draw(seeds[11], (FF, D), FF ** -0.5, 0.109375, ((0, 4),)),
        "cotangent": bell_draw_with(seeds[12], (CHAINS, L, D), 1.0, 6.0, ((0, 8), (1, 4)), (0, 2, 8, 2.0)),
    }


@jax.custom_vjp
def low(v):
    return lax.optimization_barrier(v.astype(jnp.bfloat16)).astype(jnp.float32)

@jax.custom_vjp
def low_back(v):
    return v

def low_keep(v):
    return (low(v), None)

def low_pass(kept, grad):
    return (grad,)

def back_keep(v):
    return (v, None)

def back_low(kept, grad):
    return (low(grad),)
low.defvjp(low_keep, low_pass)
low_back.defvjp(back_keep, back_low)
highest = lax.Precision.HIGHEST

def time_features(noise_times):
    half_width = COND // 2
    freq_steps = jnp.arange(half_width).astype(jnp.float32)
    frequency = jnp.exp(freq_steps * (-math.log(10000.0) / half_width))
    angles = 100.0 * noise_times[:, None] * frequency[None, :]
    return jnp.concatenate([jnp.sin(angles), jnp.cos(angles)], axis=1)

def normalize(rows_in):
    centered = rows_in - lax.optimization_barrier(jnp.mean(rows_in, axis=-1, keepdims=True))
    return centered * lax.rsqrt(lax.optimization_barrier(jnp.mean(centered * centered, axis=-1, keepdims=True)) + 1e-05)

def forward(activations, pair_rep, ada_weight, class_table, pair_weight, attn_in, attn_out, ff_in, ff_out, noise_times, class_ids, chain_lengths):
    groups = activations.shape[0]
    onehot = (class_ids[:, None] == jnp.arange(NCLASS)[None, :]).astype(jnp.float32)
    condition = time_features(noise_times) + jnp.dot(onehot, class_table, precision=highest)
    modulation = jnp.dot(condition, ada_weight, precision=highest)
    pieces = [modulation[:, entry * D:(entry + 1) * D][:, None, :] for entry in range(6)]
    scale_attn, shift_attn, gate_attn, scale_ff, shift_ff, gate_ff = pieces
    rows_attn = low(normalize(activations) * (1.0 + scale_attn) + shift_attn)
    projected = [jnp.einsum('gld,de->gle', rows_attn, attn_in[entry], precision=highest) for entry in range(4)]
    query, key_rows, value_rows = [low(low_back(entry)).reshape(groups, L, H, HD) for entry in projected[:3]]
    gate_pre = low_back(projected[3])
    pair_bias = low(jnp.einsum('gqkp,hp->ghqk', pair_rep, pair_weight, precision=highest))
    scores = low_back(jnp.einsum('gqhe,gkhe->ghqk', query, key_rows, precision=highest) * HD ** (-0.5) + pair_bias)
    key_valid = jnp.arange(L)[None, :] < chain_lengths[:, None]
    scores = jnp.where(key_valid[:, None, None, :], scores, -1e+30)
    soft_weights = jax.nn.softmax(scores, axis=-1)
    head_mix = low_back(jnp.einsum('ghqk,gkhe->gqhe', low(soft_weights), value_rows, precision=highest)).reshape(groups, L, D)
    gated_mix = low(head_mix * jax.nn.sigmoid(gate_pre))
    attended = low_back(jnp.einsum('gle,ed->gld', gated_mix, attn_out, precision=highest))
    middle = activations + jax.nn.sigmoid(gate_attn) * attended
    rows_ff = low(normalize(middle) * (1.0 + scale_ff) + shift_ff)
    gate_up = low_back(jnp.einsum('gld,df->glf', rows_ff, ff_in[0], precision=highest))
    up_rows = low_back(jnp.einsum('gld,df->glf', rows_ff, ff_in[1], precision=highest))
    hidden = low(jax.nn.silu(gate_up) * up_rows)
    transition = low_back(jnp.einsum('glf,fd->gld', hidden, ff_out, precision=highest))
    return middle + jax.nn.sigmoid(gate_ff) * transition

def reference(activations, pair_rep, noise_times, class_ids, chain_lengths, ada_weight, class_table, pair_weight, attn_in, attn_out, ff_in, ff_out, cotangent):
    weights = tuple((entry.astype(jnp.float32) for entry in (ada_weight, class_table, pair_weight, attn_in, attn_out, ff_in, ff_out)))

    def split_groups(values):
        return values.reshape((N_DP, CH_DEV) + values.shape[1:])
    items = tuple((split_groups(entry) for entry in (activations, pair_rep, noise_times, class_ids, chain_lengths, cotangent)))

    def one_group(running, item):
        inputs_group, pair_group, times_group, classes_group, lengths_group, upstream = item

        def local_layer(inputs_in, pair_in, *params):
            return forward(inputs_in, pair_in, *params, times_group, classes_group, lengths_group)
        output, pullback = jax.vjp(local_layer, inputs_group.astype(jnp.float32), pair_group.astype(jnp.float32), *weights)
        gradients = pullback(upstream.astype(jnp.float32))
        running = tuple((first + second for first, second in zip(running, gradients[2:])))
        return (running, (output.astype(jnp.bfloat16), gradients[0].astype(jnp.bfloat16), gradients[1].astype(jnp.bfloat16)))
    start_sums = tuple((jnp.zeros(entry.shape, jnp.float32) for entry in weights))
    sums, stacked = lax.scan(one_group, start_sums, items)
    outputs, input_grads, pair_grads = stacked
    return (outputs.reshape(activations.shape), input_grads.reshape(activations.shape), pair_grads.reshape(pair_rep.shape), sums[3], sums[4], sums[5], sums[6], sums[0], sums[1], sums[2])
```

```python
import math

import jax
import jax.numpy as jnp
from jax import lax
from jax.sharding import PartitionSpec as P

highest = lax.Precision.HIGHEST


def time_features(noise_times, cond_width):
    half_width = cond_width // 2
    freq_steps = jnp.arange(half_width).astype(jnp.float32)
    frequency = jnp.exp(freq_steps * (-math.log(10000.0) / half_width))
    angles = 100.0 * noise_times[:, None] * frequency[None, :]
    return jnp.concatenate([jnp.sin(angles), jnp.cos(angles)], axis=1)


def normalize(rows_in):
    centered = rows_in - jnp.mean(rows_in, axis=-1, keepdims=True)
    inverse = lax.rsqrt(jnp.mean(centered * centered, axis=-1, keepdims=True) + 1e-05)
    return (centered * inverse, inverse)


def norm_back(grad_rows, normed, inverse):
    mean_grad = jnp.mean(grad_rows, axis=-1, keepdims=True)
    mean_cross = jnp.mean(grad_rows * normed, axis=-1, keepdims=True)
    return inverse * (grad_rows - mean_grad - normed * mean_cross)


def row_sums(values):
    return jnp.sum(values, axis=1)


def local(
    activations,
    pair_rep,
    noise_times,
    class_ids,
    chain_lengths,
    ada_weight,
    class_table,
    pair_weight,
    attn_in,
    attn_out,
    ff_in,
    ff_out,
    cotangent,
):
    chains, local_rows, width = activations.shape
    length = pair_rep.shape[2]
    heads_here = pair_weight.shape[0] // lax.axis_size("tp")
    head_local = attn_in.shape[2]
    head_width = head_local // heads_here
    score_scale = head_width ** (-0.5)
    head_shape = (chains, length, heads_here, head_width)
    onehot = (class_ids[:, None] == jnp.arange(class_table.shape[0])[None, :]).astype(jnp.float32)
    table_full = class_table.astype(jnp.float32)
    ada_full = ada_weight.astype(jnp.float32)
    condition = time_features(noise_times, class_table.shape[1]) + jnp.dot(
        onehot, table_full, precision=highest
    )
    modulation = jnp.dot(condition, ada_full, precision=highest)
    pieces = [modulation[:, entry * width : (entry + 1) * width][:, None, :] for entry in range(6)]
    scale_attn, shift_attn, gate_attn, scale_ff, shift_ff, gate_ff = pieces
    inputs_full = activations.astype(jnp.float32)
    normed_attn, inverse_attn = normalize(inputs_full)
    rows_attn = (normed_attn * (1.0 + scale_attn) + shift_attn).astype(jnp.bfloat16)
    gathered_attn = lax.all_gather(rows_attn, "tp", axis=1, tiled=True)
    projected = jnp.einsum(
        "gld,kde->kgle", gathered_attn, attn_in, preferred_element_type=jnp.float32
    )
    query = projected[0].astype(jnp.bfloat16).reshape(head_shape)
    key_rows = projected[1].astype(jnp.bfloat16).reshape(head_shape)
    value_rows = projected[2].astype(jnp.bfloat16).reshape(head_shape)
    gate_pre = projected[3]
    bias_local = jnp.einsum(
        "gqkp,hp->ghqk", pair_rep, pair_weight, preferred_element_type=jnp.float32
    ).astype(jnp.bfloat16)
    pair_bias = lax.all_to_all(bias_local, "tp", split_axis=1, concat_axis=2, tiled=True)
    key_valid = (jnp.arange(length)[None, :] < chain_lengths[:, None])[:, None, None, :]

    def masked_scores():
        raw_scores = jnp.einsum(
            "gqhe,gkhe->ghqk", query, key_rows, preferred_element_type=jnp.float32
        ) * score_scale + pair_bias.astype(jnp.float32)
        return jnp.where(key_valid, raw_scores, -1e30)

    scores = masked_scores()
    row_top = jnp.max(scores, axis=-1, keepdims=True)
    log_total = row_top + jnp.log(jnp.sum(jnp.exp(scores - row_top), axis=-1, keepdims=True))
    soft_low = jnp.exp(scores - log_total).astype(jnp.bfloat16)
    head_mix = jnp.einsum(
        "ghqk,gkhe->gqhe", soft_low, value_rows, preferred_element_type=jnp.float32
    ).reshape(chains, length, head_local)
    gate_sig = jax.nn.sigmoid(gate_pre)
    gated_mix = (head_mix * gate_sig).astype(jnp.bfloat16)
    attn_terms = jnp.einsum("gle,ed->gld", gated_mix, attn_out, preferred_element_type=jnp.float32)
    attended = lax.psum_scatter(
        attn_terms.astype(jnp.bfloat16), "tp", scatter_dimension=1, tiled=True
    ).astype(jnp.float32)
    sig_attn = jax.nn.sigmoid(gate_attn)
    middle = inputs_full + sig_attn * attended
    normed_ff, inverse_ff = normalize(middle)
    rows_ff = (normed_ff * (1.0 + scale_ff) + shift_ff).astype(jnp.bfloat16)
    gathered_ff = lax.all_gather(rows_ff, "tp", axis=1, tiled=True)
    gate_up = jnp.einsum("gld,kdf->kglf", gathered_ff, ff_in, preferred_element_type=jnp.float32)
    sig_hidden = jax.nn.sigmoid(gate_up[0])
    silu_hidden = gate_up[0] * sig_hidden
    hidden = (silu_hidden * gate_up[1]).astype(jnp.bfloat16)
    ff_terms = jnp.einsum("glf,fd->gld", hidden, ff_out, preferred_element_type=jnp.float32)
    transition = lax.psum_scatter(
        ff_terms.astype(jnp.bfloat16), "tp", scatter_dimension=1, tiled=True
    ).astype(jnp.float32)
    sig_ff = jax.nn.sigmoid(gate_ff)
    result = (middle + sig_ff * transition).astype(jnp.bfloat16)
    upstream = cotangent.astype(jnp.float32)
    grad_trans = (sig_ff * upstream).astype(jnp.bfloat16)
    grad_gate_ff = row_sums(upstream * transition) * (sig_ff * (1.0 - sig_ff))[:, 0, :]
    gathered_grad_ff = lax.all_gather(grad_trans, "tp", axis=1, tiled=True)
    grad_ff_out = jnp.einsum(
        "glf,gld->fd", hidden, gathered_grad_ff, preferred_element_type=jnp.float32
    )
    grad_hidden = jnp.einsum(
        "gld,fd->glf", gathered_grad_ff, ff_out, preferred_element_type=jnp.float32
    )
    silu_slope = sig_hidden * (1.0 + gate_up[0] * (1.0 - sig_hidden))
    grad_gate_up = jnp.stack(
        [grad_hidden * gate_up[1] * silu_slope, grad_hidden * silu_hidden]
    ).astype(jnp.bfloat16)
    grad_ff_in = jnp.einsum(
        "gld,kglf->kdf", gathered_ff, grad_gate_up, preferred_element_type=jnp.float32
    )
    ff_row_terms = jnp.einsum(
        "kglf,kdf->gld", grad_gate_up, ff_in, preferred_element_type=jnp.float32
    )
    grad_rows_ff = lax.psum_scatter(
        ff_row_terms.astype(jnp.bfloat16), "tp", scatter_dimension=1, tiled=True
    ).astype(jnp.float32)
    grad_scale_ff = row_sums(grad_rows_ff * normed_ff)
    grad_shift_ff = row_sums(grad_rows_ff)
    grad_middle = upstream + norm_back(grad_rows_ff * (1.0 + scale_ff), normed_ff, inverse_ff)
    grad_attended = (sig_attn * grad_middle).astype(jnp.bfloat16)
    grad_gate_attn = row_sums(grad_middle * attended) * (sig_attn * (1.0 - sig_attn))[:, 0, :]
    gathered_grad_attn = lax.all_gather(grad_attended, "tp", axis=1, tiled=True)
    grad_attn_out = jnp.einsum(
        "gle,gld->ed", gated_mix, gathered_grad_attn, preferred_element_type=jnp.float32
    )
    grad_gated = jnp.einsum(
        "gld,ed->gle", gathered_grad_attn, attn_out, preferred_element_type=jnp.float32
    )
    grad_mix = (grad_gated * gate_sig).astype(jnp.bfloat16)
    grad_gate_pre = (grad_gated * head_mix * gate_sig * (1.0 - gate_sig)).astype(jnp.bfloat16)
    grad_mix_heads = grad_mix.reshape(head_shape)
    soft_full = jnp.exp(masked_scores() - log_total)
    grad_soft = jnp.einsum(
        "gqhe,gkhe->ghqk", grad_mix_heads, value_rows, preferred_element_type=jnp.float32
    )
    grad_scores = (
        soft_full * (grad_soft - jnp.sum(grad_soft * soft_full, axis=-1, keepdims=True))
    ).astype(jnp.bfloat16)
    grad_query = (
        jnp.einsum("ghqk,gkhe->gqhe", grad_scores, key_rows, preferred_element_type=jnp.float32)
        * score_scale
    ).astype(jnp.bfloat16)
    grad_key = (
        jnp.einsum("ghqk,gqhe->gkhe", grad_scores, query, preferred_element_type=jnp.float32)
        * score_scale
    ).astype(jnp.bfloat16)
    grad_value = jnp.einsum(
        "ghqk,gqhe->gkhe", soft_low, grad_mix_heads, preferred_element_type=jnp.float32
    ).astype(jnp.bfloat16)
    flat_shape = (chains, length, head_local)
    grad_heads = jnp.stack(
        [
            grad_query.reshape(flat_shape),
            grad_key.reshape(flat_shape),
            grad_value.reshape(flat_shape),
            grad_gate_pre,
        ]
    )
    grad_attn_in = jnp.einsum(
        "gld,kgle->kde", gathered_attn, grad_heads, preferred_element_type=jnp.float32
    )
    attn_row_terms = jnp.einsum(
        "kgle,kde->gld", grad_heads, attn_in, preferred_element_type=jnp.float32
    )
    grad_rows_attn = lax.psum_scatter(
        attn_row_terms.astype(jnp.bfloat16), "tp", scatter_dimension=1, tiled=True
    ).astype(jnp.float32)
    grad_scale_attn = row_sums(grad_rows_attn * normed_attn)
    grad_shift_attn = row_sums(grad_rows_attn)
    grad_inputs = (
        grad_middle + norm_back(grad_rows_attn * (1.0 + scale_attn), normed_attn, inverse_attn)
    ).astype(jnp.bfloat16)
    bias_grads = lax.all_to_all(grad_scores, "tp", split_axis=2, concat_axis=1, tiled=True)
    grad_pair = jnp.einsum(
        "ghqk,hp->gqkp", bias_grads, pair_weight, preferred_element_type=jnp.float32
    ).astype(jnp.bfloat16)
    pair_weight_part = jnp.einsum(
        "gqkp,ghqk->hp", pair_rep, bias_grads, preferred_element_type=jnp.float32
    )
    modulation_part = jnp.concatenate(
        [
            grad_scale_attn,
            grad_shift_attn,
            grad_gate_attn,
            grad_scale_ff,
            grad_shift_ff,
            grad_gate_ff,
        ],
        axis=1,
    )
    grad_modulation, pair_weight_sum = (
        lax.psum(modulation_part.astype(jnp.bfloat16), "tp").astype(jnp.float32),
        lax.psum(pair_weight_part.astype(jnp.bfloat16), "tp").astype(jnp.float32),
    )
    grad_condition = jnp.dot(grad_modulation, ada_full.T, precision=highest)
    parts = lax.axis_size("dp")
    place = lax.axis_index("dp")
    sizes = [ada_full.shape[1], condition.shape[1], condition.shape[1], onehot.shape[1]]
    chain_rows = jnp.concatenate([grad_modulation, grad_condition, condition, onehot], axis=1)
    packed = jnp.concatenate([chain_rows.reshape(-1), pair_weight_sum.reshape(-1)])
    packed = jnp.pad(packed, (0, -packed.size % 1024)).reshape(-1, 128)
    gathered = lax.all_gather(packed, "dp", axis=0, tiled=True).reshape(parts, -1)
    rows_all = gathered[:, : chain_rows.size].reshape(parts * chains, chain_rows.shape[1])
    pair_all = gathered[:, chain_rows.size : chain_rows.size + pair_weight.size].reshape(
        (parts,) + pair_weight.shape
    )
    cuts = [sum(sizes[:entry]) for entry in range(5)]
    mod_all, grad_cond_all, cond_all, onehot_all = [
        rows_all[:, cuts[entry] : cuts[entry + 1]] for entry in range(4)
    ]

    def own_columns(values, axis):
        width_here = values.shape[axis] // parts
        return lax.dynamic_slice_in_dim(values, place * width_here, width_here, axis)

    grad_ada = jnp.dot(cond_all.T, own_columns(mod_all, 1), precision=highest)
    grad_table = jnp.dot(onehot_all.T, own_columns(grad_cond_all, 1), precision=highest)
    grad_pair_weight = jnp.sum(own_columns(pair_all, 2), axis=0)

    def summed_over_chains(values_list, axes):
        pieces, shapes = [], []
        for values, axis in zip(values_list, axes):
            split = values.shape[:axis] + (parts, values.shape[axis] // parts) + values.shape[axis + 1 :]
            moved = jnp.moveaxis(values.astype(jnp.bfloat16).reshape(split), axis, 0)
            shapes.append(moved.shape[1:])
            pieces.append(moved.reshape(parts, -1, 128))
        joined = jnp.concatenate(pieces, axis=1)
        own = lax.psum_scatter(
            joined.reshape(-1, 128), "dp", scatter_dimension=0, tiled=True
        ).astype(jnp.float32)
        results, start = [], 0
        for piece, shape in zip(pieces, shapes):
            results.append(own[start : start + piece.shape[1]].reshape(shape))
            start += piece.shape[1]
        return results

    sum_ff_in, sum_ff_out = summed_over_chains([grad_ff_in, grad_ff_out], [1, 1])
    sum_attn_in, sum_attn_out = summed_over_chains([grad_attn_in, grad_attn_out], [1, 1])
    summed = (
        sum_attn_in,
        sum_attn_out,
        sum_ff_in,
        sum_ff_out,
        grad_ada,
        grad_table,
        grad_pair_weight,
    )
    return (result, grad_inputs, grad_pair) + tuple(summed)


def solution(mesh):
    return jax.shard_map(
        local,
        mesh=mesh,
        in_specs=(
            P("dp", "tp", None),
            P("dp", "tp", None, None),
            P("dp"),
            P("dp"),
            P("dp"),
            P(),
            P(),
            P(),
            P(None, None, "tp"),
            P("tp", None),
            P(None, None, "tp"),
            P("tp", None),
            P("dp", "tp", None),
        ),
        out_specs=(
            P("dp", "tp", None),
            P("dp", "tp", None),
            P("dp", "tp", None, None),
            P(None, "dp", "tp"),
            P("tp", "dp"),
            P(None, "dp", "tp"),
            P("tp", "dp"),
            P(None, "dp"),
            P(None, "dp"),
            P(None, "dp"),
        ),
        check_vma=False,
    )
```

```python
import functools
import math

import jax
import jax.numpy as jnp
from jax import lax
from jax.experimental import pallas as pl
from jax.experimental.pallas import tpu as pltpu
from jax.sharding import PartitionSpec as P

highest = lax.Precision.HIGHEST
MESH = pl.DeviceIdType.MESH
f32, bf16 = jnp.float32, jnp.bfloat16
EPS = 1e-05
LANES = 128
NN = (((1,), (0,)), ((), ()))
NT = (((1,), (1,)), ((), ()))
TN = (((0,), (0,)), ((), ()))


def dot(left, right, dims=NN):
    return lax.dot_general(left, right, dims, preferred_element_type=f32)


def time_features(noise_times, cond_width):
    half_width = cond_width // 2
    freq_steps = jnp.arange(half_width).astype(jnp.float32)
    frequency = jnp.exp(freq_steps * (-math.log(10000.0) / half_width))
    angles = 100.0 * noise_times[:, None] * frequency[None, :]
    return jnp.concatenate([jnp.sin(angles), jnp.cos(angles)], axis=1)


def normalize(rows_in):
    centered = rows_in - jnp.mean(rows_in, axis=-1, keepdims=True)
    inverse = lax.rsqrt(jnp.mean(centered * centered, axis=-1, keepdims=True) + EPS)
    return centered * inverse, inverse


def norm_back(grad_rows, normed, inverse):
    mean_grad = jnp.mean(grad_rows, axis=-1, keepdims=True)
    mean_cross = jnp.mean(grad_rows * normed, axis=-1, keepdims=True)
    return inverse * (grad_rows - mean_grad - normed * mean_cross)


def lanes(part):
    return slice(part * LANES, (part + 1) * LANES)


def enter(peers):
    barrier = pltpu.get_barrier_semaphore()
    for peer in peers:
        pl.semaphore_signal(barrier, inc=1, device_id=peer, device_id_type=MESH)
    pl.semaphore_wait(barrier, len(peers))


def send(src, dst, sems, index, peer):
    copy = pltpu.make_async_remote_copy(
        src_ref=src,
        dst_ref=dst,
        send_sem=sems.at[(0,) + index],
        recv_sem=sems.at[(1,) + index],
        device_id=peer,
        device_id_type=MESH,
    )
    copy.start()
    return copy


def own_rows(me, rows):
    return pl.ds(pl.multiple_of(me * rows, rows), rows)


def gather_send(full, chain, me, rows, sems, peers):
    place = full.at[chain, own_rows(me, rows)]
    return [
        send(place, place, sems, (chain, step), peer) for step, (_, peer) in enumerate(peers)
    ]


def scatter_send(terms, landing, chain, rows, sems, peers):
    return [
        send(terms.at[chain, own_rows(index, rows)], landing.at[step, chain], sems, (chain, step), peer)
        for step, (index, peer) in enumerate(peers)
    ]


def scatter_take(terms, landing, chain, me, rows):
    total = terms[chain, own_rows(me, rows)].astype(f32)
    for step in range(landing.shape[0]):
        total = total + landing[step, chain].astype(f32)
    return total


def tp_peers(n_tp):
    me = lax.axis_index("tp")
    return me, [(me ^ step, {"tp": me ^ step}) for step in range(1, n_tp)]


def attn_fwd_kernel(
    sizes,
    inputs,
    mods,
    valid,
    pair_w,
    w_in,
    w_out,
    pair_hbm,
    rows_full,
    heads_out,
    gate_out,
    soft_out,
    mix_out,
    gated_out,
    attended_out,
    middle_out,
    pair_buf,
    stack,
    bias_send,
    bias_full,
    terms,
    landing,
    rows_sems,
    bias_sems,
    terms_sems,
    pair_sems,
):
    n_tp, heads, width = sizes
    chains, rows, _ = inputs.shape
    length = rows_full.shape[1]
    block = heads * width
    me, peers = tp_peers(n_tp)
    step_rows = pair_buf.shape[1]
    steps = rows // step_rows

    def fetch(turn, slot):
        return pltpu.make_async_copy(
            pair_hbm.at[turn // steps, pl.ds(lax.rem(turn, steps) * step_rows, step_rows)],
            pair_buf.at[slot],
            pair_sems.at[slot],
        )

    fetch(0, 0).start()
    fetch(1, 1).start()
    enter([peer for _, peer in peers])
    rows_sent = []
    for chain in range(chains):
        normed, _ = normalize(inputs[chain].astype(f32))
        rows_full[chain, own_rows(me, rows)] = (normed * mods[0, chain] + mods[1, chain]).astype(bf16)
        rows_sent.append(gather_send(rows_full, chain, me, rows, rows_sems, peers))

    all_heads = heads * n_tp
    padded = pair_w.shape[0]
    pair_w_here = pair_w[...]
    bias_sent = []
    for chain in range(chains):

        def bias_step(step, carry):
            turn = chain * steps + step
            slot = lax.rem(turn, 2)
            fetch(turn, slot).wait()
            for row in range(step_rows):
                found = dot(pair_w_here, pair_buf[slot, row], NT)
                for part in range(length // LANES):
                    stack[part, row * padded : (row + 1) * padded, :] = found[:, lanes(part)]

            @pl.when(turn + 2 < chains * steps)
            def _():
                fetch(turn + 2, slot).start()

            place = pl.ds(pl.multiple_of(step * step_rows, step_rows), step_rows)
            for head in range(all_heads):
                for part in range(length // LANES):
                    bias_send[head // heads, chain, head % heads, place, lanes(part)] = stack[
                        part, pl.ds(head, step_rows, stride=padded), :
                    ].astype(bf16)
            return carry

        lax.fori_loop(0, steps, bias_step, 0)
        bias_sent.append(
            [
                send(
                    bias_send.at[index, chain],
                    bias_full.at[chain, :, own_rows(me, rows), :],
                    bias_sems,
                    (chain, step),
                    peer,
                )
                for step, (index, peer) in enumerate(peers)
            ]
        )

    for chain in range(chains):
        bias_full[chain, :, own_rows(me, rows), :] = bias_send[me, chain]

    terms_sent = []
    for chain in range(chains):
        for copy in rows_sent[chain]:
            copy.wait_recv()
        projected = dot(rows_full[chain], w_in[...])
        heads_out[chain] = projected.astype(bf16)
        gate_out[chain] = jax.nn.sigmoid(projected[:, 3 * block :])
        for copy in bias_sent[chain]:
            copy.wait_recv()
        mixes = []
        for head in range(heads):
            at = head * width
            query = heads_out[chain, :, at : at + width]
            key_rows = heads_out[chain, :, block + at : block + at + width]
            value_rows = heads_out[chain, :, 2 * block + at : 2 * block + at + width]
            scores = dot(query, key_rows, NT) * width ** (-0.5) + bias_full[chain, head].astype(f32)
            scores = jnp.where(valid[chain] > 0.0, scores, -1e30)
            top = jnp.max(scores, axis=-1, keepdims=True)
            raised = jnp.exp(scores - top)
            soft = raised / jnp.sum(raised, axis=-1, keepdims=True)
            soft_out[chain, head] = soft
            mixes.append(dot(soft.astype(bf16), value_rows))
        mix = jnp.concatenate(mixes, axis=1)
        mix_out[chain] = mix
        gated = (mix * gate_out[chain]).astype(bf16)
        gated_out[chain] = gated
        terms[chain] = dot(gated, w_out[...]).astype(bf16)
        terms_sent.append(scatter_send(terms, landing, chain, rows, terms_sems, peers))

    for chain in range(chains):
        for copy in terms_sent[chain]:
            copy.wait_recv()
        attended = scatter_take(terms, landing, chain, me, rows)
        attended_out[chain] = attended
        middle_out[chain] = inputs[chain].astype(f32) + mods[2, chain] * attended
    for group in rows_sent + bias_sent + terms_sent:
        for copy in group:
            copy.wait_send()


def ff_kernel(
    sizes,
    middle,
    cotangent,
    attended,
    mods,
    w_in,
    w_out,
    result_out,
    grad_middle_out,
    grad_att_out,
    sums_out,
    weight_out,
    rows_full,
    grad_full,
    gate_keep,
    up_keep,
    hidden_keep,
    grad_gu,
    terms,
    back_terms,
    landing,
    back_landing,
    rows_sems,
    grad_sems,
    terms_sems,
    back_sems,
):
    n_tp, tile = sizes
    chains, rows, depth = middle.shape
    length = rows_full.shape[1]
    hidden_width = w_out.shape[0]
    tiles = hidden_width // tile
    me, peers = tp_peers(n_tp)
    enter([peer for _, peer in peers])
    rows_sent, grad_sent, terms_sent, back_sent = [], [], [], []
    for chain in range(chains):
        normed, _ = normalize(middle[chain])
        rows_full[chain, own_rows(me, rows)] = (normed * mods[3, chain] + mods[4, chain]).astype(bf16)
        rows_sent.append(gather_send(rows_full, chain, me, rows, rows_sems, peers))
    for chain in range(chains):
        grad_full[chain, own_rows(me, rows)] = (mods[5, chain] * cotangent[chain].astype(f32)).astype(bf16)
        grad_sent.append(gather_send(grad_full, chain, me, rows, grad_sems, peers))
    for chain in range(chains):
        for copy in rows_sent[chain]:
            copy.wait_recv()
        for part in range(tiles):
            here = slice(part * tile, (part + 1) * tile)
            gate = dot(rows_full[chain], w_in[0, :, here])
            up = dot(rows_full[chain], w_in[1, :, here])
            gate_keep[chain, :, here] = gate
            up_keep[chain, :, here] = up
            hidden_keep[chain, :, here] = (gate * jax.nn.sigmoid(gate) * up).astype(bf16)
        for part in range(depth // tile):
            here = slice(part * tile, (part + 1) * tile)
            terms[chain, :, here] = dot(hidden_keep[chain], w_out[:, here]).astype(bf16)
        terms_sent.append(scatter_send(terms, landing, chain, rows, terms_sems, peers))
    for chain in range(chains):
        for copy in grad_sent[chain]:
            copy.wait_recv()
        for part in range(tiles):
            here = slice(part * tile, (part + 1) * tile)
            grad_hidden = dot(grad_full[chain], w_out[here, :], NT)
            gate = gate_keep[chain, :, here]
            sig = jax.nn.sigmoid(gate)
            slope = sig * (1.0 + gate * (1.0 - sig))
            grad_gu[0, chain, :, here] = (grad_hidden * up_keep[chain, :, here] * slope).astype(bf16)
            grad_gu[1, chain, :, here] = (grad_hidden * (gate * sig)).astype(bf16)
        for part in range(depth // tile):
            here = slice(part * tile, (part + 1) * tile)
            back_terms[chain, :, here] = (
                dot(grad_gu[0, chain], w_in[0, here, :], NT) + dot(grad_gu[1, chain], w_in[1, here, :], NT)
            ).astype(bf16)
        back_sent.append(scatter_send(back_terms, back_landing, chain, rows, back_sems, peers))

    def flat(ref_value):
        return ref_value.reshape(chains * length, ref_value.shape[-1])

    for part in range(tiles):
        here = slice(part * tile, (part + 1) * tile)
        for which in range(2):
            weight_out[which, :, here] = dot(
                flat(rows_full[...]), flat(grad_gu[which, :, :, here]), TN
            ).astype(bf16)
        weight_out[2, :, here] = dot(
            flat(grad_full[...]), flat(hidden_keep[:, :, here]), TN
        ).astype(bf16)

    for chain in range(chains):
        for copy in terms_sent[chain]:
            copy.wait_recv()
        transition = scatter_take(terms, landing, chain, me, rows)
        upstream = cotangent[chain].astype(f32)
        result_out[chain] = (middle[chain] + mods[5, chain] * transition).astype(bf16)
        sums_out[3, chain] = jnp.sum(upstream * transition, axis=0, keepdims=True)
    for chain in range(chains):
        for copy in back_sent[chain]:
            copy.wait_recv()
        grad_rows = scatter_take(back_terms, back_landing, chain, me, rows)
        normed, inverse = normalize(middle[chain])
        sums_out[1, chain] = jnp.sum(grad_rows * normed, axis=0, keepdims=True)
        sums_out[2, chain] = jnp.sum(grad_rows, axis=0, keepdims=True)
        grad_middle = cotangent[chain].astype(f32) + norm_back(grad_rows * mods[3, chain], normed, inverse)
        grad_middle_out[chain] = grad_middle
        grad_att_out[chain] = (mods[2, chain] * grad_middle).astype(bf16)
        sums_out[0, chain] = jnp.sum(grad_middle * attended[chain], axis=0, keepdims=True)
    for group in rows_sent + grad_sent + terms_sent + back_sent:
        for copy in group:
            copy.wait_send()


def attn_bwd_kernel(
    sizes,
    inputs,
    mods,
    grad_att,
    grad_middle,
    rows_full,
    heads_kept,
    gate_sig,
    soft,
    mix,
    gated,
    w_in,
    w_out,
    pair_w,
    pair_hbm,
    grad_inputs_out,
    sums_out,
    pair_w_out,
    weight_out,
    grad_pair_hbm,
    grad_full,
    grad_heads,
    score_send,
    score_full,
    terms,
    landing,
    stack,
    pair_buf,
    out_buf,
    grad_sems,
    score_sems,
    terms_sems,
    pair_sems,
    out_sems,
):
    n_tp, heads, width = sizes
    chains, rows, depth = inputs.shape
    length = rows_full.shape[1]
    block = heads * width
    scale = width ** (-0.5)
    me, peers = tp_peers(n_tp)
    step_rows = pair_buf.shape[1]
    steps = rows // step_rows
    turns = chains * steps

    def fetch(turn, slot):
        return pltpu.make_async_copy(
            pair_hbm.at[turn // steps, pl.ds(lax.rem(turn, steps) * step_rows, step_rows)],
            pair_buf.at[slot],
            pair_sems.at[slot],
        )

    def put(turn, slot):
        return pltpu.make_async_copy(
            out_buf.at[slot],
            grad_pair_hbm.at[turn // steps, pl.ds(lax.rem(turn, steps) * step_rows, step_rows)],
            out_sems.at[slot],
        )

    fetch(0, 0).start()
    fetch(1, 1).start()
    enter([peer for _, peer in peers])
    grad_sent, score_sent, terms_sent = [], [], []
    for chain in range(chains):
        grad_full[chain, own_rows(me, rows)] = grad_att[chain]
        grad_sent.append(gather_send(grad_full, chain, me, rows, grad_sems, peers))
    for chain in range(chains):
        for copy in grad_sent[chain]:
            copy.wait_recv()
        grad_gated = dot(grad_full[chain], w_out[...], NT)
        sig = gate_sig[chain]
        grad_mix = (grad_gated * sig).astype(bf16)
        grad_gate = (grad_gated * mix[chain] * sig * (1.0 - sig)).astype(bf16)
        queries, keys, values = [], [], []
        for head in range(heads):
            at = head * width
            query = heads_kept[chain, :, at : at + width]
            key_rows = heads_kept[chain, :, block + at : block + at + width]
            value_rows = heads_kept[chain, :, 2 * block + at : 2 * block + at + width]
            grad_mix_head = grad_mix[:, at : at + width]
            weights = soft[chain, head]
            grad_soft = dot(grad_mix_head, value_rows, NT)
            inner = jnp.sum(grad_soft * weights, axis=-1, keepdims=True)
            grad_scores = (weights * (grad_soft - inner)).astype(bf16)
            for owner in range(n_tp):
                score_send[owner, chain, head] = grad_scores[owner * rows : (owner + 1) * rows, :]
            queries.append((dot(grad_scores, key_rows) * scale).astype(bf16))
            keys.append((dot(grad_scores, query, TN) * scale).astype(bf16))
            values.append(dot(weights.astype(bf16), grad_mix_head, TN).astype(bf16))
        score_sent.append(
            [
                send(
                    score_send.at[index, chain],
                    score_full.at[me, chain],
                    score_sems,
                    (chain, step),
                    peer,
                )
                for step, (index, peer) in enumerate(peers)
            ]
        )
        score_full[me, chain] = score_send[me, chain]
        grad_heads[chain] = jnp.concatenate(queries + keys + values + [grad_gate], axis=1)
        terms[chain] = dot(grad_heads[chain], w_in[...], NT).astype(bf16)
        terms_sent.append(scatter_send(terms, landing, chain, rows, terms_sems, peers))

    def flat(ref_value):
        return ref_value.reshape(chains * length, ref_value.shape[-1])

    weight_out[0, :, : 4 * block] = dot(flat(rows_full[...]), flat(grad_heads[...]), TN).astype(bf16)
    weight_out[0, :, 4 * block : 5 * block] = dot(
        flat(grad_full[...]), flat(gated[...]), TN
    ).astype(bf16)
    weight_out[0, :, 5 * block :] = jnp.zeros((depth, weight_out.shape[2] - 5 * block), bf16)

    for chain in range(chains):
        for copy in terms_sent[chain]:
            copy.wait_recv()
        grad_rows = scatter_take(terms, landing, chain, me, rows)
        normed, inverse = normalize(inputs[chain].astype(f32))
        sums_out[0, chain] = jnp.sum(grad_rows * normed, axis=0, keepdims=True)
        sums_out[1, chain] = jnp.sum(grad_rows, axis=0, keepdims=True)
        grad_inputs_out[chain] = (
            grad_middle[chain] + norm_back(grad_rows * mods[0, chain], normed, inverse)
        ).astype(bf16)

    for chain in range(chains):
        for copy in score_sent[chain]:
            copy.wait_recv()

    padded = pair_w.shape[0]
    pair_w_here = pair_w[...]
    pair_w_out[...] = jnp.zeros_like(pair_w_out)
    stack[...] = jnp.zeros_like(stack)

    def pair_step(turn, carry):
        slot = lax.rem(turn, 2)
        chain = turn // steps
        fetch(turn, slot).wait()
        place = pl.ds(pl.multiple_of(lax.rem(turn, steps) * step_rows, step_rows), step_rows)
        for head in range(heads * n_tp):
            for part in range(length // LANES):
                stack[part, pl.ds(head, step_rows, stride=padded), :] = score_full[
                    head // heads, chain, head % heads, place, lanes(part)
                ].astype(f32)

        @pl.when(turn >= 2)
        def _():
            put(turn - 2, slot).wait()

        total = jnp.zeros(pair_w_out.shape, f32)
        for row in range(step_rows):
            scores = jnp.concatenate(
                [stack[part, row * padded : (row + 1) * padded, :] for part in range(length // LANES)],
                axis=1,
            ).astype(bf16)
            out_buf[slot, row] = dot(scores, pair_w_here, TN).astype(bf16)
            total = total + dot(scores, pair_buf[slot, row])
        pair_w_out[...] += total

        @pl.when(turn + 2 < turns)
        def _():
            fetch(turn + 2, slot).start()

        put(turn, slot).start()
        return carry

    lax.fori_loop(0, turns, pair_step, 0)
    put(turns - 2, lax.rem(turns - 2, 2)).wait()
    put(turns - 1, lax.rem(turns - 1, 2)).wait()
    for group in grad_sent + score_sent + terms_sent:
        for copy in group:
            copy.wait_send()


def dp_sum_kernel(sizes, values, out, stage, sums, landing, first_sems, second_sems):
    n_z, n_y, pieces = sizes
    place = lax.axis_index("dp")
    z, y = place // n_y, lax.rem(place, n_y)
    other = {"dp": place ^ 1}
    line = [(lax.rem(z + step, n_z), {"dp": lax.rem(z + step, n_z) * n_y + y}) for step in range(1, n_z)]
    enter([other] + [peer for _, peer in line])
    size = out.shape[1] // pieces

    def cut(piece):
        return pl.ds(piece * size, size)

    first = {}
    for piece in range(pieces):
        for step in range(n_z):
            target = line[step][0] if step < n_z - 1 else z
            first[piece, step] = send(
                values.at[:, target * n_y + 1 - y, cut(piece)],
                stage.at[step, :, cut(piece)],
                first_sems,
                (piece, step),
                other,
            )
    second = {}
    for piece in range(pieces):
        for step in range(n_z):
            target = line[step][0] if step < n_z - 1 else z
            first[piece, step].wait_recv()
            total = values[:, target * n_y + y, cut(piece)].astype(f32) + stage[step, :, cut(piece)].astype(f32)
            if step < n_z - 1:
                sums[step, :, cut(piece)] = total.astype(bf16)
                second[piece, step] = send(
                    sums.at[step, :, cut(piece)],
                    landing.at[step, :, cut(piece)],
                    second_sems,
                    (piece, step),
                    line[step][1],
                )
            else:
                out[:, cut(piece)] = total
    for piece in range(pieces):
        for step in range(n_z - 1):
            second[piece, step].wait_recv()
            out[:, cut(piece)] += landing[step, :, cut(piece)].astype(f32)
    for copy in list(first.values()) + list(second.values()):
        copy.wait_send()


VMEM_SPEC = pl.BlockSpec(memory_space=pltpu.VMEM)
ANY_SPEC = pl.BlockSpec(memory_space=pl.ANY)


def pair_sems(*shape):
    return pltpu.SemaphoreType.DMA((2,) + shape)


def params(collective_id):
    return pltpu.CompilerParams(
        collective_id=collective_id, has_side_effects=True, vmem_limit_bytes=62 * 1024 * 1024
    )


def local(
    activations,
    pair_rep,
    noise_times,
    class_ids,
    chain_lengths,
    ada_weight,
    class_table,
    pair_weight,
    attn_in,
    attn_out,
    ff_in,
    ff_out,
    cotangent,
):
    n_tp, n_dp = lax.axis_size("tp"), lax.axis_size("dp")
    chains, rows, depth = activations.shape
    length, channels = pair_rep.shape[2:]
    all_heads = pair_weight.shape[0]
    heads = all_heads // n_tp
    block = attn_in.shape[2]
    width = block // heads
    hidden_width = ff_out.shape[0]
    sds = jax.ShapeDtypeStruct

    onehot = (class_ids[:, None] == jnp.arange(class_table.shape[0])[None, :]).astype(f32)
    table_full = class_table.astype(f32)
    ada_full = ada_weight.astype(f32)
    condition = time_features(noise_times, class_table.shape[1]) + jnp.dot(
        onehot, table_full, precision=highest
    )
    modulation = jnp.dot(condition, ada_full, precision=highest)
    pieces = modulation.reshape(chains, 6, 1, depth)
    sig_attn, sig_ff = jax.nn.sigmoid(pieces[:, 2]), jax.nn.sigmoid(pieces[:, 5])
    mods = jnp.stack(
        [1.0 + pieces[:, 0], pieces[:, 1], sig_attn, 1.0 + pieces[:, 3], pieces[:, 4], sig_ff]
    )
    valid = (jnp.arange(length)[None, :] < chain_lengths[:, None]).astype(f32)[:, None, :]
    padded = -(-all_heads // 16) * 16
    pair_w = jnp.pad(pair_weight, ((0, padded - all_heads), (0, 0)))
    w_in = jnp.swapaxes(attn_in, 0, 1).reshape(depth, 4 * block)

    step_rows = 16
    full = (chains, length, depth)
    own = (chains, rows, depth)
    rows_full, heads_kept, gate_sig, soft, mix, gated, attended, middle = pl.pallas_call(
        functools.partial(attn_fwd_kernel, (n_tp, heads, width)),
        out_shape=(
            sds(full, bf16),
            sds((chains, length, 4 * block), bf16),
            sds((chains, length, block), f32),
            sds((chains, heads, length, length), f32),
            sds((chains, length, block), f32),
            sds((chains, length, block), bf16),
            sds(own, f32),
            sds(own, f32),
        ),
        in_specs=[VMEM_SPEC] * 6 + [ANY_SPEC],
        out_specs=[VMEM_SPEC] * 8,
        scratch_shapes=[
            pltpu.VMEM((2, step_rows, length, channels), bf16),
            pltpu.VMEM((length // LANES, step_rows * padded, LANES), f32),
            pltpu.VMEM((n_tp, chains, heads, rows, length), bf16),
            pltpu.VMEM((chains, heads, length, length), bf16),
            pltpu.VMEM(full, bf16),
            pltpu.VMEM((n_tp - 1,) + own, bf16),
            pair_sems(chains, n_tp - 1),
            pair_sems(chains, n_tp - 1),
            pair_sems(chains, n_tp - 1),
            pltpu.SemaphoreType.DMA((2,)),
        ],
        compiler_params=params(0),
        name="attn_fwd",
    )(activations, mods, valid, pair_w, w_in, attn_out, pair_rep)

    result, grad_middle, grad_att, ff_sums, ff_weights = pl.pallas_call(
        functools.partial(ff_kernel, (n_tp, 256)),
        out_shape=(
            sds(own, bf16),
            sds(own, f32),
            sds(own, bf16),
            sds((4, chains, 1, depth), f32),
            sds((3, depth, hidden_width), bf16),
        ),
        in_specs=[VMEM_SPEC] * 6,
        out_specs=[VMEM_SPEC] * 5,
        scratch_shapes=[
            pltpu.VMEM(full, bf16),
            pltpu.VMEM(full, bf16),
            pltpu.VMEM((chains, length, hidden_width), f32),
            pltpu.VMEM((chains, length, hidden_width), f32),
            pltpu.VMEM((chains, length, hidden_width), bf16),
            pltpu.VMEM((2, chains, length, hidden_width), bf16),
            pltpu.VMEM(full, bf16),
            pltpu.VMEM(full, bf16),
            pltpu.VMEM((n_tp - 1,) + own, bf16),
            pltpu.VMEM((n_tp - 1,) + own, bf16),
            pair_sems(chains, n_tp - 1),
            pair_sems(chains, n_tp - 1),
            pair_sems(chains, n_tp - 1),
            pair_sems(chains, n_tp - 1),
        ],
        compiler_params=params(1),
        name="ff",
    )(middle, cotangent, attended, mods, ff_in, ff_out)

    grad_inputs, attn_sums, pair_part, attn_weights, grad_pair = pl.pallas_call(
        functools.partial(attn_bwd_kernel, (n_tp, heads, width)),
        out_shape=(
            sds(own, bf16),
            sds((2, chains, 1, depth), f32),
            sds((padded, channels), f32),
            sds((1, depth, -(-5 * block // LANES) * LANES), bf16),
            sds(pair_rep.shape, bf16),
        ),
        in_specs=[VMEM_SPEC] * 13 + [ANY_SPEC],
        out_specs=[VMEM_SPEC] * 4 + [ANY_SPEC],
        scratch_shapes=[
            pltpu.VMEM(full, bf16),
            pltpu.VMEM((chains, length, 4 * block), bf16),
            pltpu.VMEM((n_tp, chains, heads, rows, length), bf16),
            pltpu.VMEM((n_tp, chains, heads, rows, length), bf16),
            pltpu.VMEM(full, bf16),
            pltpu.VMEM((n_tp - 1,) + own, bf16),
            pltpu.VMEM((length // LANES, step_rows * padded, LANES), f32),
            pltpu.VMEM((2, step_rows, length, channels), bf16),
            pltpu.VMEM((2, step_rows, length, channels), bf16),
            pair_sems(chains, n_tp - 1),
            pair_sems(chains, n_tp - 1),
            pair_sems(chains, n_tp - 1),
            pltpu.SemaphoreType.DMA((2,)),
            pltpu.SemaphoreType.DMA((2,)),
        ],
        compiler_params=params(2),
        name="attn_bwd",
    )(
        activations,
        mods,
        grad_att,
        grad_middle,
        rows_full,
        heads_kept,
        gate_sig,
        soft,
        mix,
        gated,
        w_in,
        attn_out,
        pair_w,
        pair_rep,
    )

    slope = lambda s: (s * (1.0 - s))[:, 0, :]
    modulation_part = jnp.concatenate(
        [
            attn_sums[0, :, 0],
            attn_sums[1, :, 0],
            ff_sums[0, :, 0] * slope(sig_attn),
            ff_sums[1, :, 0],
            ff_sums[2, :, 0],
            ff_sums[3, :, 0] * slope(sig_ff),
        ],
        axis=1,
    )
    grad_modulation, pair_weight_sum = (
        lax.psum(modulation_part.astype(bf16), "tp").astype(f32),
        lax.psum(pair_part[:all_heads].astype(bf16), "tp").astype(f32),
    )
    grad_condition = jnp.dot(grad_modulation, ada_full.T, precision=highest)
    place = lax.axis_index("dp")
    sizes = [ada_full.shape[1], condition.shape[1], condition.shape[1], onehot.shape[1]]
    chain_rows = jnp.concatenate([grad_modulation, grad_condition, condition, onehot], axis=1)
    packed = jnp.concatenate([chain_rows.reshape(-1), pair_weight_sum.reshape(-1)])
    packed = jnp.pad(packed, (0, -packed.size % 1024)).reshape(-1, 128)
    gathered = lax.all_gather(packed, "dp", axis=0, tiled=True).reshape(n_dp, -1)
    rows_all = gathered[:, : chain_rows.size].reshape(n_dp * chains, chain_rows.shape[1])
    pair_all = gathered[:, chain_rows.size : chain_rows.size + pair_weight.size].reshape(
        (n_dp,) + pair_weight.shape
    )
    cuts = [sum(sizes[:entry]) for entry in range(5)]
    mod_all, grad_cond_all, cond_all, onehot_all = [
        rows_all[:, cuts[entry] : cuts[entry + 1]] for entry in range(4)
    ]

    def own_columns(values, axis):
        width_here = values.shape[axis] // n_dp
        return lax.dynamic_slice_in_dim(values, place * width_here, width_here, axis)

    grad_ada = jnp.dot(cond_all.T, own_columns(mod_all, 1), precision=highest)
    grad_table = jnp.dot(onehot_all.T, own_columns(grad_cond_all, 1), precision=highest)
    grad_pair_weight = jnp.sum(own_columns(pair_all, 2), axis=0)

    def summed_over_chains(values, collective_id, cuts_here):
        count, _, wide = values.shape
        if n_dp != 8:
            split = values.reshape(count, n_dp, depth // n_dp, wide)
            flat_values = jnp.swapaxes(split, 0, 1).reshape(-1, wide)
            own_part = lax.psum_scatter(flat_values, "dp", scatter_dimension=0, tiled=True)
            return own_part.astype(f32).reshape(count, depth // n_dp, wide)
        own_count = depth // n_dp
        n_y = 2
        n_z = n_dp // n_y
        return pl.pallas_call(
            functools.partial(dp_sum_kernel, (n_z, n_y, cuts_here)),
            out_shape=sds((count, own_count, wide), f32),
            in_specs=[VMEM_SPEC],
            out_specs=VMEM_SPEC,
            scratch_shapes=[
                pltpu.VMEM((n_z, count, own_count, wide), bf16),
                pltpu.VMEM((n_z - 1, count, own_count, wide), bf16),
                pltpu.VMEM((n_z - 1, count, own_count, wide), bf16),
                pair_sems(cuts_here, n_z),
                pair_sems(cuts_here, n_z - 1),
            ],
            compiler_params=params(collective_id),
            name="dp_sum",
        )(values.reshape(count, n_dp, own_count, wide))

    ff_own = summed_over_chains(ff_weights, 3, 6)
    attn_own = summed_over_chains(attn_weights, 4, 3)
    own_in = attn_own[0, :, : 4 * block].reshape(-1, 4, block)
    return (
        result,
        grad_inputs,
        grad_pair,
        jnp.swapaxes(own_in, 0, 1),
        attn_own[0, :, 4 * block : 5 * block].T,
        ff_own[:2],
        ff_own[2].T,
        grad_ada,
        grad_table,
        grad_pair_weight,
    )


def solution(mesh):
    return jax.shard_map(
        local,
        mesh=mesh,
        in_specs=(
            P("dp", "tp", None),
            P("dp", "tp", None, None),
            P("dp"),
            P("dp"),
            P("dp"),
            P(),
            P(),
            P(),
            P(None, None, "tp"),
            P("tp", None),
            P(None, None, "tp"),
            P("tp", None),
            P("dp", "tp", None),
        ),
        out_specs=(
            P("dp", "tp", None),
            P("dp", "tp", None),
            P("dp", "tp", None, None),
            P(None, "dp", "tp"),
            P("tp", "dp"),
            P(None, "dp", "tp"),
            P("tp", "dp"),
            P(None, "dp"),
            P(None, "dp"),
            P(None, "dp"),
        ),
        check_vma=False,
    )
```

```python
import functools
import math

import jax
import jax.numpy as jnp
from jax import lax
from jax.experimental import pallas as pl
from jax.experimental.pallas import tpu as pltpu
from jax.sharding import PartitionSpec as P

highest = lax.Precision.HIGHEST
MESH = pl.DeviceIdType.MESH
f32, bf16 = jnp.float32, jnp.bfloat16
EPS = 1e-05
LANES = 128
NN = (((1,), (0,)), ((), ()))
NT = (((1,), (1,)), ((), ()))
TN = (((0,), (0,)), ((), ()))


def dot(left, right, dims=NN):
    return lax.dot_general(left, right, dims, preferred_element_type=f32)


def time_features(noise_times, cond_width):
    half_width = cond_width // 2
    freq_steps = jnp.arange(half_width).astype(jnp.float32)
    frequency = jnp.exp(freq_steps * (-math.log(10000.0) / half_width))
    angles = 100.0 * noise_times[:, None] * frequency[None, :]
    return jnp.concatenate([jnp.sin(angles), jnp.cos(angles)], axis=1)


def normalize(rows_in):
    centered = rows_in - jnp.mean(rows_in, axis=-1, keepdims=True)
    inverse = lax.rsqrt(jnp.mean(centered * centered, axis=-1, keepdims=True) + EPS)
    return centered * inverse, inverse


def norm_back(grad_rows, normed, inverse):
    mean_grad = jnp.mean(grad_rows, axis=-1, keepdims=True)
    mean_cross = jnp.mean(grad_rows * normed, axis=-1, keepdims=True)
    return inverse * (grad_rows - mean_grad - normed * mean_cross)


def lanes(part):
    return slice(part * LANES, (part + 1) * LANES)


def enter(peers):
    barrier = pltpu.get_barrier_semaphore()
    for peer in peers:
        pl.semaphore_signal(barrier, inc=1, device_id=peer, device_id_type=MESH)
    pl.semaphore_wait(barrier, len(peers))


def send(src, dst, sems, index, peer):
    copy = pltpu.make_async_remote_copy(
        src_ref=src,
        dst_ref=dst,
        send_sem=sems.at[(0,) + index],
        recv_sem=sems.at[(1,) + index],
        device_id=peer,
        device_id_type=MESH,
    )
    copy.start()
    return copy


def own_rows(me, rows):
    return pl.ds(pl.multiple_of(me * rows, rows), rows)


def gather_send(full, chain, me, rows, sems, peers):
    place = full.at[chain, own_rows(me, rows)]
    return [
        send(place, place, sems, (chain, step), peer) for step, (_, peer) in enumerate(peers)
    ]


def scatter_send(terms, landing, chain, rows, sems, peers):
    return [
        send(terms.at[chain, own_rows(index, rows)], landing.at[step, chain], sems, (chain, step), peer)
        for step, (index, peer) in enumerate(peers)
    ]


def scatter_take(terms, landing, chain, me, rows):
    total = terms[chain, own_rows(me, rows)].astype(f32)
    for step in range(landing.shape[0]):
        total = total + landing[step, chain].astype(f32)
    return total


class DpSum:
    def __init__(self, sizes, values, out, stage, sums, landing, first_sems, second_sems):
        self.n_z, self.n_y, self.pieces = sizes
        self.values, self.out, self.stage, self.sums, self.landing = values, out, stage, sums, landing
        self.first_sems, self.second_sems = first_sems, second_sems
        place = lax.axis_index("dp")
        self.z, self.y = place // self.n_y, lax.rem(place, self.n_y)
        self.other = {"dp": place ^ 1}
        self.line = []
        for step in range(1, self.n_z):
            target = lax.rem(self.z + step, self.n_z)
            self.line.append((target, {"dp": target * self.n_y + self.y}))
        self.size = out.shape[1] // self.pieces
        self.first, self.second = {}, {}
        self.todo = [(piece, step) for piece in range(self.pieces) for step in range(self.n_z)]

    def peers(self):
        return [self.other] + [peer for _, peer in self.line]

    def cut(self, piece):
        return pl.ds(piece * self.size, self.size)

    def target(self, step):
        return self.line[step][0] if step < self.n_z - 1 else self.z

    def start(self):
        for piece, step in self.todo:
            self.first[piece, step] = send(
                self.values.at[:, self.target(step) * self.n_y + 1 - self.y, self.cut(piece)],
                self.stage.at[step, :, self.cut(piece)],
                self.first_sems,
                (piece, step),
                self.other,
            )

    def work(self, count):
        for _ in range(min(count, len(self.todo))):
            piece, step = self.todo.pop(0)
            here = self.cut(piece)
            self.first[piece, step].wait_recv()
            kept = self.values[:, self.target(step) * self.n_y + self.y, here].astype(f32)
            total = kept + self.stage[step, :, here].astype(f32)
            if step == self.n_z - 1:
                self.out[:, here] = total
                continue
            self.sums[step, :, here] = total.astype(bf16)
            self.second[piece, step] = send(
                self.sums.at[step, :, here],
                self.landing.at[step, :, here],
                self.second_sems,
                (piece, step),
                self.line[step][1],
            )

    def finish(self):
        self.work(len(self.todo))
        for piece in range(self.pieces):
            here = self.cut(piece)
            total = self.out[:, here]
            for step in range(self.n_z - 1):
                self.second[piece, step].wait_recv()
                total = total + self.landing[step, :, here].astype(f32)
            self.out[:, here] = total
        for copy in list(self.first.values()) + list(self.second.values()):
            copy.wait_send()


def dp_sum_scratch(sizes, count, own_count, wide):
    n_z, _, pieces = sizes
    return [
        pltpu.VMEM((n_z, count, own_count, wide), bf16),
        pltpu.VMEM((n_z - 1, count, own_count, wide), bf16),
        pltpu.VMEM((n_z - 1, count, own_count, wide), bf16),
        pair_sems(pieces, n_z),
        pair_sems(pieces, n_z - 1),
    ]


def dp_others(n_dp):
    place = lax.axis_index("dp")
    return place, [{"dp": lax.rem(place + step, n_dp)} for step in range(1, n_dp)]


def share_over_dp(full, place, others, sems):
    return [
        send(full.at[place], full.at[place], sems, (step,), peer)
        for step, peer in enumerate(others)
    ]


def tp_peers(n_tp):
    me = lax.axis_index("tp")
    return me, [(me ^ step, {"tp": me ^ step}) for step in range(1, n_tp)]


def attn_fwd_kernel(
    sizes,
    inputs,
    mods,
    valid,
    pair_w,
    w_in,
    w_out,
    chain_facts,
    pair_hbm,
    rows_full,
    heads_out,
    gate_out,
    soft_out,
    mix_out,
    gated_out,
    attended_out,
    middle_out,
    facts_all,
    pair_buf,
    stack,
    bias_send,
    bias_full,
    terms,
    landing,
    rows_sems,
    bias_sems,
    terms_sems,
    facts_sems,
    pair_sems,
):
    n_tp, n_dp, heads, width = sizes
    chains, rows, _ = inputs.shape
    length = rows_full.shape[1]
    block = heads * width
    me, peers = tp_peers(n_tp)
    step_rows = pair_buf.shape[1]
    steps = rows // step_rows

    def fetch(turn, slot):
        return pltpu.make_async_copy(
            pair_hbm.at[turn // steps, pl.ds(lax.rem(turn, steps) * step_rows, step_rows)],
            pair_buf.at[slot],
            pair_sems.at[slot],
        )

    fetch(0, 0).start()
    fetch(1, 1).start()
    place_dp, others = dp_others(n_dp)
    enter([peer for _, peer in peers] + others)
    rows_sent = []
    for chain in range(chains):
        normed, _ = normalize(inputs[chain].astype(f32))
        rows_full[chain, own_rows(me, rows)] = (normed * mods[0, chain] + mods[1, chain]).astype(bf16)
        rows_sent.append(gather_send(rows_full, chain, me, rows, rows_sems, peers))

    facts_all[place_dp] = chain_facts[...]
    facts_sent = share_over_dp(facts_all, place_dp, others, facts_sems)

    all_heads = heads * n_tp
    padded = pair_w.shape[0]
    pair_w_here = pair_w[...]
    bias_sent = []
    for chain in range(chains):

        def bias_step(step, carry):
            turn = chain * steps + step
            slot = lax.rem(turn, 2)
            fetch(turn, slot).wait()
            for row in range(step_rows):
                found = dot(pair_w_here, pair_buf[slot, row], NT)
                for part in range(length // LANES):
                    stack[part, row * padded : (row + 1) * padded, :] = found[:, lanes(part)]

            @pl.when(turn + 2 < chains * steps)
            def _():
                fetch(turn + 2, slot).start()

            place = pl.ds(pl.multiple_of(step * step_rows, step_rows), step_rows)
            for head in range(all_heads):
                for part in range(length // LANES):
                    bias_send[head // heads, chain, head % heads, place, lanes(part)] = stack[
                        part, pl.ds(head, step_rows, stride=padded), :
                    ].astype(bf16)
            return carry

        lax.fori_loop(0, steps, bias_step, 0)
        bias_sent.append(
            [
                send(
                    bias_send.at[index, chain],
                    bias_full.at[chain, :, own_rows(me, rows), :],
                    bias_sems,
                    (chain, step),
                    peer,
                )
                for step, (index, peer) in enumerate(peers)
            ]
        )

    for chain in range(chains):
        bias_full[chain, :, own_rows(me, rows), :] = bias_send[me, chain]

    terms_sent = []
    for chain in range(chains):
        for copy in rows_sent[chain]:
            copy.wait_recv()
        projected = dot(rows_full[chain], w_in[...])
        heads_out[chain] = projected.astype(bf16)
        gate_out[chain] = jax.nn.sigmoid(projected[:, 3 * block :])
        for copy in bias_sent[chain]:
            copy.wait_recv()
        mixes = []
        for head in range(heads):
            at = head * width
            query = heads_out[chain, :, at : at + width]
            key_rows = heads_out[chain, :, block + at : block + at + width]
            value_rows = heads_out[chain, :, 2 * block + at : 2 * block + at + width]
            scores = dot(query, key_rows, NT) * width ** (-0.5) + bias_full[chain, head].astype(f32)
            scores = jnp.where(valid[chain] > 0.0, scores, -1e30)
            top = jnp.max(scores, axis=-1, keepdims=True)
            raised = jnp.exp(scores - top)
            soft = raised / jnp.sum(raised, axis=-1, keepdims=True)
            soft_out[chain, head] = soft
            mixes.append(dot(soft.astype(bf16), value_rows))
        mix = jnp.concatenate(mixes, axis=1)
        mix_out[chain] = mix
        gated = (mix * gate_out[chain]).astype(bf16)
        gated_out[chain] = gated
        terms[chain] = dot(gated, w_out[...]).astype(bf16)
        terms_sent.append(scatter_send(terms, landing, chain, rows, terms_sems, peers))

    for chain in range(chains):
        for copy in terms_sent[chain]:
            copy.wait_recv()
        attended = scatter_take(terms, landing, chain, me, rows)
        attended_out[chain] = attended
        middle_out[chain] = inputs[chain].astype(f32) + mods[2, chain] * attended
    for copy in facts_sent:
        copy.wait_recv()
    for group in rows_sent + bias_sent + terms_sent + [facts_sent]:
        for copy in group:
            copy.wait_send()


def ff_kernel(
    sizes,
    middle,
    cotangent,
    attended,
    mods,
    w_in,
    w_out,
    result_out,
    grad_middle_out,
    grad_att_out,
    sums_out,
    weight_out,
    rows_full,
    grad_full,
    gate_keep,
    up_keep,
    hidden_keep,
    grad_gu,
    terms,
    back_terms,
    landing,
    back_landing,
    rows_sems,
    grad_sems,
    terms_sems,
    back_sems,
):
    n_tp, tile = sizes
    chains, rows, depth = middle.shape
    length = rows_full.shape[1]
    hidden_width = w_out.shape[0]
    tiles = hidden_width // tile
    me, peers = tp_peers(n_tp)
    enter([peer for _, peer in peers])
    rows_sent, grad_sent, terms_sent, back_sent = [], [], [], []
    for chain in range(chains):
        normed, _ = normalize(middle[chain])
        rows_full[chain, own_rows(me, rows)] = (normed * mods[3, chain] + mods[4, chain]).astype(bf16)
        rows_sent.append(gather_send(rows_full, chain, me, rows, rows_sems, peers))
    for chain in range(chains):
        grad_full[chain, own_rows(me, rows)] = (mods[5, chain] * cotangent[chain].astype(f32)).astype(bf16)
        grad_sent.append(gather_send(grad_full, chain, me, rows, grad_sems, peers))
    for chain in range(chains):
        for copy in rows_sent[chain]:
            copy.wait_recv()
        for part in range(tiles):
            here = slice(part * tile, (part + 1) * tile)
            gate = dot(rows_full[chain], w_in[0, :, here])
            up = dot(rows_full[chain], w_in[1, :, here])
            gate_keep[chain, :, here] = gate
            up_keep[chain, :, here] = up
            hidden_keep[chain, :, here] = (gate * jax.nn.sigmoid(gate) * up).astype(bf16)
        for part in range(depth // tile):
            here = slice(part * tile, (part + 1) * tile)
            terms[chain, :, here] = dot(hidden_keep[chain], w_out[:, here]).astype(bf16)
        terms_sent.append(scatter_send(terms, landing, chain, rows, terms_sems, peers))
    for chain in range(chains):
        for copy in grad_sent[chain]:
            copy.wait_recv()
        for part in range(tiles):
            here = slice(part * tile, (part + 1) * tile)
            grad_hidden = dot(grad_full[chain], w_out[here, :], NT)
            gate = gate_keep[chain, :, here]
            sig = jax.nn.sigmoid(gate)
            slope = sig * (1.0 + gate * (1.0 - sig))
            grad_gu[0, chain, :, here] = (grad_hidden * up_keep[chain, :, here] * slope).astype(bf16)
            grad_gu[1, chain, :, here] = (grad_hidden * (gate * sig)).astype(bf16)
        for part in range(depth // tile):
            here = slice(part * tile, (part + 1) * tile)
            back_terms[chain, :, here] = (
                dot(grad_gu[0, chain], w_in[0, here, :], NT) + dot(grad_gu[1, chain], w_in[1, here, :], NT)
            ).astype(bf16)
        back_sent.append(scatter_send(back_terms, back_landing, chain, rows, back_sems, peers))

    def flat(ref_value):
        return ref_value.reshape(chains * length, ref_value.shape[-1])

    for part in range(tiles):
        here = slice(part * tile, (part + 1) * tile)
        for which in range(2):
            weight_out[which, :, here] = dot(
                flat(rows_full[...]), flat(grad_gu[which, :, :, here]), TN
            ).astype(bf16)
        weight_out[2, :, here] = dot(
            flat(grad_full[...]), flat(hidden_keep[:, :, here]), TN
        ).astype(bf16)

    for chain in range(chains):
        for copy in terms_sent[chain]:
            copy.wait_recv()
        transition = scatter_take(terms, landing, chain, me, rows)
        upstream = cotangent[chain].astype(f32)
        result_out[chain] = (middle[chain] + mods[5, chain] * transition).astype(bf16)
        sums_out[3, chain] = jnp.sum(upstream * transition, axis=0, keepdims=True)
    for chain in range(chains):
        for copy in back_sent[chain]:
            copy.wait_recv()
        grad_rows = scatter_take(back_terms, back_landing, chain, me, rows)
        normed, inverse = normalize(middle[chain])
        sums_out[1, chain] = jnp.sum(grad_rows * normed, axis=0, keepdims=True)
        sums_out[2, chain] = jnp.sum(grad_rows, axis=0, keepdims=True)
        grad_middle = cotangent[chain].astype(f32) + norm_back(grad_rows * mods[3, chain], normed, inverse)
        grad_middle_out[chain] = grad_middle
        grad_att_out[chain] = (mods[2, chain] * grad_middle).astype(bf16)
        sums_out[0, chain] = jnp.sum(grad_middle * attended[chain], axis=0, keepdims=True)
    for group in rows_sent + grad_sent + terms_sent + back_sent:
        for copy in group:
            copy.wait_send()


def attn_bwd_kernel(
    sizes,
    inputs,
    mods,
    grad_att,
    grad_middle,
    rows_full,
    heads_kept,
    gate_sig,
    soft,
    mix,
    gated,
    w_in,
    w_out,
    ff_values,
    grad_inputs_out,
    sums_out,
    weight_out,
    score_full,
    ff_out,
    grad_full,
    grad_heads,
    score_send,
    terms,
    landing,
    grad_sems,
    score_sems,
    terms_sems,
    *dp_scratch,
):
    n_tp, heads, width, dp_sizes = sizes
    chains, rows, depth = inputs.shape
    length = rows_full.shape[1]
    block = heads * width
    scale = width ** (-0.5)
    me, peers = tp_peers(n_tp)
    ff_sum = DpSum(dp_sizes, ff_values, ff_out, *dp_scratch) if dp_sizes else None
    enter([peer for _, peer in peers] + (ff_sum.peers() if ff_sum else []))

    def work(count):
        if ff_sum:
            ff_sum.work(count)

    grad_sent, score_sent, terms_sent = [], [], []
    for chain in range(chains):
        grad_full[chain, own_rows(me, rows)] = grad_att[chain]
        grad_sent.append(gather_send(grad_full, chain, me, rows, grad_sems, peers))
    if ff_sum:
        ff_sum.start()
    for chain in range(chains):
        for copy in grad_sent[chain]:
            copy.wait_recv()
        work(2)
        grad_gated = dot(grad_full[chain], w_out[...], NT)
        sig = gate_sig[chain]
        grad_mix = (grad_gated * sig).astype(bf16)
        grad_gate = (grad_gated * mix[chain] * sig * (1.0 - sig)).astype(bf16)
        queries, keys, values = [], [], []
        for head in range(heads):
            at = head * width
            query = heads_kept[chain, :, at : at + width]
            key_rows = heads_kept[chain, :, block + at : block + at + width]
            value_rows = heads_kept[chain, :, 2 * block + at : 2 * block + at + width]
            grad_mix_head = grad_mix[:, at : at + width]
            weights = soft[chain, head]
            grad_soft = dot(grad_mix_head, value_rows, NT)
            inner = jnp.sum(grad_soft * weights, axis=-1, keepdims=True)
            grad_scores = (weights * (grad_soft - inner)).astype(bf16)
            for owner in range(n_tp):
                score_send[owner, chain, head] = grad_scores[owner * rows : (owner + 1) * rows, :]
            queries.append((dot(grad_scores, key_rows) * scale).astype(bf16))
            keys.append((dot(grad_scores, query, TN) * scale).astype(bf16))
            values.append(dot(weights.astype(bf16), grad_mix_head, TN).astype(bf16))
        score_sent.append(
            [
                send(
                    score_send.at[index, chain],
                    score_full.at[me, chain],
                    score_sems,
                    (chain, step),
                    peer,
                )
                for step, (index, peer) in enumerate(peers)
            ]
        )
        score_full[me, chain] = score_send[me, chain]
        work(2)
        grad_heads[chain] = jnp.concatenate(queries + keys + values + [grad_gate], axis=1)
        terms[chain] = dot(grad_heads[chain], w_in[...], NT).astype(bf16)
        terms_sent.append(scatter_send(terms, landing, chain, rows, terms_sems, peers))
        work(2)

    def flat(ref_value):
        return ref_value.reshape(chains * length, ref_value.shape[-1])

    weight_out[0, :, : 4 * block] = dot(flat(rows_full[...]), flat(grad_heads[...]), TN).astype(bf16)
    work(2)
    weight_out[0, :, 4 * block : 5 * block] = dot(
        flat(grad_full[...]), flat(gated[...]), TN
    ).astype(bf16)
    weight_out[0, :, 5 * block :] = jnp.zeros((depth, weight_out.shape[2] - 5 * block), bf16)
    work(1)

    for chain in range(chains):
        for copy in terms_sent[chain]:
            copy.wait_recv()
        work(2)
        grad_rows = scatter_take(terms, landing, chain, me, rows)
        normed, inverse = normalize(inputs[chain].astype(f32))
        sums_out[0, chain] = jnp.sum(grad_rows * normed, axis=0, keepdims=True)
        sums_out[1, chain] = jnp.sum(grad_rows, axis=0, keepdims=True)
        grad_inputs_out[chain] = (
            grad_middle[chain] + norm_back(grad_rows * mods[0, chain], normed, inverse)
        ).astype(bf16)

    for chain in range(chains):
        for copy in score_sent[chain]:
            copy.wait_recv()
    if ff_sum:
        ff_sum.finish()
    else:
        ff_out[...] = jnp.zeros_like(ff_out)
    for group in grad_sent + score_sent + terms_sent:
        for copy in group:
            copy.wait_send()


def pair_kernel(
    sizes,
    score_full,
    pair_w,
    pair_hbm,
    pair_w_out,
    grad_pair_hbm,
    stack,
    pair_buf,
    out_buf,
    in_sems,
    out_sems,
):
    n_tp, heads = sizes
    chains, rows, length = score_full.shape[1], score_full.shape[3], score_full.shape[4]
    step_rows = pair_buf.shape[1]
    steps = rows // step_rows
    turns = chains * steps

    def fetch(turn, slot):
        return pltpu.make_async_copy(
            pair_hbm.at[turn // steps, pl.ds(lax.rem(turn, steps) * step_rows, step_rows)],
            pair_buf.at[slot],
            in_sems.at[slot],
        )

    def put(turn, slot):
        return pltpu.make_async_copy(
            out_buf.at[slot],
            grad_pair_hbm.at[turn // steps, pl.ds(lax.rem(turn, steps) * step_rows, step_rows)],
            out_sems.at[slot],
        )

    fetch(0, 0).start()
    fetch(1, 1).start()
    padded = pair_w.shape[0]
    pair_w_here = pair_w[...]
    pair_w_out[...] = jnp.zeros_like(pair_w_out)
    stack[...] = jnp.zeros_like(stack)

    def pair_step(turn, carry):
        slot = lax.rem(turn, 2)
        chain = turn // steps
        fetch(turn, slot).wait()
        place = pl.ds(pl.multiple_of(lax.rem(turn, steps) * step_rows, step_rows), step_rows)
        for head in range(heads * n_tp):
            for part in range(length // LANES):
                stack[part, pl.ds(head, step_rows, stride=padded), :] = score_full[
                    head // heads, chain, head % heads, place, lanes(part)
                ].astype(f32)

        @pl.when(turn >= 2)
        def _():
            put(turn - 2, slot).wait()

        total = jnp.zeros(pair_w_out.shape, f32)
        for row in range(step_rows):
            scores = jnp.concatenate(
                [stack[part, row * padded : (row + 1) * padded, :] for part in range(length // LANES)],
                axis=1,
            ).astype(bf16)
            out_buf[slot, row] = dot(scores, pair_w_here, TN).astype(bf16)
            total = total + dot(scores, pair_buf[slot, row])
        pair_w_out[...] += total

        @pl.when(turn + 2 < turns)
        def _():
            fetch(turn + 2, slot).start()

        put(turn, slot).start()
        return carry

    lax.fori_loop(0, turns, pair_step, 0)
    put(turns - 2, lax.rem(turns - 2, 2)).wait()
    put(turns - 1, lax.rem(turns - 1, 2)).wait()


def tail_kernel(
    sizes,
    attn_sums,
    ff_sums,
    pair_part,
    mods,
    *rest,
):
    n_tp, n_dp, all_heads, dp_sizes = sizes
    if dp_sizes:
        values, totals, own_out, own, arrived, tp_sems, dp_sems, *dp_scratch = rest
        attn_sum = DpSum(dp_sizes, values, own_out, *dp_scratch)
    else:
        totals, own, arrived, tp_sems, dp_sems = rest
        attn_sum = None
    chains, depth = mods.shape[1], mods.shape[3]
    channels = pair_part.shape[1]
    _, peers = tp_peers(n_tp)
    place, others = dp_others(n_dp)
    enter([peer for _, peer in peers] + others)
    if attn_sum:
        attn_sum.start()
    for chain in range(chains):
        sig_attn, sig_ff = mods[2, chain], mods[5, chain]
        entries = [
            attn_sums[0, chain],
            attn_sums[1, chain],
            ff_sums[0, chain] * (sig_attn * (1.0 - sig_attn)),
            ff_sums[1, chain],
            ff_sums[2, chain],
            ff_sums[3, chain] * (sig_ff * (1.0 - sig_ff)),
        ]
        for entry, value in enumerate(entries):
            own[entry * chains + chain : entry * chains + chain + 1, :] = value.astype(bf16)
    per_row = depth // channels
    for head in range(all_heads):
        row = 6 * chains + head // per_row
        at = head % per_row * channels
        own[row : row + 1, at : at + channels] = pair_part[head : head + 1, :].astype(bf16)
    tp_sent = [send(own, arrived.at[step], tp_sems, (step,), peer) for step, (_, peer) in enumerate(peers)]
    for copy in tp_sent:
        copy.wait_recv()
    total = own[...].astype(f32)
    for step in range(n_tp - 1):
        total = total + arrived[step].astype(f32)
    totals[place] = total.astype(bf16)
    dp_sent = share_over_dp(totals, place, others, dp_sems)
    if attn_sum:
        attn_sum.finish()
    for copy in dp_sent:
        copy.wait_recv()
    for copy in tp_sent + dp_sent:
        copy.wait_send()


VMEM_SPEC = pl.BlockSpec(memory_space=pltpu.VMEM)
ANY_SPEC = pl.BlockSpec(memory_space=pl.ANY)


def pair_sems(*shape):
    return pltpu.SemaphoreType.DMA((2,) + shape)


def params(collective_id):
    return pltpu.CompilerParams(
        collective_id=collective_id, has_side_effects=True, vmem_limit_bytes=62 * 1024 * 1024
    )


def local(
    activations,
    pair_rep,
    noise_times,
    class_ids,
    chain_lengths,
    ada_weight,
    class_table,
    pair_weight,
    attn_in,
    attn_out,
    ff_in,
    ff_out,
    cotangent,
):
    n_tp, n_dp = lax.axis_size("tp"), lax.axis_size("dp")
    chains, rows, depth = activations.shape
    length, channels = pair_rep.shape[2:]
    all_heads = pair_weight.shape[0]
    heads = all_heads // n_tp
    block = attn_in.shape[2]
    width = block // heads
    hidden_width = ff_out.shape[0]
    sds = jax.ShapeDtypeStruct

    onehot = (class_ids[:, None] == jnp.arange(class_table.shape[0])[None, :]).astype(f32)
    table_full = class_table.astype(f32)
    ada_full = ada_weight.astype(f32)
    condition = time_features(noise_times, class_table.shape[1]) + jnp.dot(
        onehot, table_full, precision=highest
    )
    modulation = jnp.dot(condition, ada_full, precision=highest)
    pieces = modulation.reshape(chains, 6, 1, depth)
    sig_attn, sig_ff = jax.nn.sigmoid(pieces[:, 2]), jax.nn.sigmoid(pieces[:, 5])
    mods = jnp.stack(
        [1.0 + pieces[:, 0], pieces[:, 1], sig_attn, 1.0 + pieces[:, 3], pieces[:, 4], sig_ff]
    )
    valid = (jnp.arange(length)[None, :] < chain_lengths[:, None]).astype(f32)[:, None, :]
    padded = -(-all_heads // 16) * 16
    pair_w = jnp.pad(pair_weight, ((0, padded - all_heads), (0, 0)))
    w_in = jnp.swapaxes(attn_in, 0, 1).reshape(depth, 4 * block)

    high = condition.astype(bf16)
    low = (condition - high.astype(f32)).astype(bf16)
    classes = onehot.shape[1]
    facts = jnp.concatenate([high, low, onehot.astype(bf16)], axis=1)
    facts = jnp.pad(facts, ((0, -chains % 16), (0, -facts.shape[1] % LANES)))
    direct = n_dp == 8
    dp_grid = (n_dp // 2, 2)
    own_count = depth // n_dp
    step_rows = 16
    full = (chains, length, depth)
    own = (chains, rows, depth)
    rows_full, heads_kept, gate_sig, soft, mix, gated, attended, middle, facts_all = pl.pallas_call(
        functools.partial(attn_fwd_kernel, (n_tp, n_dp, heads, width)),
        out_shape=(
            sds(full, bf16),
            sds((chains, length, 4 * block), bf16),
            sds((chains, length, block), f32),
            sds((chains, heads, length, length), f32),
            sds((chains, length, block), f32),
            sds((chains, length, block), bf16),
            sds(own, f32),
            sds(own, f32),
            sds((n_dp,) + facts.shape, bf16),
        ),
        in_specs=[VMEM_SPEC] * 7 + [ANY_SPEC],
        out_specs=[VMEM_SPEC] * 9,
        scratch_shapes=[
            pltpu.VMEM((2, step_rows, length, channels), bf16),
            pltpu.VMEM((length // LANES, step_rows * padded, LANES), f32),
            pltpu.VMEM((n_tp, chains, heads, rows, length), bf16),
            pltpu.VMEM((chains, heads, length, length), bf16),
            pltpu.VMEM(full, bf16),
            pltpu.VMEM((n_tp - 1,) + own, bf16),
            pair_sems(chains, n_tp - 1),
            pair_sems(chains, n_tp - 1),
            pair_sems(chains, n_tp - 1),
            pair_sems(n_dp - 1),
            pltpu.SemaphoreType.DMA((2,)),
        ],
        compiler_params=params(0),
        name="attn_fwd",
    )(activations, mods, valid, pair_w, w_in, attn_out, facts, pair_rep)

    result, grad_middle, grad_att, ff_sums, ff_weights = pl.pallas_call(
        functools.partial(ff_kernel, (n_tp, 256)),
        out_shape=(
            sds(own, bf16),
            sds(own, f32),
            sds(own, bf16),
            sds((4, chains, 1, depth), f32),
            sds((3, depth, hidden_width), bf16),
        ),
        in_specs=[VMEM_SPEC] * 6,
        out_specs=[VMEM_SPEC] * 5,
        scratch_shapes=[
            pltpu.VMEM(full, bf16),
            pltpu.VMEM(full, bf16),
            pltpu.VMEM((chains, length, hidden_width), f32),
            pltpu.VMEM((chains, length, hidden_width), f32),
            pltpu.VMEM((chains, length, hidden_width), bf16),
            pltpu.VMEM((2, chains, length, hidden_width), bf16),
            pltpu.VMEM(full, bf16),
            pltpu.VMEM(full, bf16),
            pltpu.VMEM((n_tp - 1,) + own, bf16),
            pltpu.VMEM((n_tp - 1,) + own, bf16),
            pair_sems(chains, n_tp - 1),
            pair_sems(chains, n_tp - 1),
            pair_sems(chains, n_tp - 1),
            pair_sems(chains, n_tp - 1),
        ],
        compiler_params=params(1),
        name="ff",
    )(middle, cotangent, attended, mods, ff_in, ff_out)

    wide = -(-5 * block // LANES) * LANES
    ff_sizes = dp_grid + (6,) if direct else None
    ff_values = ff_weights.reshape(3, n_dp, own_count, hidden_width)
    score_shape = (n_tp, chains, heads, rows, length)
    grad_inputs, attn_sums, attn_weights, score_full, ff_own = pl.pallas_call(
        functools.partial(attn_bwd_kernel, (n_tp, heads, width, ff_sizes)),
        out_shape=(
            sds(own, bf16),
            sds((2, chains, 1, depth), f32),
            sds((1, depth, wide), bf16),
            sds(score_shape, bf16),
            sds((3, own_count, hidden_width), f32),
        ),
        in_specs=[VMEM_SPEC] * 13,
        out_specs=[VMEM_SPEC] * 5,
        scratch_shapes=[
            pltpu.VMEM(full, bf16),
            pltpu.VMEM((chains, length, 4 * block), bf16),
            pltpu.VMEM(score_shape, bf16),
            pltpu.VMEM(full, bf16),
            pltpu.VMEM((n_tp - 1,) + own, bf16),
            pair_sems(chains, n_tp - 1),
            pair_sems(chains, n_tp - 1),
            pair_sems(chains, n_tp - 1),
        ]
        + (dp_sum_scratch(ff_sizes, 3, own_count, hidden_width) if direct else []),
        compiler_params=params(2),
        name="attn_bwd",
    )(
        activations,
        mods,
        grad_att,
        grad_middle,
        rows_full,
        heads_kept,
        gate_sig,
        soft,
        mix,
        gated,
        w_in,
        attn_out,
        ff_values,
    )

    pair_part, grad_pair = pl.pallas_call(
        functools.partial(pair_kernel, (n_tp, heads)),
        out_shape=(sds((padded, channels), f32), sds(pair_rep.shape, bf16)),
        in_specs=[VMEM_SPEC] * 2 + [ANY_SPEC],
        out_specs=[VMEM_SPEC, ANY_SPEC],
        scratch_shapes=[
            pltpu.VMEM((length // LANES, step_rows * padded, LANES), f32),
            pltpu.VMEM((2, step_rows, length, channels), bf16),
            pltpu.VMEM((2, step_rows, length, channels), bf16),
            pltpu.SemaphoreType.DMA((2,)),
            pltpu.SemaphoreType.DMA((2,)),
        ],
        compiler_params=pltpu.CompilerParams(vmem_limit_bytes=62 * 1024 * 1024),
        name="pair_grad",
    )(score_full, pair_w, pair_rep)

    attn_sizes = dp_grid + (6,) if direct else None
    total_rows = 6 * chains + all_heads * channels // depth
    tail_in = [attn_sums, ff_sums, pair_part, mods]
    tail_out = [sds((n_dp, total_rows, depth), bf16)]
    tail_scratch = [
        pltpu.VMEM((total_rows, depth), bf16),
        pltpu.VMEM((n_tp - 1, total_rows, depth), bf16),
        pair_sems(n_tp - 1),
        pair_sems(n_dp - 1),
    ]
    if direct:
        tail_in.append(attn_weights.reshape(1, n_dp, own_count, wide))
        tail_out.append(sds((1, own_count, wide), f32))
        tail_scratch += dp_sum_scratch(attn_sizes, 1, own_count, wide)
    totals, *rest = pl.pallas_call(
        functools.partial(tail_kernel, (n_tp, n_dp, all_heads, attn_sizes)),
        out_shape=tuple(tail_out),
        in_specs=[VMEM_SPEC] * len(tail_in),
        out_specs=tuple([VMEM_SPEC] * len(tail_out)),
        scratch_shapes=tail_scratch,
        compiler_params=params(3),
        name="tail",
    )(*tail_in)

    def summed_over_chains(values):
        count, _, here = values.shape
        split = values.reshape(count, n_dp, own_count, here)
        flat_values = jnp.swapaxes(split, 0, 1).reshape(-1, here)
        own_part = lax.psum_scatter(flat_values, "dp", scatter_dimension=0, tiled=True)
        return own_part.astype(f32).reshape(count, own_count, here)

    if direct:
        attn_own = rest[0]
    else:
        ff_own, attn_own = summed_over_chains(ff_weights), summed_over_chains(attn_weights)

    place = lax.axis_index("dp")

    def own_columns(values, axis):
        width_here = values.shape[axis] // n_dp
        return lax.dynamic_slice_in_dim(values, place * width_here, width_here, axis)

    totals = totals.astype(f32)
    mod_all = totals[:, : 6 * chains].reshape(n_dp, 6, chains, depth)
    mod_all = jnp.swapaxes(mod_all, 1, 2).reshape(n_dp * chains, 6 * depth)
    pair_all = totals[:, 6 * chains :].reshape(n_dp, all_heads, channels)
    facts_rows = facts_all[:, :chains].astype(f32).reshape(n_dp * chains, -1)
    cond_wide = condition.shape[1]
    cond_all = facts_rows[:, :cond_wide] + facts_rows[:, cond_wide : 2 * cond_wide]
    onehot_all = facts_rows[:, 2 * cond_wide : 2 * cond_wide + classes]
    grad_ada = jnp.dot(cond_all.T, own_columns(mod_all, 1), precision=highest)
    grad_cond = jnp.dot(mod_all, own_columns(ada_weight, 0).astype(f32).T, precision=highest)
    grad_table = jnp.dot(onehot_all.T, grad_cond, precision=highest)
    grad_pair_weight = jnp.sum(own_columns(pair_all, 2), axis=0)
    own_in = attn_own[0, :, : 4 * block].reshape(-1, 4, block)
    return (
        result,
        grad_inputs,
        grad_pair,
        jnp.swapaxes(own_in, 0, 1),
        attn_own[0, :, 4 * block : 5 * block].T,
        ff_own[:2],
        ff_own[2].T,
        grad_ada,
        grad_table,
        grad_pair_weight,
    )


def solution(mesh):
    return jax.shard_map(
        local,
        mesh=mesh,
        in_specs=(
            P("dp", "tp", None),
            P("dp", "tp", None, None),
            P("dp"),
            P("dp"),
            P("dp"),
            P(),
            P(),
            P(),
            P(None, None, "tp"),
            P("tp", None),
            P(None, None, "tp"),
            P("tp", None),
            P("dp", "tp", None),
        ),
        out_specs=(
            P("dp", "tp", None),
            P("dp", "tp", None),
            P("dp", "tp", None, None),
            P(None, "dp", "tp"),
            P("tp", "dp"),
            P(None, "dp", "tp"),
            P("tp", "dp"),
            P(None, "dp"),
            P(None, "dp"),
            P(None, "dp"),
        ),
        check_vma=False,
    )
```

```python
import functools
import math

import jax
import jax.numpy as jnp
from jax import lax
from jax.experimental import pallas as pl
from jax.experimental.pallas import tpu as pltpu
from jax.sharding import PartitionSpec as P

highest = lax.Precision.HIGHEST
MESH = pl.DeviceIdType.MESH
f32, bf16 = jnp.float32, jnp.bfloat16
EPS = 1e-05
LANES = 128
NN = (((1,), (0,)), ((), ()))
NT = (((1,), (1,)), ((), ()))
TN = (((0,), (0,)), ((), ()))


def dot(left, right, dims=NN):
    return lax.dot_general(left, right, dims, preferred_element_type=f32)


def time_features(noise_times, cond_width):
    half_width = cond_width // 2
    freq_steps = jnp.arange(half_width).astype(jnp.float32)
    frequency = jnp.exp(freq_steps * (-math.log(10000.0) / half_width))
    angles = 100.0 * noise_times[:, None] * frequency[None, :]
    return jnp.concatenate([jnp.sin(angles), jnp.cos(angles)], axis=1)


def normalize(rows_in):
    centered = rows_in - jnp.mean(rows_in, axis=-1, keepdims=True)
    inverse = lax.rsqrt(jnp.mean(centered * centered, axis=-1, keepdims=True) + EPS)
    return centered * inverse, inverse


def norm_back(grad_rows, normed, inverse):
    mean_grad = jnp.mean(grad_rows, axis=-1, keepdims=True)
    mean_cross = jnp.mean(grad_rows * normed, axis=-1, keepdims=True)
    return inverse * (grad_rows - mean_grad - normed * mean_cross)


def lanes(part):
    return slice(part * LANES, (part + 1) * LANES)


def enter(peers):
    barrier = pltpu.get_barrier_semaphore()
    for peer in peers:
        pl.semaphore_signal(barrier, inc=1, device_id=peer, device_id_type=MESH)
    pl.semaphore_wait(barrier, len(peers))


def send(src, dst, sems, index, peer):
    copy = pltpu.make_async_remote_copy(
        src_ref=src,
        dst_ref=dst,
        send_sem=sems.at[(0,) + index],
        recv_sem=sems.at[(1,) + index],
        device_id=peer,
        device_id_type=MESH,
    )
    copy.start()
    return copy


def own_rows(me, rows):
    return pl.ds(pl.multiple_of(me * rows, rows), rows)


class Gather:
    def __init__(self, full, rows, sems):
        self.full, self.rows, self.sems = full, rows, sems
        self.me = lax.axis_index("tp")
        self.cross, self.direct, self.handed = {}, {}, {}

    def place(self, chain, index):
        return self.full.at[chain, own_rows(index, self.rows)]

    def send(self, chain):
        here = self.place(chain, self.me)
        self.cross[chain] = send(here, here, self.sems, (chain, 0), {"tp": self.me ^ 2})
        self.direct[chain] = send(here, here, self.sems, (chain, 1), {"tp": self.me ^ 1})

    def relay(self, chain):
        self.cross[chain].wait_recv()
        here = self.place(chain, self.me ^ 2)
        self.handed[chain] = send(here, here, self.sems, (chain, 2), {"tp": self.me ^ 1})

    def take(self, chain):
        self.direct[chain].wait_recv()
        self.handed[chain].wait_recv()

    def done(self):
        for group in (self.cross, self.direct, self.handed):
            for copy in group.values():
                copy.wait_send()


class Scatter:
    def __init__(self, terms, near, joint, far, rows, sems):
        self.terms, self.near, self.joint, self.far = terms, near, joint, far
        self.rows, self.sems = rows, sems
        self.me = lax.axis_index("tp")
        self.cross, self.direct, self.handed = {}, {}, {}

    def place(self, chain, index):
        return self.terms.at[chain, own_rows(index, self.rows)]

    def send(self, chain):
        other = {"tp": self.me ^ 1}
        self.handed[chain] = send(
            self.place(chain, self.me ^ 3), self.near.at[1, chain], self.sems, (chain, 0), other
        )
        self.direct[chain] = send(
            self.place(chain, self.me ^ 1), self.near.at[0, chain], self.sems, (chain, 1), other
        )

    def relay(self, chain):
        self.handed[chain].wait_recv()
        mine = self.terms[chain, own_rows(self.me ^ 2, self.rows)].astype(f32)
        self.joint[chain] = (mine + self.near[1, chain].astype(f32)).astype(bf16)
        self.cross[chain] = send(
            self.joint.at[chain], self.far.at[chain], self.sems, (chain, 2), {"tp": self.me ^ 2}
        )

    def take(self, chain):
        self.direct[chain].wait_recv()
        self.cross[chain].wait_recv()
        total = self.terms[chain, own_rows(self.me, self.rows)].astype(f32)
        return total + self.near[0, chain].astype(f32) + self.far[chain].astype(f32)

    def done(self):
        for group in (self.cross, self.direct, self.handed):
            for copy in group.values():
                copy.wait_send()


def scatter_scratch(chains, rows, length, depth):
    return [
        pltpu.VMEM((chains, length, depth), bf16),
        pltpu.VMEM((2, chains, rows, depth), bf16),
        pltpu.VMEM((chains, rows, depth), bf16),
        pltpu.VMEM((chains, rows, depth), bf16),
        pair_sems(chains, 3),
    ]


class DpSum:
    def __init__(self, sizes, values, out, stage, sums, landing, first_sems, second_sems):
        self.n_z, self.n_y, self.pieces = sizes
        self.values, self.out, self.stage, self.sums, self.landing = values, out, stage, sums, landing
        self.first_sems, self.second_sems = first_sems, second_sems
        place = lax.axis_index("dp")
        self.z, self.y = place // self.n_y, lax.rem(place, self.n_y)
        self.other = {"dp": place ^ 1}
        self.line = []
        for step in range(1, self.n_z):
            target = lax.rem(self.z + step, self.n_z)
            self.line.append((target, {"dp": target * self.n_y + self.y}))
        self.size = out.shape[1] // self.pieces
        self.first, self.second = {}, {}
        self.todo = [(piece, step) for piece in range(self.pieces) for step in range(self.n_z)]

    def peers(self):
        return [self.other] + [peer for _, peer in self.line]

    def cut(self, piece):
        return pl.ds(piece * self.size, self.size)

    def target(self, step):
        return self.line[step][0] if step < self.n_z - 1 else self.z

    def start(self):
        for piece, step in self.todo:
            self.first[piece, step] = send(
                self.values.at[:, self.target(step) * self.n_y + 1 - self.y, self.cut(piece)],
                self.stage.at[step, :, self.cut(piece)],
                self.first_sems,
                (piece, step),
                self.other,
            )

    def work(self, count):
        for _ in range(min(count, len(self.todo))):
            piece, step = self.todo.pop(0)
            here = self.cut(piece)
            self.first[piece, step].wait_recv()
            kept = self.values[:, self.target(step) * self.n_y + self.y, here].astype(f32)
            total = kept + self.stage[step, :, here].astype(f32)
            if step == self.n_z - 1:
                self.out[:, here] = total
                continue
            self.sums[step, :, here] = total.astype(bf16)
            self.second[piece, step] = send(
                self.sums.at[step, :, here],
                self.landing.at[step, :, here],
                self.second_sems,
                (piece, step),
                self.line[step][1],
            )

    def finish(self):
        self.work(len(self.todo))
        for piece in range(self.pieces):
            here = self.cut(piece)
            total = self.out[:, here]
            for step in range(self.n_z - 1):
                self.second[piece, step].wait_recv()
                total = total + self.landing[step, :, here].astype(f32)
            self.out[:, here] = total
        for copy in list(self.first.values()) + list(self.second.values()):
            copy.wait_send()


def dp_sum_scratch(sizes, count, own_count, wide):
    n_z, _, pieces = sizes
    return [
        pltpu.VMEM((n_z, count, own_count, wide), bf16),
        pltpu.VMEM((n_z - 1, count, own_count, wide), bf16),
        pltpu.VMEM((n_z - 1, count, own_count, wide), bf16),
        pair_sems(pieces, n_z),
        pair_sems(pieces, n_z - 1),
    ]


def dp_others(n_dp):
    place = lax.axis_index("dp")
    return place, [{"dp": lax.rem(place + step, n_dp)} for step in range(1, n_dp)]


def share_over_dp(full, place, others, sems):
    return [
        send(full.at[place], full.at[place], sems, (step,), peer)
        for step, peer in enumerate(others)
    ]


def tp_peers(n_tp):
    me = lax.axis_index("tp")
    return me, [(me ^ step, {"tp": me ^ step}) for step in range(1, n_tp)]


def attn_fwd_kernel(
    sizes,
    inputs,
    mods,
    valid,
    pair_w,
    w_in,
    w_out,
    cotangent,
    pair_hbm,
    rows_full,
    heads_out,
    gate_out,
    soft_out,
    mix_out,
    gated_out,
    attended_out,
    middle_out,
    grad_full,
    pair_buf,
    stack,
    bias_send,
    bias_full,
    rows_sems,
    grad_sems,
    bias_sems,
    pair_sems,
    terms,
    near,
    joint,
    far,
    terms_sems,
):
    n_tp, heads, width = sizes
    chains, rows, _ = inputs.shape
    length = rows_full.shape[1]
    block = heads * width
    me, peers = tp_peers(n_tp)
    step_rows = pair_buf.shape[1]
    steps = rows // step_rows

    def fetch(turn, slot):
        return pltpu.make_async_copy(
            pair_hbm.at[turn // steps, pl.ds(lax.rem(turn, steps) * step_rows, step_rows)],
            pair_buf.at[slot],
            pair_sems.at[slot],
        )

    fetch(0, 0).start()
    fetch(1, 1).start()
    enter([peer for _, peer in peers])
    gather = Gather(rows_full, rows, rows_sems)
    grad_gather = Gather(grad_full, rows, grad_sems)
    scatter = Scatter(terms, near, joint, far, rows, terms_sems)
    for chain in range(chains):
        normed, _ = normalize(inputs[chain].astype(f32))
        rows_full[chain, own_rows(me, rows)] = (normed * mods[0, chain] + mods[1, chain]).astype(bf16)
        gather.send(chain)

    for chain in range(chains):
        grad_full[chain, own_rows(me, rows)] = (mods[5, chain] * cotangent[chain].astype(f32)).astype(bf16)

    all_heads = heads * n_tp
    padded = pair_w.shape[0]
    pair_w_here = pair_w[...]
    bias_sent = []
    for chain in range(chains):

        def bias_step(step, carry):
            turn = chain * steps + step
            slot = lax.rem(turn, 2)
            fetch(turn, slot).wait()
            for row in range(step_rows):
                found = dot(pair_w_here, pair_buf[slot, row], NT)
                for part in range(length // LANES):
                    stack[part, row * padded : (row + 1) * padded, :] = found[:, lanes(part)]

            @pl.when(turn + 2 < chains * steps)
            def _():
                fetch(turn + 2, slot).start()

            place = pl.ds(pl.multiple_of(step * step_rows, step_rows), step_rows)
            for head in range(all_heads):
                for part in range(length // LANES):
                    bias_send[head // heads, chain, head % heads, place, lanes(part)] = stack[
                        part, pl.ds(head, step_rows, stride=padded), :
                    ].astype(bf16)
            return carry

        lax.fori_loop(0, steps, bias_step, 0)
        bias_sent.append(
            [
                send(
                    bias_send.at[index, chain],
                    bias_full.at[chain, :, own_rows(me, rows), :],
                    bias_sems,
                    (chain, step),
                    peer,
                )
                for step, (index, peer) in enumerate(peers)
            ]
        )

        gather.relay(chain)
        bias_full[chain, :, own_rows(me, rows), :] = bias_send[me, chain]

    for chain in range(chains):
        grad_gather.send(chain)
    for chain in range(chains):
        gather.take(chain)
        projected = dot(rows_full[chain], w_in[...])
        heads_out[chain] = projected.astype(bf16)
        gate_out[chain] = jax.nn.sigmoid(projected[:, 3 * block :])
    for chain in range(chains):
        for copy in bias_sent[chain]:
            copy.wait_recv()
        mixes = []
        for head in range(heads):
            at = head * width
            query = heads_out[chain, :, at : at + width]
            key_rows = heads_out[chain, :, block + at : block + at + width]
            value_rows = heads_out[chain, :, 2 * block + at : 2 * block + at + width]
            scores = dot(query, key_rows, NT) * width ** (-0.5) + bias_full[chain, head].astype(f32)
            scores = jnp.where(valid[chain] > 0.0, scores, -1e30)
            top = jnp.max(scores, axis=-1, keepdims=True)
            raised = jnp.exp(scores - top)
            soft = raised / jnp.sum(raised, axis=-1, keepdims=True)
            soft_out[chain, head] = soft
            mixes.append(dot(soft.astype(bf16), value_rows))
        mix = jnp.concatenate(mixes, axis=1)
        mix_out[chain] = mix
        gated = (mix * gate_out[chain]).astype(bf16)
        gated_out[chain] = gated
        terms[chain] = dot(gated, w_out[...]).astype(bf16)
        scatter.send(chain)
        grad_gather.relay(chain)
        if chain > 0:
            scatter.relay(chain - 1)
    scatter.relay(chains - 1)

    for chain in range(chains):
        attended = scatter.take(chain)
        attended_out[chain] = attended
        middle_out[chain] = inputs[chain].astype(f32) + mods[2, chain] * attended
    for chain in range(chains):
        grad_gather.take(chain)
    for part in (gather, grad_gather, scatter):
        part.done()
    for group in bias_sent:
        for copy in group:
            copy.wait_send()


def ff_kernel(
    sizes,
    middle,
    cotangent,
    attended,
    mods,
    grad_full,
    w_in,
    w_out,
    result_out,
    grad_middle_out,
    grad_att_out,
    sums_out,
    weight_out,
    rows_full,
    gate_keep,
    up_keep,
    hidden_keep,
    grad_gu,
    rows_sems,
    *scatter_parts,
):
    n_tp, tile = sizes
    chains, rows, depth = middle.shape
    length = rows_full.shape[1]
    hidden_width = w_out.shape[0]
    tiles = hidden_width // tile
    me, peers = tp_peers(n_tp)
    half = len(scatter_parts) // 2
    enter([peer for _, peer in peers])
    gather = Gather(rows_full, rows, rows_sems)
    forward = Scatter(*scatter_parts[: half - 1], rows, scatter_parts[half - 1])
    backward = Scatter(*scatter_parts[half:-1], rows, scatter_parts[-1])
    terms, back_terms = forward.terms, backward.terms
    for chain in range(chains):
        normed, _ = normalize(middle[chain])
        rows_full[chain, own_rows(me, rows)] = (normed * mods[3, chain] + mods[4, chain]).astype(bf16)
        gather.send(chain)
    gather.relay(0)
    for chain in range(chains):
        gather.take(chain)
        for part in range(tiles):
            here = slice(part * tile, (part + 1) * tile)
            gate = dot(rows_full[chain], w_in[0, :, here])
            up = dot(rows_full[chain], w_in[1, :, here])
            gate_keep[chain, :, here] = gate
            up_keep[chain, :, here] = up
            hidden_keep[chain, :, here] = (gate * jax.nn.sigmoid(gate) * up).astype(bf16)
        if chain + 1 < chains:
            gather.relay(chain + 1)
        if chain > 0:
            backward.relay(chain - 1)
        for part in range(tiles):
            here = slice(part * tile, (part + 1) * tile)
            grad_hidden = dot(grad_full[chain], w_out[here, :], NT)
            gate = gate_keep[chain, :, here]
            sig = jax.nn.sigmoid(gate)
            slope = sig * (1.0 + gate * (1.0 - sig))
            grad_gu[0, chain, :, here] = (grad_hidden * up_keep[chain, :, here] * slope).astype(bf16)
            grad_gu[1, chain, :, here] = (grad_hidden * (gate * sig)).astype(bf16)
        for part in range(depth // tile):
            here = slice(part * tile, (part + 1) * tile)
            back_terms[chain, :, here] = (
                dot(grad_gu[0, chain], w_in[0, here, :], NT) + dot(grad_gu[1, chain], w_in[1, here, :], NT)
            ).astype(bf16)
        backward.send(chain)
    for chain in range(chains):
        for part in range(depth // tile):
            here = slice(part * tile, (part + 1) * tile)
            terms[chain, :, here] = dot(hidden_keep[chain], w_out[:, here]).astype(bf16)
        forward.send(chain)
        if chain == 0:
            backward.relay(chains - 1)

    def flat(ref_value):
        return ref_value.reshape(chains * length, ref_value.shape[-1])

    for part in range(tiles):
        here = slice(part * tile, (part + 1) * tile)
        for which in range(2):
            weight_out[which, :, here] = dot(
                flat(rows_full[...]), flat(grad_gu[which, :, :, here]), TN
            ).astype(bf16)
        weight_out[2, :, here] = dot(
            flat(grad_full[...]), flat(hidden_keep[:, :, here]), TN
        ).astype(bf16)
        if part < chains:
            forward.relay(part)
    for chain in range(tiles, chains):
        forward.relay(chain)

    for chain in range(chains):
        grad_rows = backward.take(chain)
        normed, inverse = normalize(middle[chain])
        sums_out[1, chain] = jnp.sum(grad_rows * normed, axis=0, keepdims=True)
        sums_out[2, chain] = jnp.sum(grad_rows, axis=0, keepdims=True)
        grad_middle = cotangent[chain].astype(f32) + norm_back(grad_rows * mods[3, chain], normed, inverse)
        grad_middle_out[chain] = grad_middle
        grad_att_out[chain] = (mods[2, chain] * grad_middle).astype(bf16)
        sums_out[0, chain] = jnp.sum(grad_middle * attended[chain], axis=0, keepdims=True)
    for chain in range(chains):
        transition = forward.take(chain)
        upstream = cotangent[chain].astype(f32)
        result_out[chain] = (middle[chain] + mods[5, chain] * transition).astype(bf16)
        sums_out[3, chain] = jnp.sum(upstream * transition, axis=0, keepdims=True)
    for part in (gather, forward, backward):
        part.done()


def attn_bwd_kernel(
    sizes,
    inputs,
    mods,
    grad_att,
    grad_middle,
    rows_full,
    heads_kept,
    gate_sig,
    soft,
    mix,
    gated,
    w_in,
    w_out,
    ff_values,
    grad_inputs_out,
    sums_out,
    weight_out,
    score_full,
    ff_out,
    grad_full,
    grad_heads,
    score_send,
    grad_sems,
    score_sems,
    terms,
    near,
    joint,
    far,
    terms_sems,
    *dp_scratch,
):
    n_tp, heads, width, dp_sizes = sizes
    chains, rows, depth = inputs.shape
    length = rows_full.shape[1]
    block = heads * width
    scale = width ** (-0.5)
    me, peers = tp_peers(n_tp)
    ff_sum = DpSum(dp_sizes, ff_values, ff_out, *dp_scratch) if dp_sizes else None
    enter([peer for _, peer in peers] + (ff_sum.peers() if ff_sum else []))

    def work(count):
        if ff_sum:
            ff_sum.work(count)

    score_sent = []
    gather = Gather(grad_full, rows, grad_sems)
    scatter = Scatter(terms, near, joint, far, rows, terms_sems)
    for chain in range(chains):
        grad_full[chain, own_rows(me, rows)] = grad_att[chain]
        gather.send(chain)
    if ff_sum:
        ff_sum.start()
    gather.relay(0)
    for chain in range(chains):
        gather.take(chain)
        work(2)
        grad_gated = dot(grad_full[chain], w_out[...], NT)
        sig = gate_sig[chain]
        grad_mix = (grad_gated * sig).astype(bf16)
        grad_gate = (grad_gated * mix[chain] * sig * (1.0 - sig)).astype(bf16)
        queries, keys, values = [], [], []
        for head in range(heads):
            at = head * width
            query = heads_kept[chain, :, at : at + width]
            key_rows = heads_kept[chain, :, block + at : block + at + width]
            value_rows = heads_kept[chain, :, 2 * block + at : 2 * block + at + width]
            grad_mix_head = grad_mix[:, at : at + width]
            weights = soft[chain, head]
            grad_soft = dot(grad_mix_head, value_rows, NT)
            inner = jnp.sum(grad_soft * weights, axis=-1, keepdims=True)
            grad_scores = (weights * (grad_soft - inner)).astype(bf16)
            for owner in range(n_tp):
                score_send[owner, chain, head] = grad_scores[owner * rows : (owner + 1) * rows, :]
            queries.append((dot(grad_scores, key_rows) * scale).astype(bf16))
            keys.append((dot(grad_scores, query, TN) * scale).astype(bf16))
            values.append(dot(weights.astype(bf16), grad_mix_head, TN).astype(bf16))
            if head == 0 and chain > 0:
                scatter.relay(chain - 1)
        if chain + 1 < chains:
            gather.relay(chain + 1)
        score_sent.append(
            [
                send(
                    score_send.at[index, chain],
                    score_full.at[me, chain],
                    score_sems,
                    (chain, step),
                    peer,
                )
                for step, (index, peer) in enumerate(peers)
            ]
        )
        score_full[me, chain] = score_send[me, chain]
        work(2)
        grad_heads[chain] = jnp.concatenate(queries + keys + values + [grad_gate], axis=1)
        terms[chain] = dot(grad_heads[chain], w_in[...], NT).astype(bf16)
        scatter.send(chain)
        work(2)

    def flat(ref_value):
        return ref_value.reshape(chains * length, ref_value.shape[-1])

    scatter.relay(chains - 1)
    weight_out[0, :, : 4 * block] = dot(flat(rows_full[...]), flat(grad_heads[...]), TN).astype(bf16)
    work(2)
    weight_out[0, :, 4 * block : 5 * block] = dot(
        flat(grad_full[...]), flat(gated[...]), TN
    ).astype(bf16)
    weight_out[0, :, 5 * block :] = jnp.zeros((depth, weight_out.shape[2] - 5 * block), bf16)
    work(1)

    for chain in range(chains):
        grad_rows = scatter.take(chain)
        work(2)
        normed, inverse = normalize(inputs[chain].astype(f32))
        sums_out[0, chain] = jnp.sum(grad_rows * normed, axis=0, keepdims=True)
        sums_out[1, chain] = jnp.sum(grad_rows, axis=0, keepdims=True)
        grad_inputs_out[chain] = (
            grad_middle[chain] + norm_back(grad_rows * mods[0, chain], normed, inverse)
        ).astype(bf16)

    for chain in range(chains):
        for copy in score_sent[chain]:
            copy.wait_recv()
    if ff_sum:
        ff_sum.finish()
    else:
        ff_out[...] = jnp.zeros_like(ff_out)
    gather.done()
    scatter.done()
    for group in score_sent:
        for copy in group:
            copy.wait_send()


def pair_kernel(
    sizes,
    score_full,
    pair_w,
    pair_hbm,
    pair_w_out,
    grad_pair_hbm,
    stack,
    pair_buf,
    out_buf,
    in_sems,
    out_sems,
):
    n_tp, heads = sizes
    chains, rows, length = score_full.shape[1], score_full.shape[3], score_full.shape[4]
    step_rows = pair_buf.shape[1]
    steps = rows // step_rows
    turns = chains * steps

    def fetch(turn, slot):
        return pltpu.make_async_copy(
            pair_hbm.at[turn // steps, pl.ds(lax.rem(turn, steps) * step_rows, step_rows)],
            pair_buf.at[slot],
            in_sems.at[slot],
        )

    def put(turn, slot):
        return pltpu.make_async_copy(
            out_buf.at[slot],
            grad_pair_hbm.at[turn // steps, pl.ds(lax.rem(turn, steps) * step_rows, step_rows)],
            out_sems.at[slot],
        )

    fetch(0, 0).start()
    fetch(1, 1).start()
    padded = pair_w.shape[0]
    pair_w_here = pair_w[...]
    pair_w_out[...] = jnp.zeros_like(pair_w_out)
    stack[...] = jnp.zeros_like(stack)

    def pair_step(turn, carry):
        slot = lax.rem(turn, 2)
        chain = turn // steps
        fetch(turn, slot).wait()
        place = pl.ds(pl.multiple_of(lax.rem(turn, steps) * step_rows, step_rows), step_rows)
        for head in range(heads * n_tp):
            for part in range(length // LANES):
                stack[part, pl.ds(head, step_rows, stride=padded), :] = score_full[
                    head // heads, chain, head % heads, place, lanes(part)
                ].astype(f32)

        @pl.when(turn >= 2)
        def _():
            put(turn - 2, slot).wait()

        total = jnp.zeros(pair_w_out.shape, f32)
        for row in range(step_rows):
            scores = jnp.concatenate(
                [stack[part, row * padded : (row + 1) * padded, :] for part in range(length // LANES)],
                axis=1,
            ).astype(bf16)
            out_buf[slot, row] = dot(scores, pair_w_here, TN).astype(bf16)
            total = total + dot(scores, pair_buf[slot, row])
        pair_w_out[...] += total

        @pl.when(turn + 2 < turns)
        def _():
            fetch(turn + 2, slot).start()

        put(turn, slot).start()
        return carry

    lax.fori_loop(0, turns, pair_step, 0)
    put(turns - 2, lax.rem(turns - 2, 2)).wait()
    put(turns - 1, lax.rem(turns - 1, 2)).wait()


def tail_kernel(
    sizes,
    attn_sums,
    ff_sums,
    pair_part,
    mods,
    chain_facts,
    *rest,
):
    n_tp, n_dp, all_heads, dp_sizes = sizes
    if dp_sizes:
        values, totals, facts_all, own_out, own, arrived, tp_sems, dp_sems, facts_sems, *dp_scratch = rest
        attn_sum = DpSum(dp_sizes, values, own_out, *dp_scratch)
    else:
        totals, facts_all, own, arrived, tp_sems, dp_sems, facts_sems = rest
        attn_sum = None
    chains, depth = mods.shape[1], mods.shape[3]
    channels = pair_part.shape[1]
    _, peers = tp_peers(n_tp)
    place, others = dp_others(n_dp)
    enter([peer for _, peer in peers] + others)
    facts_all[place] = chain_facts[...]
    facts_sent = share_over_dp(facts_all, place, others, facts_sems)
    if attn_sum:
        attn_sum.start()
    for chain in range(chains):
        sig_attn, sig_ff = mods[2, chain], mods[5, chain]
        entries = [
            attn_sums[0, chain],
            attn_sums[1, chain],
            ff_sums[0, chain] * (sig_attn * (1.0 - sig_attn)),
            ff_sums[1, chain],
            ff_sums[2, chain],
            ff_sums[3, chain] * (sig_ff * (1.0 - sig_ff)),
        ]
        for entry, value in enumerate(entries):
            own[entry * chains + chain : entry * chains + chain + 1, :] = value.astype(bf16)
    per_row = depth // channels
    for head in range(all_heads):
        row = 6 * chains + head // per_row
        at = head % per_row * channels
        own[row : row + 1, at : at + channels] = pair_part[head : head + 1, :].astype(bf16)
    tp_sent = [send(own, arrived.at[step], tp_sems, (step,), peer) for step, (_, peer) in enumerate(peers)]
    for copy in tp_sent:
        copy.wait_recv()
    total = own[...].astype(f32)
    for step in range(n_tp - 1):
        total = total + arrived[step].astype(f32)
    totals[place] = total.astype(bf16)
    dp_sent = share_over_dp(totals, place, others, dp_sems)
    if attn_sum:
        attn_sum.finish()
    for copy in dp_sent + facts_sent:
        copy.wait_recv()
    for copy in tp_sent + dp_sent + facts_sent:
        copy.wait_send()


VMEM_SPEC = pl.BlockSpec(memory_space=pltpu.VMEM)
ANY_SPEC = pl.BlockSpec(memory_space=pl.ANY)


def pair_sems(*shape):
    return pltpu.SemaphoreType.DMA((2,) + shape)


def params(collective_id):
    return pltpu.CompilerParams(
        collective_id=collective_id, has_side_effects=True, vmem_limit_bytes=62 * 1024 * 1024
    )


def local(
    activations,
    pair_rep,
    noise_times,
    class_ids,
    chain_lengths,
    ada_weight,
    class_table,
    pair_weight,
    attn_in,
    attn_out,
    ff_in,
    ff_out,
    cotangent,
):
    n_tp, n_dp = lax.axis_size("tp"), lax.axis_size("dp")
    chains, rows, depth = activations.shape
    length, channels = pair_rep.shape[2:]
    all_heads = pair_weight.shape[0]
    heads = all_heads // n_tp
    block = attn_in.shape[2]
    width = block // heads
    hidden_width = ff_out.shape[0]
    sds = jax.ShapeDtypeStruct

    onehot = (class_ids[:, None] == jnp.arange(class_table.shape[0])[None, :]).astype(f32)
    table_full = class_table.astype(f32)
    ada_full = ada_weight.astype(f32)
    condition = time_features(noise_times, class_table.shape[1]) + jnp.dot(
        onehot, table_full, precision=highest
    )
    modulation = jnp.dot(condition, ada_full, precision=highest)
    pieces = modulation.reshape(chains, 6, 1, depth)
    sig_attn, sig_ff = jax.nn.sigmoid(pieces[:, 2]), jax.nn.sigmoid(pieces[:, 5])
    mods = jnp.stack(
        [1.0 + pieces[:, 0], pieces[:, 1], sig_attn, 1.0 + pieces[:, 3], pieces[:, 4], sig_ff]
    )
    valid = (jnp.arange(length)[None, :] < chain_lengths[:, None]).astype(f32)[:, None, :]
    padded = -(-all_heads // 16) * 16
    pair_w = jnp.pad(pair_weight, ((0, padded - all_heads), (0, 0)))
    w_in = jnp.swapaxes(attn_in, 0, 1).reshape(depth, 4 * block)

    classes = onehot.shape[1]
    facts = jnp.concatenate([condition, onehot], axis=1)
    facts = jnp.pad(facts, ((0, 0), (0, -facts.shape[1] % LANES)))
    direct = n_dp == 8
    dp_grid = (n_dp // 2, 2)
    own_count = depth // n_dp
    step_rows = 16
    full = (chains, length, depth)
    own = (chains, rows, depth)
    rows_full, heads_kept, gate_sig, soft, mix, gated, attended, middle, grad_trans_full = pl.pallas_call(
        functools.partial(attn_fwd_kernel, (n_tp, heads, width)),
        out_shape=(
            sds(full, bf16),
            sds((chains, length, 4 * block), bf16),
            sds((chains, length, block), f32),
            sds((chains, heads, length, length), f32),
            sds((chains, length, block), f32),
            sds((chains, length, block), bf16),
            sds(own, f32),
            sds(own, f32),
            sds(full, bf16),
        ),
        in_specs=[VMEM_SPEC] * 7 + [ANY_SPEC],
        out_specs=[VMEM_SPEC] * 9,
        scratch_shapes=[
            pltpu.VMEM((2, step_rows, length, channels), bf16),
            pltpu.VMEM((length // LANES, step_rows * padded, LANES), f32),
            pltpu.VMEM((n_tp, chains, heads, rows, length), bf16),
            pltpu.VMEM((chains, heads, length, length), bf16),
            pair_sems(chains, 3),
            pair_sems(chains, 3),
            pair_sems(chains, n_tp - 1),
            pltpu.SemaphoreType.DMA((2,)),
        ]
        + scatter_scratch(chains, rows, length, depth),
        compiler_params=params(0),
        name="attn_fwd",
    )(activations, mods, valid, pair_w, w_in, attn_out, cotangent, pair_rep)

    result, grad_middle, grad_att, ff_sums, ff_weights = pl.pallas_call(
        functools.partial(ff_kernel, (n_tp, 256)),
        out_shape=(
            sds(own, bf16),
            sds(own, f32),
            sds(own, bf16),
            sds((4, chains, 1, depth), f32),
            sds((3, depth, hidden_width), bf16),
        ),
        in_specs=[VMEM_SPEC] * 7,
        out_specs=[VMEM_SPEC] * 5,
        scratch_shapes=[
            pltpu.VMEM(full, bf16),
            pltpu.VMEM((chains, length, hidden_width), f32),
            pltpu.VMEM((chains, length, hidden_width), f32),
            pltpu.VMEM((chains, length, hidden_width), bf16),
            pltpu.VMEM((2, chains, length, hidden_width), bf16),
            pair_sems(chains, 3),
        ]
        + scatter_scratch(chains, rows, length, depth) * 2,
        compiler_params=params(1),
        name="ff",
    )(middle, cotangent, attended, mods, grad_trans_full, ff_in, ff_out)

    wide = -(-5 * block // LANES) * LANES
    ff_sizes = dp_grid + (6,) if direct else None
    ff_values = ff_weights.reshape(3, n_dp, own_count, hidden_width)
    score_shape = (n_tp, chains, heads, rows, length)
    grad_inputs, attn_sums, attn_weights, score_full, ff_own = pl.pallas_call(
        functools.partial(attn_bwd_kernel, (n_tp, heads, width, ff_sizes)),
        out_shape=(
            sds(own, bf16),
            sds((2, chains, 1, depth), f32),
            sds((1, depth, wide), bf16),
            sds(score_shape, bf16),
            sds((3, own_count, hidden_width), f32),
        ),
        in_specs=[VMEM_SPEC] * 13,
        out_specs=[VMEM_SPEC] * 5,
        scratch_shapes=[
            pltpu.VMEM(full, bf16),
            pltpu.VMEM((chains, length, 4 * block), bf16),
            pltpu.VMEM(score_shape, bf16),
            pair_sems(chains, 3),
            pair_sems(chains, n_tp - 1),
        ]
        + scatter_scratch(chains, rows, length, depth)
        + (dp_sum_scratch(ff_sizes, 3, own_count, hidden_width) if direct else []),
        compiler_params=params(2),
        name="attn_bwd",
    )(
        activations,
        mods,
        grad_att,
        grad_middle,
        rows_full,
        heads_kept,
        gate_sig,
        soft,
        mix,
        gated,
        w_in,
        attn_out,
        ff_values,
    )

    pair_part, grad_pair = pl.pallas_call(
        functools.partial(pair_kernel, (n_tp, heads)),
        out_shape=(sds((padded, channels), f32), sds(pair_rep.shape, bf16)),
        in_specs=[VMEM_SPEC] * 2 + [ANY_SPEC],
        out_specs=[VMEM_SPEC, ANY_SPEC],
        scratch_shapes=[
            pltpu.VMEM((length // LANES, step_rows * padded, LANES), f32),
            pltpu.VMEM((2, step_rows, length, channels), bf16),
            pltpu.VMEM((2, step_rows, length, channels), bf16),
            pltpu.SemaphoreType.DMA((2,)),
            pltpu.SemaphoreType.DMA((2,)),
        ],
        compiler_params=pltpu.CompilerParams(vmem_limit_bytes=62 * 1024 * 1024),
        name="pair_grad",
    )(score_full, pair_w, pair_rep)

    attn_sizes = dp_grid + (6,) if direct else None
    total_rows = 6 * chains + all_heads * channels // depth
    tail_in = [attn_sums, ff_sums, pair_part, mods, facts]
    tail_out = [sds((n_dp, total_rows, depth), bf16), sds((n_dp,) + facts.shape, f32)]
    tail_scratch = [
        pltpu.VMEM((total_rows, depth), bf16),
        pltpu.VMEM((n_tp - 1, total_rows, depth), bf16),
        pair_sems(n_tp - 1),
        pair_sems(n_dp - 1),
        pair_sems(n_dp - 1),
    ]
    if direct:
        tail_in.append(attn_weights.reshape(1, n_dp, own_count, wide))
        tail_out.append(sds((1, own_count, wide), f32))
        tail_scratch += dp_sum_scratch(attn_sizes, 1, own_count, wide)
    totals, facts_all, *rest = pl.pallas_call(
        functools.partial(tail_kernel, (n_tp, n_dp, all_heads, attn_sizes)),
        out_shape=tuple(tail_out),
        in_specs=[VMEM_SPEC] * len(tail_in),
        out_specs=tuple([VMEM_SPEC] * len(tail_out)),
        scratch_shapes=tail_scratch,
        compiler_params=params(3),
        name="tail",
    )(*tail_in)

    def summed_over_chains(values):
        count, _, here = values.shape
        split = values.reshape(count, n_dp, own_count, here)
        flat_values = jnp.swapaxes(split, 0, 1).reshape(-1, here)
        own_part = lax.psum_scatter(flat_values, "dp", scatter_dimension=0, tiled=True)
        return own_part.astype(f32).reshape(count, own_count, here)

    if direct:
        attn_own = rest[0]
    else:
        ff_own, attn_own = summed_over_chains(ff_weights), summed_over_chains(attn_weights)

    place = lax.axis_index("dp")

    def own_columns(values, axis):
        width_here = values.shape[axis] // n_dp
        return lax.dynamic_slice_in_dim(values, place * width_here, width_here, axis)

    totals = totals.astype(f32)
    mod_all = totals[:, : 6 * chains].reshape(n_dp, 6, chains, depth)
    mod_all = jnp.swapaxes(mod_all, 1, 2).reshape(n_dp * chains, 6 * depth)
    pair_all = totals[:, 6 * chains :].reshape(n_dp, all_heads, channels)
    facts_rows = facts_all.reshape(n_dp * chains, -1)
    cond_wide = condition.shape[1]
    cond_all = facts_rows[:, :cond_wide]
    onehot_all = facts_rows[:, cond_wide : cond_wide + classes]
    grad_ada = jnp.dot(cond_all.T, own_columns(mod_all, 1), precision=highest)
    grad_cond = jnp.dot(mod_all, own_columns(ada_weight, 0).astype(f32).T, precision=highest)
    grad_table = jnp.dot(onehot_all.T, grad_cond, precision=highest)
    grad_pair_weight = jnp.sum(own_columns(pair_all, 2), axis=0)
    own_in = attn_own[0, :, : 4 * block].reshape(-1, 4, block)
    return (
        result,
        grad_inputs,
        grad_pair,
        jnp.swapaxes(own_in, 0, 1),
        attn_own[0, :, 4 * block : 5 * block].T,
        ff_own[:2],
        ff_own[2].T,
        grad_ada,
        grad_table,
        grad_pair_weight,
    )


def solution(mesh):
    return jax.shard_map(
        local,
        mesh=mesh,
        in_specs=(
            P("dp", "tp", None),
            P("dp", "tp", None, None),
            P("dp"),
            P("dp"),
            P("dp"),
            P(),
            P(),
            P(),
            P(None, None, "tp"),
            P("tp", None),
            P(None, None, "tp"),
            P("tp", None),
            P("dp", "tp", None),
        ),
        out_specs=(
            P("dp", "tp", None),
            P("dp", "tp", None),
            P("dp", "tp", None, None),
            P(None, "dp", "tp"),
            P("tp", "dp"),
            P(None, "dp", "tp"),
            P("tp", "dp"),
            P(None, "dp"),
            P(None, "dp"),
            P(None, "dp"),
        ),
        check_vma=False,
    )
```

```python
import functools
import math

import jax
import jax.numpy as jnp
from jax import lax
from jax.experimental import pallas as pl
from jax.experimental.pallas import tpu as pltpu
from jax.sharding import PartitionSpec as P

highest = lax.Precision.HIGHEST
MESH = pl.DeviceIdType.MESH
f32, bf16 = jnp.float32, jnp.bfloat16
EPS = 1e-05
LANES = 128
NN = (((1,), (0,)), ((), ()))
NT = (((1,), (1,)), ((), ()))
TN = (((0,), (0,)), ((), ()))


def dot(left, right, dims=NN):
    return lax.dot_general(left, right, dims, preferred_element_type=f32)


def time_features(noise_times, cond_width):
    half_width = cond_width // 2
    freq_steps = jnp.arange(half_width).astype(jnp.float32)
    frequency = jnp.exp(freq_steps * (-math.log(10000.0) / half_width))
    angles = 100.0 * noise_times[:, None] * frequency[None, :]
    return jnp.concatenate([jnp.sin(angles), jnp.cos(angles)], axis=1)


def normalize(rows_in):
    centered = rows_in - jnp.mean(rows_in, axis=-1, keepdims=True)
    inverse = lax.rsqrt(jnp.mean(centered * centered, axis=-1, keepdims=True) + EPS)
    return centered * inverse, inverse


def norm_back(grad_rows, normed, inverse):
    mean_grad = jnp.mean(grad_rows, axis=-1, keepdims=True)
    mean_cross = jnp.mean(grad_rows * normed, axis=-1, keepdims=True)
    return inverse * (grad_rows - mean_grad - normed * mean_cross)


def lanes(part):
    return slice(part * LANES, (part + 1) * LANES)


def enter(peers):
    barrier = pltpu.get_barrier_semaphore()
    for peer in peers:
        pl.semaphore_signal(barrier, inc=1, device_id=peer, device_id_type=MESH)
    pl.semaphore_wait(barrier, len(peers))


def send(src, dst, sems, index, peer):
    copy = pltpu.make_async_remote_copy(
        src_ref=src,
        dst_ref=dst,
        send_sem=sems.at[(0,) + index],
        recv_sem=sems.at[(1,) + index],
        device_id=peer,
        device_id_type=MESH,
    )
    copy.start()
    return copy


def own_rows(me, rows):
    return pl.ds(pl.multiple_of(me * rows, rows), rows)


class Gather:
    def __init__(self, full, rows, sems):
        self.full, self.rows, self.sems = full, rows, sems
        self.me = lax.axis_index("tp")
        self.cross, self.direct, self.handed = {}, {}, {}

    def place(self, chain, index):
        return self.full.at[chain, own_rows(index, self.rows)]

    def send(self, chain):
        here = self.place(chain, self.me)
        self.cross[chain] = send(here, here, self.sems, (chain, 0), {"tp": self.me ^ 2})
        self.direct[chain] = send(here, here, self.sems, (chain, 1), {"tp": self.me ^ 1})

    def relay(self, chain):
        self.cross[chain].wait_recv()
        here = self.place(chain, self.me ^ 2)
        self.handed[chain] = send(here, here, self.sems, (chain, 2), {"tp": self.me ^ 1})

    def take(self, chain):
        self.direct[chain].wait_recv()
        self.handed[chain].wait_recv()

    def done(self):
        for group in (self.cross, self.direct, self.handed):
            for copy in group.values():
                copy.wait_send()


class Scatter:
    def __init__(self, terms, near, joint, far, rows, sems):
        self.terms, self.near, self.joint, self.far = terms, near, joint, far
        self.rows, self.sems = rows, sems
        self.me = lax.axis_index("tp")
        self.cross, self.direct, self.handed = {}, {}, {}

    def place(self, chain, index):
        return self.terms.at[chain, own_rows(index, self.rows)]

    def send(self, chain):
        other = {"tp": self.me ^ 1}
        self.handed[chain] = send(
            self.place(chain, self.me ^ 3), self.near.at[1, chain], self.sems, (chain, 0), other
        )
        self.direct[chain] = send(
            self.place(chain, self.me ^ 1), self.near.at[0, chain], self.sems, (chain, 1), other
        )

    def relay(self, chain):
        self.handed[chain].wait_recv()
        mine = self.terms[chain, own_rows(self.me ^ 2, self.rows)].astype(f32)
        self.joint[chain] = (mine + self.near[1, chain].astype(f32)).astype(bf16)
        self.cross[chain] = send(
            self.joint.at[chain], self.far.at[chain], self.sems, (chain, 2), {"tp": self.me ^ 2}
        )

    def take(self, chain):
        self.direct[chain].wait_recv()
        self.cross[chain].wait_recv()
        total = self.terms[chain, own_rows(self.me, self.rows)].astype(f32)
        return total + self.near[0, chain].astype(f32) + self.far[chain].astype(f32)

    def done(self):
        for group in (self.cross, self.direct, self.handed):
            for copy in group.values():
                copy.wait_send()


def scatter_scratch(chains, rows, length, depth):
    return [
        pltpu.VMEM((chains, length, depth), bf16),
        pltpu.VMEM((2, chains, rows, depth), bf16),
        pltpu.VMEM((chains, rows, depth), bf16),
        pltpu.VMEM((chains, rows, depth), bf16),
        pair_sems(chains, 3),
    ]


class DpSum:
    def __init__(self, sizes, values, out, stage, sums, landing, first_sems, second_sems):
        self.n_z, self.n_y, self.pieces = sizes
        self.values, self.out, self.stage, self.sums, self.landing = values, out, stage, sums, landing
        self.first_sems, self.second_sems = first_sems, second_sems
        place = lax.axis_index("dp")
        self.z, self.y = place // self.n_y, lax.rem(place, self.n_y)
        self.other = {"dp": place ^ 1}
        self.line = []
        for step in range(1, self.n_z):
            target = lax.rem(self.z + step, self.n_z)
            self.line.append((target, {"dp": target * self.n_y + self.y}))
        self.size = out.shape[1] // self.pieces
        self.first, self.second = {}, {}
        self.todo = [(piece, step) for piece in range(self.pieces) for step in range(self.n_z)]

    def peers(self):
        return [self.other] + [peer for _, peer in self.line]

    def cut(self, piece):
        return pl.ds(piece * self.size, self.size)

    def target(self, step):
        return self.line[step][0] if step < self.n_z - 1 else self.z

    def start(self):
        for piece, step in self.todo:
            self.first[piece, step] = send(
                self.values.at[:, self.target(step) * self.n_y + 1 - self.y, self.cut(piece)],
                self.stage.at[step, :, self.cut(piece)],
                self.first_sems,
                (piece, step),
                self.other,
            )

    def work(self, count):
        for _ in range(min(count, len(self.todo))):
            piece, step = self.todo.pop(0)
            here = self.cut(piece)
            self.first[piece, step].wait_recv()
            kept = self.values[:, self.target(step) * self.n_y + self.y, here].astype(f32)
            total = kept + self.stage[step, :, here].astype(f32)
            if step == self.n_z - 1:
                self.out[:, here] = total
                continue
            self.sums[step, :, here] = total.astype(bf16)
            self.second[piece, step] = send(
                self.sums.at[step, :, here],
                self.landing.at[step, :, here],
                self.second_sems,
                (piece, step),
                self.line[step][1],
            )

    def finish(self):
        self.work(len(self.todo))
        for piece in range(self.pieces):
            here = self.cut(piece)
            total = self.out[:, here]
            for step in range(self.n_z - 1):
                self.second[piece, step].wait_recv()
                total = total + self.landing[step, :, here].astype(f32)
            self.out[:, here] = total
        for copy in list(self.first.values()) + list(self.second.values()):
            copy.wait_send()


def dp_sum_scratch(sizes, count, own_count, wide):
    n_z, _, pieces = sizes
    return [
        pltpu.VMEM((n_z, count, own_count, wide), bf16),
        pltpu.VMEM((n_z - 1, count, own_count, wide), bf16),
        pltpu.VMEM((n_z - 1, count, own_count, wide), bf16),
        pair_sems(pieces, n_z),
        pair_sems(pieces, n_z - 1),
    ]


def dp_others(n_dp):
    place = lax.axis_index("dp")
    return place, [{"dp": lax.rem(place + step, n_dp)} for step in range(1, n_dp)]


def share_over_dp(full, place, others, sems):
    return [
        send(full.at[place], full.at[place], sems, (step,), peer)
        for step, peer in enumerate(others)
    ]


def tp_peers(n_tp):
    me = lax.axis_index("tp")
    return me, [(me ^ step, {"tp": me ^ step}) for step in range(1, n_tp)]


def attn_fwd_kernel(
    sizes,
    inputs,
    mods,
    valid,
    pair_w,
    w_in,
    w_out,
    cotangent,
    pair_hbm,
    rows_full,
    heads_out,
    gate_out,
    soft_out,
    mix_out,
    gated_out,
    attended_out,
    middle_out,
    grad_full,
    pair_buf,
    stack,
    bias_send,
    bias_full,
    rows_sems,
    grad_sems,
    bias_sems,
    pair_sems,
    terms,
    near,
    joint,
    far,
    terms_sems,
):
    n_tp, heads, width = sizes
    chains, rows, _ = inputs.shape
    length = rows_full.shape[1]
    block = heads * width
    me, peers = tp_peers(n_tp)
    step_rows = pair_buf.shape[1]
    steps = rows // step_rows

    def fetch(turn, slot):
        return pltpu.make_async_copy(
            pair_hbm.at[turn // steps, pl.ds(lax.rem(turn, steps) * step_rows, step_rows)],
            pair_buf.at[slot],
            pair_sems.at[slot],
        )

    fetch(0, 0).start()
    fetch(1, 1).start()
    enter([peer for _, peer in peers])
    gather = Gather(rows_full, rows, rows_sems)
    grad_gather = Gather(grad_full, rows, grad_sems)
    scatter = Scatter(terms, near, joint, far, rows, terms_sems)
    for chain in range(chains):
        normed, _ = normalize(inputs[chain].astype(f32))
        rows_full[chain, own_rows(me, rows)] = (normed * mods[0, chain] + mods[1, chain]).astype(bf16)
        gather.send(chain)

    for chain in range(chains):
        grad_full[chain, own_rows(me, rows)] = (mods[5, chain] * cotangent[chain].astype(f32)).astype(bf16)

    all_heads = heads * n_tp
    padded = pair_w.shape[0]
    pair_w_here = pair_w[...]
    bias_sent = []
    for chain in range(chains):

        def bias_step(step, carry):
            turn = chain * steps + step
            slot = lax.rem(turn, 2)
            fetch(turn, slot).wait()
            for row in range(step_rows):
                found = dot(pair_w_here, pair_buf[slot, row], NT)
                for part in range(length // LANES):
                    stack[part, row * padded : (row + 1) * padded, :] = found[:, lanes(part)]

            @pl.when(turn + 2 < chains * steps)
            def _():
                fetch(turn + 2, slot).start()

            place = pl.ds(pl.multiple_of(step * step_rows, step_rows), step_rows)
            for head in range(all_heads):
                for part in range(length // LANES):
                    bias_send[head // heads, chain, head % heads, place, lanes(part)] = stack[
                        part, pl.ds(head, step_rows, stride=padded), :
                    ].astype(bf16)
            return carry

        lax.fori_loop(0, steps, bias_step, 0)
        bias_sent.append(
            [
                send(
                    bias_send.at[index, chain],
                    bias_full.at[chain, :, own_rows(me, rows), :],
                    bias_sems,
                    (chain, step),
                    peer,
                )
                for step, (index, peer) in enumerate(peers)
            ]
        )

        gather.relay(chain)
        bias_full[chain, :, own_rows(me, rows), :] = bias_send[me, chain]

    for chain in range(chains):
        grad_gather.send(chain)
    for chain in range(chains):
        gather.take(chain)
        projected = dot(rows_full[chain], w_in[...])
        heads_out[chain] = projected.astype(bf16)
        gate_out[chain] = jax.nn.sigmoid(projected[:, 3 * block :])
    for chain in range(chains):
        for copy in bias_sent[chain]:
            copy.wait_recv()
        mixes = []
        for head in range(heads):
            at = head * width
            query = heads_out[chain, :, at : at + width]
            key_rows = heads_out[chain, :, block + at : block + at + width]
            value_rows = heads_out[chain, :, 2 * block + at : 2 * block + at + width]
            scores = dot(query, key_rows, NT) * width ** (-0.5) + bias_full[chain, head].astype(f32)
            scores = jnp.where(valid[chain] > 0.0, scores, -1e30)
            top = jnp.max(scores, axis=-1, keepdims=True)
            raised = jnp.exp(scores - top)
            soft = raised / jnp.sum(raised, axis=-1, keepdims=True)
            soft_out[chain, head] = soft
            mixes.append(dot(soft.astype(bf16), value_rows))
        mix = jnp.concatenate(mixes, axis=1)
        mix_out[chain] = mix
        gated = (mix * gate_out[chain]).astype(bf16)
        gated_out[chain] = gated
        terms[chain] = dot(gated, w_out[...]).astype(bf16)
        scatter.send(chain)
        grad_gather.relay(chain)
        if chain > 0:
            scatter.relay(chain - 1)
    scatter.relay(chains - 1)

    for chain in range(chains):
        attended = scatter.take(chain)
        attended_out[chain] = attended
        middle_out[chain] = inputs[chain].astype(f32) + mods[2, chain] * attended
    for chain in range(chains):
        grad_gather.take(chain)
    for part in (gather, grad_gather, scatter):
        part.done()
    for group in bias_sent:
        for copy in group:
            copy.wait_send()


def ff_kernel(
    sizes,
    middle,
    cotangent,
    attended,
    mods,
    grad_full,
    w_in,
    w_out,
    result_out,
    grad_middle_out,
    grad_att_out,
    sums_out,
    weight_out,
    rows_full,
    gate_keep,
    up_keep,
    hidden_keep,
    grad_gu,
    rows_sems,
    *scatter_parts,
):
    n_tp, tile = sizes
    chains, rows, depth = middle.shape
    length = rows_full.shape[1]
    hidden_width = w_out.shape[0]
    tiles = hidden_width // tile
    me, peers = tp_peers(n_tp)
    half = len(scatter_parts) // 2
    enter([peer for _, peer in peers])
    gather = Gather(rows_full, rows, rows_sems)
    forward = Scatter(*scatter_parts[: half - 1], rows, scatter_parts[half - 1])
    backward = Scatter(*scatter_parts[half:-1], rows, scatter_parts[-1])
    terms, back_terms = forward.terms, backward.terms
    for chain in range(chains):
        normed, _ = normalize(middle[chain])
        rows_full[chain, own_rows(me, rows)] = (normed * mods[3, chain] + mods[4, chain]).astype(bf16)
        gather.send(chain)
    gather.relay(0)
    for chain in range(chains):
        gather.take(chain)
        for part in range(tiles):
            here = slice(part * tile, (part + 1) * tile)
            gate = dot(rows_full[chain], w_in[0, :, here])
            up = dot(rows_full[chain], w_in[1, :, here])
            gate_keep[chain, :, here] = gate
            up_keep[chain, :, here] = up
            hidden_keep[chain, :, here] = (gate * jax.nn.sigmoid(gate) * up).astype(bf16)
        if chain + 1 < chains:
            gather.relay(chain + 1)
        if chain > 0:
            backward.relay(chain - 1)
        for part in range(tiles):
            here = slice(part * tile, (part + 1) * tile)
            grad_hidden = dot(grad_full[chain], w_out[here, :], NT)
            gate = gate_keep[chain, :, here]
            sig = jax.nn.sigmoid(gate)
            slope = sig * (1.0 + gate * (1.0 - sig))
            grad_gu[0, chain, :, here] = (grad_hidden * up_keep[chain, :, here] * slope).astype(bf16)
            grad_gu[1, chain, :, here] = (grad_hidden * (gate * sig)).astype(bf16)
        for part in range(depth // tile):
            here = slice(part * tile, (part + 1) * tile)
            back_terms[chain, :, here] = (
                dot(grad_gu[0, chain], w_in[0, here, :], NT) + dot(grad_gu[1, chain], w_in[1, here, :], NT)
            ).astype(bf16)
        backward.send(chain)
    for chain in range(chains):
        for part in range(depth // tile):
            here = slice(part * tile, (part + 1) * tile)
            terms[chain, :, here] = dot(hidden_keep[chain], w_out[:, here]).astype(bf16)
        forward.send(chain)
        if chain == 0:
            backward.relay(chains - 1)

    def flat(ref_value):
        return ref_value.reshape(chains * length, ref_value.shape[-1])

    for part in range(tiles):
        here = slice(part * tile, (part + 1) * tile)
        for which in range(2):
            weight_out[which, :, here] = dot(
                flat(rows_full[...]), flat(grad_gu[which, :, :, here]), TN
            ).astype(bf16)
        weight_out[2, :, here] = dot(
            flat(grad_full[...]), flat(hidden_keep[:, :, here]), TN
        ).astype(bf16)
        if part < chains:
            forward.relay(part)
    for chain in range(tiles, chains):
        forward.relay(chain)

    for chain in range(chains):
        grad_rows = backward.take(chain)
        normed, inverse = normalize(middle[chain])
        sums_out[1, chain] = jnp.sum(grad_rows * normed, axis=0, keepdims=True)
        sums_out[2, chain] = jnp.sum(grad_rows, axis=0, keepdims=True)
        grad_middle = cotangent[chain].astype(f32) + norm_back(grad_rows * mods[3, chain], normed, inverse)
        grad_middle_out[chain] = grad_middle
        grad_att_out[chain] = (mods[2, chain] * grad_middle).astype(bf16)
        sums_out[0, chain] = jnp.sum(grad_middle * attended[chain], axis=0, keepdims=True)
    for chain in range(chains):
        transition = forward.take(chain)
        upstream = cotangent[chain].astype(f32)
        result_out[chain] = (middle[chain] + mods[5, chain] * transition).astype(bf16)
        sums_out[3, chain] = jnp.sum(upstream * transition, axis=0, keepdims=True)
    for part in (gather, forward, backward):
        part.done()


def attn_bwd_kernel(
    sizes,
    inputs,
    mods,
    grad_att,
    grad_middle,
    rows_full,
    heads_kept,
    gate_sig,
    soft,
    mix,
    gated,
    w_in,
    w_out,
    ff_values,
    pair_w,
    pair_hbm,
    grad_inputs_out,
    sums_out,
    weight_out,
    score_full,
    ff_out,
    pair_w_out,
    stacked_out,
    grad_full,
    grad_heads,
    score_send,
    grad_sems,
    score_sems,
    terms,
    near,
    joint,
    far,
    terms_sems,
    stack,
    pair_buf,
    in_sems,
    *dp_scratch,
):
    n_tp, heads, width, dp_sizes = sizes
    chains, rows, depth = inputs.shape
    length = rows_full.shape[1]
    block = heads * width
    scale = width ** (-0.5)
    me, peers = tp_peers(n_tp)
    step_rows = pair_buf.shape[1]
    steps = rows // step_rows
    turns = chains * steps

    def fetch(turn):
        return pltpu.make_async_copy(
            pair_hbm.at[turn // steps, pl.ds(turn % steps * step_rows, step_rows)],
            pair_buf.at[turn % 2],
            in_sems.at[turn % 2],
        )

    fetch(0).start()
    fetch(1).start()
    ff_sum = DpSum(dp_sizes, ff_values, ff_out, *dp_scratch) if dp_sizes else None
    enter([peer for _, peer in peers] + (ff_sum.peers() if ff_sum else []))

    def work(count):
        if ff_sum:
            ff_sum.work(count)

    score_sent = []
    gather = Gather(grad_full, rows, grad_sems)
    scatter = Scatter(terms, near, joint, far, rows, terms_sems)
    for chain in range(chains):
        grad_full[chain, own_rows(me, rows)] = grad_att[chain]
        gather.send(chain)
    if ff_sum:
        ff_sum.start()
    gather.relay(0)
    for chain in range(chains):
        gather.take(chain)
        if chain == 0:
            work(2)
        grad_gated = dot(grad_full[chain], w_out[...], NT)
        sig = gate_sig[chain]
        grad_mix = (grad_gated * sig).astype(bf16)
        grad_gate = (grad_gated * mix[chain] * sig * (1.0 - sig)).astype(bf16)
        queries, keys, values = [], [], []
        for head in range(heads):
            at = head * width
            query = heads_kept[chain, :, at : at + width]
            key_rows = heads_kept[chain, :, block + at : block + at + width]
            value_rows = heads_kept[chain, :, 2 * block + at : 2 * block + at + width]
            grad_mix_head = grad_mix[:, at : at + width]
            weights = soft[chain, head]
            grad_soft = dot(grad_mix_head, value_rows, NT)
            inner = jnp.sum(grad_soft * weights, axis=-1, keepdims=True)
            grad_scores = (weights * (grad_soft - inner)).astype(bf16)
            for owner in range(n_tp):
                score_send[owner, chain, head] = grad_scores[owner * rows : (owner + 1) * rows, :]
            queries.append((dot(grad_scores, key_rows) * scale).astype(bf16))
            keys.append((dot(grad_scores, query, TN) * scale).astype(bf16))
            values.append(dot(weights.astype(bf16), grad_mix_head, TN).astype(bf16))
            if head == 0 and chain > 0:
                scatter.relay(chain - 1)
        if chain + 1 < chains:
            gather.relay(chain + 1)
        score_sent.append(
            [
                send(
                    score_send.at[index, chain],
                    score_full.at[me, chain],
                    score_sems,
                    (chain, step),
                    peer,
                )
                for step, (index, peer) in enumerate(peers)
            ]
        )
        score_full[me, chain] = score_send[me, chain]
        work(2)
        grad_heads[chain] = jnp.concatenate(queries + keys + values + [grad_gate], axis=1)
        terms[chain] = dot(grad_heads[chain], w_in[...], NT).astype(bf16)
        scatter.send(chain)
        work(1)

    def flat(ref_value):
        return ref_value.reshape(chains * length, ref_value.shape[-1])

    scatter.relay(chains - 1)
    weight_out[0, :, : 4 * block] = dot(flat(rows_full[...]), flat(grad_heads[...]), TN).astype(bf16)
    work(1)
    weight_out[0, :, 4 * block : 5 * block] = dot(
        flat(grad_full[...]), flat(gated[...]), TN
    ).astype(bf16)
    weight_out[0, :, 5 * block :] = jnp.zeros((depth, weight_out.shape[2] - 5 * block), bf16)
    work(1)

    for chain in range(chains):
        grad_rows = scatter.take(chain)
        work(1)
        normed, inverse = normalize(inputs[chain].astype(f32))
        sums_out[0, chain] = jnp.sum(grad_rows * normed, axis=0, keepdims=True)
        sums_out[1, chain] = jnp.sum(grad_rows, axis=0, keepdims=True)
        grad_inputs_out[chain] = (
            grad_middle[chain] + norm_back(grad_rows * mods[0, chain], normed, inverse)
        ).astype(bf16)

    for chain in range(chains):
        for copy in score_sent[chain]:
            copy.wait_recv()

    padded = pair_w.shape[0]
    pair_w_out[...] = jnp.zeros_like(pair_w_out)
    stack[...] = jnp.zeros_like(stack)
    for turn in range(turns):
        chain, first_row = turn // steps, turn % steps * step_rows
        fetch(turn).wait()
        for head in range(heads * n_tp):
            for part in range(length // LANES):
                stack[part, pl.ds(head, step_rows, stride=padded), :] = score_full[
                    head // heads, chain, head % heads, first_row : first_row + step_rows, lanes(part)
                ].astype(f32)

        def pair_row(row, total):
            at = pl.ds(pl.multiple_of(row * padded, padded), padded)
            scores = jnp.concatenate(
                [stack[part, at, :] for part in range(length // LANES)], axis=1
            ).astype(bf16)
            stacked_out[chain, first_row + row] = scores
            return total + dot(scores, pair_buf[turn % 2, row])

        pair_w_out[...] += lax.fori_loop(
            0, step_rows, pair_row, jnp.zeros(pair_w_out.shape, f32), unroll=True
        )
        if turn + 2 < turns:
            fetch(turn + 2).start()
        work(1)
    if ff_sum:
        ff_sum.finish()
    else:
        ff_out[...] = jnp.zeros_like(ff_out)
    gather.done()
    scatter.done()
    for group in score_sent:
        for copy in group:
            copy.wait_send()


def pair_kernel(stacked, pair_w, grad_pair):
    for row in range(stacked.shape[1]):
        grad_pair[0, row] = dot(stacked[0, row], pair_w[...], TN).astype(bf16)


def tail_kernel(
    sizes,
    attn_sums,
    ff_sums,
    pair_part,
    mods,
    chain_facts,
    *rest,
):
    n_tp, n_dp, all_heads, dp_sizes = sizes
    if dp_sizes:
        values, totals, facts_all, own_out, own, arrived, tp_sems, dp_sems, facts_sems, *dp_scratch = rest
        attn_sum = DpSum(dp_sizes, values, own_out, *dp_scratch)
    else:
        totals, facts_all, own, arrived, tp_sems, dp_sems, facts_sems = rest
        attn_sum = None
    chains, depth = mods.shape[1], mods.shape[3]
    channels = pair_part.shape[1]
    _, peers = tp_peers(n_tp)
    place, others = dp_others(n_dp)
    enter([peer for _, peer in peers] + others)
    facts_all[place] = chain_facts[...]
    facts_sent = share_over_dp(facts_all, place, others, facts_sems)
    if attn_sum:
        attn_sum.start()
    for chain in range(chains):
        sig_attn, sig_ff = mods[2, chain], mods[5, chain]
        entries = [
            attn_sums[0, chain],
            attn_sums[1, chain],
            ff_sums[0, chain] * (sig_attn * (1.0 - sig_attn)),
            ff_sums[1, chain],
            ff_sums[2, chain],
            ff_sums[3, chain] * (sig_ff * (1.0 - sig_ff)),
        ]
        for entry, value in enumerate(entries):
            own[entry * chains + chain : entry * chains + chain + 1, :] = value.astype(bf16)
    per_row = depth // channels
    for head in range(all_heads):
        row = 6 * chains + head // per_row
        at = head % per_row * channels
        own[row : row + 1, at : at + channels] = pair_part[head : head + 1, :].astype(bf16)
    tp_sent = [send(own, arrived.at[step], tp_sems, (step,), peer) for step, (_, peer) in enumerate(peers)]
    for copy in tp_sent:
        copy.wait_recv()
    total = own[...].astype(f32)
    for step in range(n_tp - 1):
        total = total + arrived[step].astype(f32)
    totals[place] = total.astype(bf16)
    dp_sent = share_over_dp(totals, place, others, dp_sems)
    if attn_sum:
        attn_sum.finish()
    for copy in dp_sent + facts_sent:
        copy.wait_recv()
    for copy in tp_sent + dp_sent + facts_sent:
        copy.wait_send()


VMEM_SPEC = pl.BlockSpec(memory_space=pltpu.VMEM)
ANY_SPEC = pl.BlockSpec(memory_space=pl.ANY)


def pair_sems(*shape):
    return pltpu.SemaphoreType.DMA((2,) + shape)


def params(collective_id):
    return pltpu.CompilerParams(
        collective_id=collective_id, has_side_effects=True, vmem_limit_bytes=62 * 1024 * 1024
    )


def local(
    activations,
    pair_rep,
    noise_times,
    class_ids,
    chain_lengths,
    ada_weight,
    class_table,
    pair_weight,
    attn_in,
    attn_out,
    ff_in,
    ff_out,
    cotangent,
):
    n_tp, n_dp = lax.axis_size("tp"), lax.axis_size("dp")
    chains, rows, depth = activations.shape
    length, channels = pair_rep.shape[2:]
    all_heads = pair_weight.shape[0]
    heads = all_heads // n_tp
    block = attn_in.shape[2]
    width = block // heads
    hidden_width = ff_out.shape[0]
    sds = jax.ShapeDtypeStruct

    onehot = (class_ids[:, None] == jnp.arange(class_table.shape[0])[None, :]).astype(f32)
    table_full = class_table.astype(f32)
    ada_full = ada_weight.astype(f32)
    condition = time_features(noise_times, class_table.shape[1]) + jnp.dot(
        onehot, table_full, precision=highest
    )
    modulation = jnp.dot(condition, ada_full, precision=highest)
    pieces = modulation.reshape(chains, 6, 1, depth)
    sig_attn, sig_ff = jax.nn.sigmoid(pieces[:, 2]), jax.nn.sigmoid(pieces[:, 5])
    mods = jnp.stack(
        [1.0 + pieces[:, 0], pieces[:, 1], sig_attn, 1.0 + pieces[:, 3], pieces[:, 4], sig_ff]
    )
    valid = (jnp.arange(length)[None, :] < chain_lengths[:, None]).astype(f32)[:, None, :]
    padded = -(-all_heads // 16) * 16
    pair_w = jnp.pad(pair_weight, ((0, padded - all_heads), (0, 0)))
    w_in = jnp.swapaxes(attn_in, 0, 1).reshape(depth, 4 * block)

    classes = onehot.shape[1]
    facts = jnp.concatenate([condition, onehot], axis=1)
    facts = jnp.pad(facts, ((0, 0), (0, -facts.shape[1] % LANES)))
    direct = n_dp == 8
    dp_grid = (n_dp // 2, 2)
    own_count = depth // n_dp
    step_rows = 16
    full = (chains, length, depth)
    own = (chains, rows, depth)
    rows_full, heads_kept, gate_sig, soft, mix, gated, attended, middle, grad_trans_full = pl.pallas_call(
        functools.partial(attn_fwd_kernel, (n_tp, heads, width)),
        out_shape=(
            sds(full, bf16),
            sds((chains, length, 4 * block), bf16),
            sds((chains, length, block), f32),
            sds((chains, heads, length, length), f32),
            sds((chains, length, block), f32),
            sds((chains, length, block), bf16),
            sds(own, f32),
            sds(own, f32),
            sds(full, bf16),
        ),
        in_specs=[VMEM_SPEC] * 7 + [ANY_SPEC],
        out_specs=[VMEM_SPEC] * 9,
        scratch_shapes=[
            pltpu.VMEM((2, step_rows, length, channels), bf16),
            pltpu.VMEM((length // LANES, step_rows * padded, LANES), f32),
            pltpu.VMEM((n_tp, chains, heads, rows, length), bf16),
            pltpu.VMEM((chains, heads, length, length), bf16),
            pair_sems(chains, 3),
            pair_sems(chains, 3),
            pair_sems(chains, n_tp - 1),
            pltpu.SemaphoreType.DMA((2,)),
        ]
        + scatter_scratch(chains, rows, length, depth),
        compiler_params=params(0),
        name="attn_fwd",
    )(activations, mods, valid, pair_w, w_in, attn_out, cotangent, pair_rep)

    result, grad_middle, grad_att, ff_sums, ff_weights = pl.pallas_call(
        functools.partial(ff_kernel, (n_tp, 256)),
        out_shape=(
            sds(own, bf16),
            sds(own, f32),
            sds(own, bf16),
            sds((4, chains, 1, depth), f32),
            sds((3, depth, hidden_width), bf16),
        ),
        in_specs=[VMEM_SPEC] * 7,
        out_specs=[VMEM_SPEC] * 5,
        scratch_shapes=[
            pltpu.VMEM(full, bf16),
            pltpu.VMEM((chains, length, hidden_width), f32),
            pltpu.VMEM((chains, length, hidden_width), f32),
            pltpu.VMEM((chains, length, hidden_width), bf16),
            pltpu.VMEM((2, chains, length, hidden_width), bf16),
            pair_sems(chains, 3),
        ]
        + scatter_scratch(chains, rows, length, depth) * 2,
        compiler_params=params(1),
        name="ff",
    )(middle, cotangent, attended, mods, grad_trans_full, ff_in, ff_out)

    wide = -(-5 * block // LANES) * LANES
    ff_sizes = dp_grid + (6,) if direct else None
    ff_values = ff_weights.reshape(3, n_dp, own_count, hidden_width)
    score_shape = (n_tp, chains, heads, rows, length)
    grad_inputs, attn_sums, attn_weights, _, ff_own, pair_part, stacked = pl.pallas_call(
        functools.partial(attn_bwd_kernel, (n_tp, heads, width, ff_sizes)),
        out_shape=(
            sds(own, bf16),
            sds((2, chains, 1, depth), f32),
            sds((1, depth, wide), bf16),
            sds(score_shape, bf16),
            sds((3, own_count, hidden_width), f32),
            sds((padded, channels), f32),
            sds((chains, rows, padded, length), bf16),
        ),
        in_specs=[VMEM_SPEC] * 14 + [ANY_SPEC],
        out_specs=[VMEM_SPEC] * 7,
        scratch_shapes=[
            pltpu.VMEM(full, bf16),
            pltpu.VMEM((chains, length, 4 * block), bf16),
            pltpu.VMEM(score_shape, bf16),
            pair_sems(chains, 3),
            pair_sems(chains, n_tp - 1),
        ]
        + scatter_scratch(chains, rows, length, depth)
        + [
            pltpu.VMEM((length // LANES, step_rows * padded, LANES), f32),
            pltpu.VMEM((2, step_rows, length, channels), bf16),
            pltpu.SemaphoreType.DMA((2,)),
        ]
        + (dp_sum_scratch(ff_sizes, 3, own_count, hidden_width) if direct else []),
        compiler_params=params(2),
        name="attn_bwd",
    )(
        activations,
        mods,
        grad_att,
        grad_middle,
        rows_full,
        heads_kept,
        gate_sig,
        soft,
        mix,
        gated,
        w_in,
        attn_out,
        ff_values,
        pair_w,
        pair_rep,
    )

    grad_pair = pl.pallas_call(
        pair_kernel,
        out_shape=sds(pair_rep.shape, bf16),
        grid=(chains, rows // step_rows),
        in_specs=[
            pl.BlockSpec((1, step_rows, padded, length), lambda chain, step: (chain, step, 0, 0)),
            pl.BlockSpec((padded, channels), lambda chain, step: (0, 0)),
        ],
        out_specs=pl.BlockSpec(
            (1, step_rows, length, channels), lambda chain, step: (chain, step, 0, 0)
        ),
        name="pair_grad",
    )(stacked, pair_w)

    attn_sizes = dp_grid + (6,) if direct else None
    total_rows = 6 * chains + all_heads * channels // depth
    tail_in = [attn_sums, ff_sums, pair_part, mods, facts]
    tail_out = [sds((n_dp, total_rows, depth), bf16), sds((n_dp,) + facts.shape, f32)]
    tail_scratch = [
        pltpu.VMEM((total_rows, depth), bf16),
        pltpu.VMEM((n_tp - 1, total_rows, depth), bf16),
        pair_sems(n_tp - 1),
        pair_sems(n_dp - 1),
        pair_sems(n_dp - 1),
    ]
    if direct:
        tail_in.append(attn_weights.reshape(1, n_dp, own_count, wide))
        tail_out.append(sds((1, own_count, wide), f32))
        tail_scratch += dp_sum_scratch(attn_sizes, 1, own_count, wide)
    totals, facts_all, *rest = pl.pallas_call(
        functools.partial(tail_kernel, (n_tp, n_dp, all_heads, attn_sizes)),
        out_shape=tuple(tail_out),
        in_specs=[VMEM_SPEC] * len(tail_in),
        out_specs=tuple([VMEM_SPEC] * len(tail_out)),
        scratch_shapes=tail_scratch,
        compiler_params=params(3),
        name="tail",
    )(*tail_in)

    def summed_over_chains(values):
        count, _, here = values.shape
        split = values.reshape(count, n_dp, own_count, here)
        flat_values = jnp.swapaxes(split, 0, 1).reshape(-1, here)
        own_part = lax.psum_scatter(flat_values, "dp", scatter_dimension=0, tiled=True)
        return own_part.astype(f32).reshape(count, own_count, here)

    if direct:
        attn_own = rest[0]
    else:
        ff_own, attn_own = summed_over_chains(ff_weights), summed_over_chains(attn_weights)

    place = lax.axis_index("dp")

    def own_columns(values, axis):
        width_here = values.shape[axis] // n_dp
        return lax.dynamic_slice_in_dim(values, place * width_here, width_here, axis)

    totals = totals.astype(f32)
    mod_all = totals[:, : 6 * chains].reshape(n_dp, 6, chains, depth)
    mod_all = jnp.swapaxes(mod_all, 1, 2).reshape(n_dp * chains, 6 * depth)
    pair_all = totals[:, 6 * chains :].reshape(n_dp, all_heads, channels)
    facts_rows = facts_all.reshape(n_dp * chains, -1)
    cond_wide = condition.shape[1]
    cond_all = facts_rows[:, :cond_wide]
    onehot_all = facts_rows[:, cond_wide : cond_wide + classes]
    grad_ada = jnp.dot(cond_all.T, own_columns(mod_all, 1), precision=highest)
    grad_cond = jnp.dot(mod_all, own_columns(ada_weight, 0).astype(f32).T, precision=highest)
    grad_table = jnp.dot(onehot_all.T, grad_cond, precision=highest)
    grad_pair_weight = jnp.sum(own_columns(pair_all, 2), axis=0)
    own_in = attn_own[0, :, : 4 * block].reshape(-1, 4, block)
    return (
        result,
        grad_inputs,
        grad_pair,
        jnp.swapaxes(own_in, 0, 1),
        attn_own[0, :, 4 * block : 5 * block].T,
        ff_own[:2],
        ff_own[2].T,
        grad_ada,
        grad_table,
        grad_pair_weight,
    )


def solution(mesh):
    return jax.shard_map(
        local,
        mesh=mesh,
        in_specs=(
            P("dp", "tp", None),
            P("dp", "tp", None, None),
            P("dp"),
            P("dp"),
            P("dp"),
            P(),
            P(),
            P(),
            P(None, None, "tp"),
            P("tp", None),
            P(None, None, "tp"),
            P("tp", None),
            P("dp", "tp", None),
        ),
        out_specs=(
            P("dp", "tp", None),
            P("dp", "tp", None),
            P("dp", "tp", None, None),
            P(None, "dp", "tp"),
            P("tp", "dp"),
            P(None, "dp", "tp"),
            P("tp", "dp"),
            P(None, "dp"),
            P(None, "dp"),
            P(None, "dp"),
        ),
        check_vma=False,
    )
```

```python
import functools
import math

import jax
import jax.numpy as jnp
from jax import lax
from jax.experimental import pallas as pl
from jax.experimental.pallas import tpu as pltpu
from jax.sharding import PartitionSpec as P

highest = lax.Precision.HIGHEST
MESH = pl.DeviceIdType.MESH
f32, bf16 = jnp.float32, jnp.bfloat16
EPS = 1e-05
LANES = 128
NN = (((1,), (0,)), ((), ()))
NT = (((1,), (1,)), ((), ()))
TN = (((0,), (0,)), ((), ()))


def dot(left, right, dims=NN):
    return lax.dot_general(left, right, dims, preferred_element_type=f32)


def time_features(noise_times, cond_width):
    half_width = cond_width // 2
    freq_steps = jnp.arange(half_width).astype(jnp.float32)
    frequency = jnp.exp(freq_steps * (-math.log(10000.0) / half_width))
    angles = 100.0 * noise_times[:, None] * frequency[None, :]
    return jnp.concatenate([jnp.sin(angles), jnp.cos(angles)], axis=1)


def normalize(rows_in):
    centered = rows_in - jnp.mean(rows_in, axis=-1, keepdims=True)
    inverse = lax.rsqrt(jnp.mean(centered * centered, axis=-1, keepdims=True) + EPS)
    return centered * inverse, inverse


def norm_back(grad_rows, normed, inverse):
    mean_grad = jnp.mean(grad_rows, axis=-1, keepdims=True)
    mean_cross = jnp.mean(grad_rows * normed, axis=-1, keepdims=True)
    return inverse * (grad_rows - mean_grad - normed * mean_cross)


def lanes(part):
    return slice(part * LANES, (part + 1) * LANES)


def enter(peers):
    barrier = pltpu.get_barrier_semaphore()
    for peer in peers:
        pl.semaphore_signal(barrier, inc=1, device_id=peer, device_id_type=MESH)
    pl.semaphore_wait(barrier, len(peers))


def send(src, dst, sems, index, peer):
    copy = pltpu.make_async_remote_copy(
        src_ref=src,
        dst_ref=dst,
        send_sem=sems.at[(0,) + index],
        recv_sem=sems.at[(1,) + index],
        device_id=peer,
        device_id_type=MESH,
    )
    copy.start()
    return copy


def own_rows(me, rows):
    return pl.ds(pl.multiple_of(me * rows, rows), rows)


class Gather:
    def __init__(self, full, rows, sems):
        self.full, self.rows, self.sems = full, rows, sems
        self.me = lax.axis_index("tp")
        self.cross, self.direct, self.handed = {}, {}, {}

    def place(self, chain, index):
        return self.full.at[chain, own_rows(index, self.rows)]

    def send(self, chain):
        here = self.place(chain, self.me)
        self.cross[chain] = send(here, here, self.sems, (chain, 0), {"tp": self.me ^ 2})
        self.direct[chain] = send(here, here, self.sems, (chain, 1), {"tp": self.me ^ 1})

    def relay(self, chain):
        self.cross[chain].wait_recv()
        here = self.place(chain, self.me ^ 2)
        self.handed[chain] = send(here, here, self.sems, (chain, 2), {"tp": self.me ^ 1})

    def take(self, chain):
        self.direct[chain].wait_recv()
        self.handed[chain].wait_recv()

    def done(self):
        for group in (self.cross, self.direct, self.handed):
            for copy in group.values():
                copy.wait_send()


class Scatter:
    def __init__(self, terms, near, joint, far, rows, sems):
        self.terms, self.near, self.joint, self.far = terms, near, joint, far
        self.rows, self.sems = rows, sems
        self.me = lax.axis_index("tp")
        self.cross, self.direct, self.handed = {}, {}, {}

    def place(self, chain, index):
        return self.terms.at[chain, own_rows(index, self.rows)]

    def send(self, chain):
        other = {"tp": self.me ^ 1}
        self.handed[chain] = send(
            self.place(chain, self.me ^ 3), self.near.at[1, chain], self.sems, (chain, 0), other
        )
        self.direct[chain] = send(
            self.place(chain, self.me ^ 1), self.near.at[0, chain], self.sems, (chain, 1), other
        )

    def relay(self, chain):
        self.handed[chain].wait_recv()
        mine = self.terms[chain, own_rows(self.me ^ 2, self.rows)].astype(f32)
        self.joint[chain] = (mine + self.near[1, chain].astype(f32)).astype(bf16)
        self.cross[chain] = send(
            self.joint.at[chain], self.far.at[chain], self.sems, (chain, 2), {"tp": self.me ^ 2}
        )

    def take(self, chain):
        self.direct[chain].wait_recv()
        self.cross[chain].wait_recv()
        total = self.terms[chain, own_rows(self.me, self.rows)].astype(f32)
        return total + self.near[0, chain].astype(f32) + self.far[chain].astype(f32)

    def done(self):
        for group in (self.cross, self.direct, self.handed):
            for copy in group.values():
                copy.wait_send()


def scatter_scratch(chains, rows, length, depth):
    return [
        pltpu.VMEM((chains, length, depth), bf16),
        pltpu.VMEM((2, chains, rows, depth), bf16),
        pltpu.VMEM((chains, rows, depth), bf16),
        pltpu.VMEM((chains, rows, depth), bf16),
        pair_sems(chains, 3),
    ]


class DpSum:
    def __init__(self, sizes, values, out, stage, sums, landing, first_sems, second_sems):
        self.n_z, self.n_y, self.pieces = sizes
        self.values, self.out, self.stage, self.sums, self.landing = values, out, stage, sums, landing
        self.first_sems, self.second_sems = first_sems, second_sems
        place = lax.axis_index("dp")
        self.z, self.y = place // self.n_y, lax.rem(place, self.n_y)
        self.other = {"dp": place ^ 1}
        self.line = []
        for step in range(1, self.n_z):
            target = lax.rem(self.z + step, self.n_z)
            self.line.append((target, {"dp": target * self.n_y + self.y}))
        self.size = out.shape[1] // self.pieces
        self.first, self.second = {}, {}
        self.todo = [(piece, step) for piece in range(self.pieces) for step in range(self.n_z)]

    def peers(self):
        return [self.other] + [peer for _, peer in self.line]

    def cut(self, piece):
        return pl.ds(piece * self.size, self.size)

    def target(self, step):
        return self.line[step][0] if step < self.n_z - 1 else self.z

    def start(self):
        for piece, step in self.todo:
            self.first[piece, step] = send(
                self.values.at[:, self.target(step) * self.n_y + 1 - self.y, self.cut(piece)],
                self.stage.at[step, :, self.cut(piece)],
                self.first_sems,
                (piece, step),
                self.other,
            )

    def work(self, count):
        for _ in range(min(count, len(self.todo))):
            piece, step = self.todo.pop(0)
            here = self.cut(piece)
            self.first[piece, step].wait_recv()
            kept = self.values[:, self.target(step) * self.n_y + self.y, here].astype(f32)
            total = kept + self.stage[step, :, here].astype(f32)
            if step == self.n_z - 1:
                self.out[:, here] = total
                continue
            self.sums[step, :, here] = total.astype(bf16)
            self.second[piece, step] = send(
                self.sums.at[step, :, here],
                self.landing.at[step, :, here],
                self.second_sems,
                (piece, step),
                self.line[step][1],
            )

    def finish(self):
        self.work(len(self.todo))
        for piece in range(self.pieces):
            here = self.cut(piece)
            total = self.out[:, here]
            for step in range(self.n_z - 1):
                self.second[piece, step].wait_recv()
                total = total + self.landing[step, :, here].astype(f32)
            self.out[:, here] = total
        for copy in list(self.first.values()) + list(self.second.values()):
            copy.wait_send()


def dp_sum_scratch(sizes, count, own_count, wide):
    n_z, _, pieces = sizes
    return [
        pltpu.VMEM((n_z, count, own_count, wide), bf16),
        pltpu.VMEM((n_z - 1, count, own_count, wide), bf16),
        pltpu.VMEM((n_z - 1, count, own_count, wide), bf16),
        pair_sems(pieces, n_z),
        pair_sems(pieces, n_z - 1),
    ]


def dp_others(n_dp):
    place = lax.axis_index("dp")
    return place, [{"dp": lax.rem(place + step, n_dp)} for step in range(1, n_dp)]


def share_over_dp(full, place, others, sems):
    return [
        send(full.at[place], full.at[place], sems, (step,), peer)
        for step, peer in enumerate(others)
    ]


def tp_peers(n_tp):
    me = lax.axis_index("tp")
    return me, [(me ^ step, {"tp": me ^ step}) for step in range(1, n_tp)]


def attn_fwd_kernel(
    sizes,
    inputs,
    mods,
    valid,
    pair_w,
    w_in,
    w_out,
    cotangent,
    pair_hbm,
    rows_full,
    heads_out,
    gate_out,
    soft_out,
    mix_out,
    gated_out,
    attended_out,
    middle_out,
    grad_full,
    pair_buf,
    stack,
    bias_send,
    bias_full,
    rows_sems,
    grad_sems,
    bias_sems,
    pair_sems,
    terms,
    near,
    joint,
    far,
    terms_sems,
):
    n_tp, heads, width = sizes
    chains, rows, _ = inputs.shape
    length = rows_full.shape[1]
    block = heads * width
    me, peers = tp_peers(n_tp)
    step_rows = pair_buf.shape[1]
    steps = rows // step_rows

    def fetch(turn, slot):
        return pltpu.make_async_copy(
            pair_hbm.at[turn // steps, pl.ds(lax.rem(turn, steps) * step_rows, step_rows)],
            pair_buf.at[slot],
            pair_sems.at[slot],
        )

    fetch(0, 0).start()
    fetch(1, 1).start()
    enter([peer for _, peer in peers])
    gather = Gather(rows_full, rows, rows_sems)
    grad_gather = Gather(grad_full, rows, grad_sems)
    scatter = Scatter(terms, near, joint, far, rows, terms_sems)
    for chain in range(chains):
        normed, _ = normalize(inputs[chain].astype(f32))
        rows_full[chain, own_rows(me, rows)] = (normed * mods[0, chain] + mods[1, chain]).astype(bf16)
        gather.send(chain)

    for chain in range(chains):
        grad_full[chain, own_rows(me, rows)] = (mods[5, chain] * cotangent[chain].astype(f32)).astype(bf16)

    all_heads = heads * n_tp
    padded = pair_w.shape[0]
    pair_w_here = pair_w[...]
    bias_sent = []
    for chain in range(chains):

        def bias_step(step, carry):
            turn = chain * steps + step
            slot = lax.rem(turn, 2)
            fetch(turn, slot).wait()
            for row in range(step_rows):
                found = dot(pair_w_here, pair_buf[slot, row], NT)
                for part in range(length // LANES):
                    stack[part, row * padded : (row + 1) * padded, :] = found[:, lanes(part)]

            @pl.when(turn + 2 < chains * steps)
            def _():
                fetch(turn + 2, slot).start()

            place = pl.ds(pl.multiple_of(step * step_rows, step_rows), step_rows)
            for head in range(all_heads):
                for part in range(length // LANES):
                    bias_send[head // heads, chain, head % heads, place, lanes(part)] = stack[
                        part, pl.ds(head, step_rows, stride=padded), :
                    ].astype(bf16)
            return carry

        lax.fori_loop(0, steps, bias_step, 0)
        bias_sent.append(
            [
                send(
                    bias_send.at[index, chain],
                    bias_full.at[chain, :, own_rows(me, rows), :],
                    bias_sems,
                    (chain, step),
                    peer,
                )
                for step, (index, peer) in enumerate(peers)
            ]
        )

        gather.relay(chain)
        bias_full[chain, :, own_rows(me, rows), :] = bias_send[me, chain]

    for chain in range(chains):
        grad_gather.send(chain)
    for chain in range(chains):
        gather.take(chain)
        projected = dot(rows_full[chain], w_in[...])
        heads_out[chain] = projected.astype(bf16)
        gate_out[chain] = jax.nn.sigmoid(projected[:, 3 * block :])
    for chain in range(chains):
        for copy in bias_sent[chain]:
            copy.wait_recv()
        mixes = []
        for head in range(heads):
            at = head * width
            query = heads_out[chain, :, at : at + width]
            key_rows = heads_out[chain, :, block + at : block + at + width]
            value_rows = heads_out[chain, :, 2 * block + at : 2 * block + at + width]
            scores = dot(query, key_rows, NT) * width ** (-0.5) + bias_full[chain, head].astype(f32)
            scores = jnp.where(valid[chain] > 0.0, scores, -1e30)
            top = jnp.max(scores, axis=-1, keepdims=True)
            raised = jnp.exp(scores - top)
            soft = raised / jnp.sum(raised, axis=-1, keepdims=True)
            soft_out[chain, head] = soft
            mixes.append(dot(soft.astype(bf16), value_rows))
        mix = jnp.concatenate(mixes, axis=1)
        mix_out[chain] = mix
        gated = (mix * gate_out[chain]).astype(bf16)
        gated_out[chain] = gated
        terms[chain] = dot(gated, w_out[...]).astype(bf16)
        scatter.send(chain)
        grad_gather.relay(chain)
        if chain > 0:
            scatter.relay(chain - 1)
    scatter.relay(chains - 1)

    for chain in range(chains):
        attended = scatter.take(chain)
        attended_out[chain] = attended
        middle_out[chain] = inputs[chain].astype(f32) + mods[2, chain] * attended
    for chain in range(chains):
        grad_gather.take(chain)
    for part in (gather, grad_gather, scatter):
        part.done()
    for group in bias_sent:
        for copy in group:
            copy.wait_send()


def ff_kernel(
    sizes,
    middle,
    cotangent,
    attended,
    mods,
    grad_full,
    w_in,
    w_out,
    result_out,
    grad_middle_out,
    grad_att_out,
    sums_out,
    weight_out,
    rows_full,
    gate_keep,
    up_keep,
    hidden_keep,
    grad_gu,
    rows_sems,
    *scatter_parts,
):
    n_tp, tile = sizes
    chains, rows, depth = middle.shape
    length = rows_full.shape[1]
    hidden_width = w_out.shape[0]
    tiles = hidden_width // tile
    me, peers = tp_peers(n_tp)
    half = len(scatter_parts) // 2
    enter([peer for _, peer in peers])
    gather = Gather(rows_full, rows, rows_sems)
    forward = Scatter(*scatter_parts[: half - 1], rows, scatter_parts[half - 1])
    backward = Scatter(*scatter_parts[half:-1], rows, scatter_parts[-1])
    terms, back_terms = forward.terms, backward.terms
    for chain in range(chains):
        normed, _ = normalize(middle[chain])
        rows_full[chain, own_rows(me, rows)] = (normed * mods[3, chain] + mods[4, chain]).astype(bf16)
        gather.send(chain)
    gather.relay(0)
    for chain in range(chains):
        gather.take(chain)
        for part in range(tiles):
            here = slice(part * tile, (part + 1) * tile)
            gate = dot(rows_full[chain], w_in[0, :, here])
            up = dot(rows_full[chain], w_in[1, :, here])
            gate_keep[chain, :, here] = gate
            up_keep[chain, :, here] = up
            hidden_keep[chain, :, here] = (gate * jax.nn.sigmoid(gate) * up).astype(bf16)
        if chain + 1 < chains:
            gather.relay(chain + 1)
        if chain > 0:
            backward.relay(chain - 1)
        for part in range(tiles):
            here = slice(part * tile, (part + 1) * tile)
            grad_hidden = dot(grad_full[chain], w_out[here, :], NT)
            gate = gate_keep[chain, :, here]
            sig = jax.nn.sigmoid(gate)
            slope = sig * (1.0 + gate * (1.0 - sig))
            grad_gu[0, chain, :, here] = (grad_hidden * up_keep[chain, :, here] * slope).astype(bf16)
            grad_gu[1, chain, :, here] = (grad_hidden * (gate * sig)).astype(bf16)
        for part in range(depth // tile):
            here = slice(part * tile, (part + 1) * tile)
            back_terms[chain, :, here] = (
                dot(grad_gu[0, chain], w_in[0, here, :], NT) + dot(grad_gu[1, chain], w_in[1, here, :], NT)
            ).astype(bf16)
        backward.send(chain)
    for chain in range(chains):
        for part in range(depth // tile):
            here = slice(part * tile, (part + 1) * tile)
            terms[chain, :, here] = dot(hidden_keep[chain], w_out[:, here]).astype(bf16)
        forward.send(chain)
        if chain == 0:
            backward.relay(chains - 1)

    def flat(ref_value):
        return ref_value.reshape(chains * length, ref_value.shape[-1])

    for part in range(tiles):
        here = slice(part * tile, (part + 1) * tile)
        for which in range(2):
            weight_out[which, :, here] = dot(
                flat(rows_full[...]), flat(grad_gu[which, :, :, here]), TN
            ).astype(bf16)
        weight_out[2, :, here] = dot(
            flat(grad_full[...]), flat(hidden_keep[:, :, here]), TN
        ).astype(bf16)
        if part < chains:
            forward.relay(part)
    for chain in range(tiles, chains):
        forward.relay(chain)

    for chain in range(chains):
        grad_rows = backward.take(chain)
        normed, inverse = normalize(middle[chain])
        sums_out[1, chain] = jnp.sum(grad_rows * normed, axis=0, keepdims=True)
        sums_out[2, chain] = jnp.sum(grad_rows, axis=0, keepdims=True)
        grad_middle = cotangent[chain].astype(f32) + norm_back(grad_rows * mods[3, chain], normed, inverse)
        grad_middle_out[chain] = grad_middle
        grad_att_out[chain] = (mods[2, chain] * grad_middle).astype(bf16)
        sums_out[0, chain] = jnp.sum(grad_middle * attended[chain], axis=0, keepdims=True)
    for chain in range(chains):
        transition = forward.take(chain)
        upstream = cotangent[chain].astype(f32)
        result_out[chain] = (middle[chain] + mods[5, chain] * transition).astype(bf16)
        sums_out[3, chain] = jnp.sum(upstream * transition, axis=0, keepdims=True)
    for part in (gather, forward, backward):
        part.done()


def attn_bwd_kernel(
    sizes,
    inputs,
    mods,
    grad_att,
    grad_middle,
    rows_full,
    heads_kept,
    gate_sig,
    soft,
    mix,
    gated,
    w_in,
    w_out,
    ff_values,
    pair_w,
    pair_hbm,
    grad_inputs_out,
    sums_out,
    weight_out,
    score_full,
    ff_out,
    pair_w_out,
    stacked_out,
    grad_full,
    grad_heads,
    score_send,
    grad_sems,
    score_sems,
    terms,
    near,
    joint,
    far,
    terms_sems,
    stack,
    pair_buf,
    in_sems,
    *dp_scratch,
):
    n_tp, heads, width, dp_sizes = sizes
    chains, rows, depth = inputs.shape
    length = rows_full.shape[1]
    block = heads * width
    scale = width ** (-0.5)
    me, peers = tp_peers(n_tp)
    step_rows = pair_buf.shape[1]
    steps = rows // step_rows
    turns = chains * steps

    def fetch(turn):
        return pltpu.make_async_copy(
            pair_hbm.at[turn // steps, pl.ds(turn % steps * step_rows, step_rows)],
            pair_buf.at[turn % 2],
            in_sems.at[turn % 2],
        )

    fetch(0).start()
    fetch(1).start()
    ff_sum = DpSum(dp_sizes, ff_values, ff_out, *dp_scratch) if dp_sizes else None
    enter([peer for _, peer in peers] + (ff_sum.peers() if ff_sum else []))

    def work(count):
        if ff_sum:
            ff_sum.work(count)

    score_sent = []
    gather = Gather(grad_full, rows, grad_sems)
    scatter = Scatter(terms, near, joint, far, rows, terms_sems)
    for chain in range(chains):
        grad_full[chain, own_rows(me, rows)] = grad_att[chain]
        gather.send(chain)
    if ff_sum:
        ff_sum.start()
    gather.relay(0)
    for chain in range(chains):
        gather.take(chain)
        if chain == 0:
            work(2)
        grad_gated = dot(grad_full[chain], w_out[...], NT)
        sig = gate_sig[chain]
        grad_mix = (grad_gated * sig).astype(bf16)
        grad_gate = (grad_gated * mix[chain] * sig * (1.0 - sig)).astype(bf16)
        queries, keys, values = [], [], []
        for head in range(heads):
            at = head * width
            query = heads_kept[chain, :, at : at + width]
            key_rows = heads_kept[chain, :, block + at : block + at + width]
            value_rows = heads_kept[chain, :, 2 * block + at : 2 * block + at + width]
            grad_mix_head = grad_mix[:, at : at + width]
            weights = soft[chain, head]
            grad_soft = dot(grad_mix_head, value_rows, NT)
            inner = jnp.sum(grad_soft * weights, axis=-1, keepdims=True)
            grad_scores = (weights * (grad_soft - inner)).astype(bf16)
            for owner in range(n_tp):
                score_send[owner, chain, head] = grad_scores[owner * rows : (owner + 1) * rows, :]
            queries.append((dot(grad_scores, key_rows) * scale).astype(bf16))
            keys.append((dot(grad_scores, query, TN) * scale).astype(bf16))
            values.append(dot(weights.astype(bf16), grad_mix_head, TN).astype(bf16))
            if head == 0 and chain > 0:
                scatter.relay(chain - 1)
        if chain + 1 < chains:
            gather.relay(chain + 1)
        score_sent.append(
            [
                send(
                    score_send.at[index, chain],
                    score_full.at[me, chain],
                    score_sems,
                    (chain, step),
                    peer,
                )
                for step, (index, peer) in enumerate(peers)
            ]
        )
        score_full[me, chain] = score_send[me, chain]
        work(2)
        grad_heads[chain] = jnp.concatenate(queries + keys + values + [grad_gate], axis=1)
        terms[chain] = dot(grad_heads[chain], w_in[...], NT).astype(bf16)
        scatter.send(chain)
        work(1)

    def flat(ref_value):
        return ref_value.reshape(chains * length, ref_value.shape[-1])

    scatter.relay(chains - 1)
    weight_out[0, :, : 4 * block] = dot(flat(rows_full[...]), flat(grad_heads[...]), TN).astype(bf16)
    work(1)
    weight_out[0, :, 4 * block : 5 * block] = dot(
        flat(grad_full[...]), flat(gated[...]), TN
    ).astype(bf16)
    weight_out[0, :, 5 * block :] = jnp.zeros((depth, weight_out.shape[2] - 5 * block), bf16)
    work(1)

    for chain in range(chains):
        grad_rows = scatter.take(chain)
        work(1)
        normed, inverse = normalize(inputs[chain].astype(f32))
        sums_out[0, chain] = jnp.sum(grad_rows * normed, axis=0, keepdims=True)
        sums_out[1, chain] = jnp.sum(grad_rows, axis=0, keepdims=True)
        grad_inputs_out[chain] = (
            grad_middle[chain] + norm_back(grad_rows * mods[0, chain], normed, inverse)
        ).astype(bf16)

    for chain in range(chains):
        for copy in score_sent[chain]:
            copy.wait_recv()

    padded = pair_w.shape[0]
    pair_w_out[...] = jnp.zeros_like(pair_w_out)
    stack[...] = jnp.zeros_like(stack)
    for turn in range(turns):
        chain, first_row = turn // steps, turn % steps * step_rows
        fetch(turn).wait()
        for head in range(heads * n_tp):
            for part in range(length // LANES):
                stack[part, pl.ds(head, step_rows, stride=padded), :] = score_full[
                    head // heads, chain, head % heads, first_row : first_row + step_rows, lanes(part)
                ].astype(f32)

        def pair_row(row, total):
            at = pl.ds(pl.multiple_of(row * padded, padded), padded)
            scores = jnp.concatenate(
                [stack[part, at, :] for part in range(length // LANES)], axis=1
            ).astype(bf16)
            stacked_out[chain, first_row + row] = scores
            return total + dot(scores, pair_buf[turn % 2, row])

        pair_w_out[...] += lax.fori_loop(
            0, step_rows, pair_row, jnp.zeros(pair_w_out.shape, f32), unroll=True
        )
        if turn + 2 < turns:
            fetch(turn + 2).start()
        work(1)
    if ff_sum:
        ff_sum.finish()
    else:
        ff_out[...] = jnp.zeros_like(ff_out)
    gather.done()
    scatter.done()
    for group in score_sent:
        for copy in group:
            copy.wait_send()


def pair_kernel(stacked, pair_w, grad_pair):
    for row in range(stacked.shape[1]):
        grad_pair[0, row] = dot(stacked[0, row], pair_w[...], TN).astype(bf16)


def unpack_kernel(attn_own, ff_own, result, grad_inputs, w_in, w_out, ff_in, ff_out, result_out, inputs_out):
    parts, _, block = w_in.shape
    for part in range(parts):
        w_in[part] = attn_own[0, :, part * block : (part + 1) * block]
    w_out[...] = attn_own[0, :, parts * block : (parts + 1) * block]
    for part in range(ff_in.shape[0]):
        ff_in[part] = ff_own[part]
    ff_out[...] = ff_own[ff_in.shape[0]]
    result_out[...] = result[...]
    inputs_out[...] = grad_inputs[...]


def tail_kernel(
    sizes,
    attn_sums,
    ff_sums,
    pair_part,
    mods,
    chain_facts,
    *rest,
):
    n_tp, n_dp, all_heads, dp_sizes = sizes
    if dp_sizes:
        values, totals, facts_all, own_out, own, arrived, tp_sems, dp_sems, facts_sems, *dp_scratch = rest
        attn_sum = DpSum(dp_sizes, values, own_out, *dp_scratch)
    else:
        totals, facts_all, own, arrived, tp_sems, dp_sems, facts_sems = rest
        attn_sum = None
    chains, depth = mods.shape[1], mods.shape[3]
    channels = pair_part.shape[1]
    _, peers = tp_peers(n_tp)
    place, others = dp_others(n_dp)
    enter([peer for _, peer in peers] + others)
    facts_all[place] = chain_facts[...]
    facts_sent = share_over_dp(facts_all, place, others, facts_sems)
    if attn_sum:
        attn_sum.start()
    for chain in range(chains):
        sig_attn, sig_ff = mods[2, chain], mods[5, chain]
        entries = [
            attn_sums[0, chain],
            attn_sums[1, chain],
            ff_sums[0, chain] * (sig_attn * (1.0 - sig_attn)),
            ff_sums[1, chain],
            ff_sums[2, chain],
            ff_sums[3, chain] * (sig_ff * (1.0 - sig_ff)),
        ]
        for entry, value in enumerate(entries):
            own[entry * chains + chain : entry * chains + chain + 1, :] = value.astype(bf16)
    per_row = depth // channels
    for head in range(all_heads):
        row = 6 * chains + head // per_row
        at = head % per_row * channels
        own[row : row + 1, at : at + channels] = pair_part[head : head + 1, :].astype(bf16)
    tp_sent = [send(own, arrived.at[step], tp_sems, (step,), peer) for step, (_, peer) in enumerate(peers)]
    for copy in tp_sent:
        copy.wait_recv()
    total = own[...].astype(f32)
    for step in range(n_tp - 1):
        total = total + arrived[step].astype(f32)
    totals[place] = total.astype(bf16)
    dp_sent = share_over_dp(totals, place, others, dp_sems)
    if attn_sum:
        attn_sum.finish()
    for copy in dp_sent + facts_sent:
        copy.wait_recv()
    for copy in tp_sent + dp_sent + facts_sent:
        copy.wait_send()


VMEM_SPEC = pl.BlockSpec(memory_space=pltpu.VMEM)
ANY_SPEC = pl.BlockSpec(memory_space=pl.ANY)


def pair_sems(*shape):
    return pltpu.SemaphoreType.DMA((2,) + shape)


def params(collective_id):
    return pltpu.CompilerParams(
        collective_id=collective_id, has_side_effects=True, vmem_limit_bytes=62 * 1024 * 1024
    )


def local(
    activations,
    pair_rep,
    noise_times,
    class_ids,
    chain_lengths,
    ada_weight,
    class_table,
    pair_weight,
    attn_in,
    attn_out,
    ff_in,
    ff_out,
    cotangent,
):
    n_tp, n_dp = lax.axis_size("tp"), lax.axis_size("dp")
    chains, rows, depth = activations.shape
    length, channels = pair_rep.shape[2:]
    all_heads = pair_weight.shape[0]
    heads = all_heads // n_tp
    block = attn_in.shape[2]
    width = block // heads
    hidden_width = ff_out.shape[0]
    sds = jax.ShapeDtypeStruct

    onehot = (class_ids[:, None] == jnp.arange(class_table.shape[0])[None, :]).astype(f32)
    table_full = class_table.astype(f32)
    ada_full = ada_weight.astype(f32)
    condition = time_features(noise_times, class_table.shape[1]) + jnp.dot(
        onehot, table_full, precision=highest
    )
    modulation = jnp.dot(condition, ada_full, precision=highest)
    pieces = modulation.reshape(chains, 6, 1, depth)
    sig_attn, sig_ff = jax.nn.sigmoid(pieces[:, 2]), jax.nn.sigmoid(pieces[:, 5])
    mods = jnp.stack(
        [1.0 + pieces[:, 0], pieces[:, 1], sig_attn, 1.0 + pieces[:, 3], pieces[:, 4], sig_ff]
    )
    valid = (jnp.arange(length)[None, :] < chain_lengths[:, None]).astype(f32)[:, None, :]
    padded = -(-all_heads // 16) * 16
    pair_w = jnp.pad(pair_weight, ((0, padded - all_heads), (0, 0)))
    w_in = jnp.swapaxes(attn_in, 0, 1).reshape(depth, 4 * block)

    classes = onehot.shape[1]
    facts = jnp.concatenate([condition, onehot], axis=1)
    facts = jnp.pad(facts, ((0, 0), (0, -facts.shape[1] % LANES)))
    direct = n_dp == 8
    dp_grid = (n_dp // 2, 2)
    own_count = depth // n_dp
    step_rows = 16
    full = (chains, length, depth)
    own = (chains, rows, depth)
    rows_full, heads_kept, gate_sig, soft, mix, gated, attended, middle, grad_trans_full = pl.pallas_call(
        functools.partial(attn_fwd_kernel, (n_tp, heads, width)),
        out_shape=(
            sds(full, bf16),
            sds((chains, length, 4 * block), bf16),
            sds((chains, length, block), f32),
            sds((chains, heads, length, length), f32),
            sds((chains, length, block), f32),
            sds((chains, length, block), bf16),
            sds(own, f32),
            sds(own, f32),
            sds(full, bf16),
        ),
        in_specs=[VMEM_SPEC] * 7 + [ANY_SPEC],
        out_specs=[VMEM_SPEC] * 9,
        scratch_shapes=[
            pltpu.VMEM((2, step_rows, length, channels), bf16),
            pltpu.VMEM((length // LANES, step_rows * padded, LANES), f32),
            pltpu.VMEM((n_tp, chains, heads, rows, length), bf16),
            pltpu.VMEM((chains, heads, length, length), bf16),
            pair_sems(chains, 3),
            pair_sems(chains, 3),
            pair_sems(chains, n_tp - 1),
            pltpu.SemaphoreType.DMA((2,)),
        ]
        + scatter_scratch(chains, rows, length, depth),
        compiler_params=params(0),
        name="attn_fwd",
    )(activations, mods, valid, pair_w, w_in, attn_out, cotangent, pair_rep)

    result, grad_middle, grad_att, ff_sums, ff_weights = pl.pallas_call(
        functools.partial(ff_kernel, (n_tp, 256)),
        out_shape=(
            sds(own, bf16),
            sds(own, f32),
            sds(own, bf16),
            sds((4, chains, 1, depth), f32),
            sds((3, depth, hidden_width), bf16),
        ),
        in_specs=[VMEM_SPEC] * 7,
        out_specs=[VMEM_SPEC] * 5,
        scratch_shapes=[
            pltpu.VMEM(full, bf16),
            pltpu.VMEM((chains, length, hidden_width), f32),
            pltpu.VMEM((chains, length, hidden_width), f32),
            pltpu.VMEM((chains, length, hidden_width), bf16),
            pltpu.VMEM((2, chains, length, hidden_width), bf16),
            pair_sems(chains, 3),
        ]
        + scatter_scratch(chains, rows, length, depth) * 2,
        compiler_params=params(1),
        name="ff",
    )(middle, cotangent, attended, mods, grad_trans_full, ff_in, ff_out)

    wide = -(-5 * block // LANES) * LANES
    ff_sizes = dp_grid + (6,) if direct else None
    ff_values = ff_weights.reshape(3, n_dp, own_count, hidden_width)
    score_shape = (n_tp, chains, heads, rows, length)
    grad_inputs, attn_sums, attn_weights, _, ff_own, pair_part, stacked = pl.pallas_call(
        functools.partial(attn_bwd_kernel, (n_tp, heads, width, ff_sizes)),
        out_shape=(
            sds(own, bf16),
            sds((2, chains, 1, depth), f32),
            sds((1, depth, wide), bf16),
            sds(score_shape, bf16),
            sds((3, own_count, hidden_width), f32),
            sds((padded, channels), f32),
            sds((chains, rows, padded, length), bf16),
        ),
        in_specs=[VMEM_SPEC] * 14 + [ANY_SPEC],
        out_specs=[VMEM_SPEC] * 7,
        scratch_shapes=[
            pltpu.VMEM(full, bf16),
            pltpu.VMEM((chains, length, 4 * block), bf16),
            pltpu.VMEM(score_shape, bf16),
            pair_sems(chains, 3),
            pair_sems(chains, n_tp - 1),
        ]
        + scatter_scratch(chains, rows, length, depth)
        + [
            pltpu.VMEM((length // LANES, step_rows * padded, LANES), f32),
            pltpu.VMEM((2, step_rows, length, channels), bf16),
            pltpu.SemaphoreType.DMA((2,)),
        ]
        + (dp_sum_scratch(ff_sizes, 3, own_count, hidden_width) if direct else []),
        compiler_params=params(2),
        name="attn_bwd",
    )(
        activations,
        mods,
        grad_att,
        grad_middle,
        rows_full,
        heads_kept,
        gate_sig,
        soft,
        mix,
        gated,
        w_in,
        attn_out,
        ff_values,
        pair_w,
        pair_rep,
    )

    grad_pair = pl.pallas_call(
        pair_kernel,
        out_shape=sds(pair_rep.shape, bf16),
        grid=(chains, rows // step_rows),
        in_specs=[
            pl.BlockSpec((1, step_rows, padded, length), lambda chain, step: (chain, step, 0, 0)),
            pl.BlockSpec((padded, channels), lambda chain, step: (0, 0)),
        ],
        out_specs=pl.BlockSpec(
            (1, step_rows, length, channels), lambda chain, step: (chain, step, 0, 0)
        ),
        name="pair_grad",
    )(stacked, pair_w)

    attn_sizes = dp_grid + (6,) if direct else None
    total_rows = 6 * chains + all_heads * channels // depth
    tail_in = [attn_sums, ff_sums, pair_part, mods, facts]
    tail_out = [sds((n_dp, total_rows, depth), bf16), sds((n_dp,) + facts.shape, f32)]
    tail_scratch = [
        pltpu.VMEM((total_rows, depth), bf16),
        pltpu.VMEM((n_tp - 1, total_rows, depth), bf16),
        pair_sems(n_tp - 1),
        pair_sems(n_dp - 1),
        pair_sems(n_dp - 1),
    ]
    if direct:
        tail_in.append(attn_weights.reshape(1, n_dp, own_count, wide))
        tail_out.append(sds((1, own_count, wide), f32))
        tail_scratch += dp_sum_scratch(attn_sizes, 1, own_count, wide)
    totals, facts_all, *rest = pl.pallas_call(
        functools.partial(tail_kernel, (n_tp, n_dp, all_heads, attn_sizes)),
        out_shape=tuple(tail_out),
        in_specs=[VMEM_SPEC] * len(tail_in),
        out_specs=tuple([VMEM_SPEC] * len(tail_out)),
        scratch_shapes=tail_scratch,
        compiler_params=params(3),
        name="tail",
    )(*tail_in)

    def summed_over_chains(values):
        count, _, here = values.shape
        split = values.reshape(count, n_dp, own_count, here)
        flat_values = jnp.swapaxes(split, 0, 1).reshape(-1, here)
        own_part = lax.psum_scatter(flat_values, "dp", scatter_dimension=0, tiled=True)
        return own_part.astype(f32).reshape(count, own_count, here)

    if direct:
        attn_own = rest[0]
    else:
        ff_own, attn_own = summed_over_chains(ff_weights), summed_over_chains(attn_weights)

    place = lax.axis_index("dp")

    def own_columns(values, axis):
        width_here = values.shape[axis] // n_dp
        return lax.dynamic_slice_in_dim(values, place * width_here, width_here, axis)

    totals = totals.astype(f32)
    mod_all = totals[:, : 6 * chains].reshape(n_dp, 6, chains, depth)
    mod_all = jnp.swapaxes(mod_all, 1, 2).reshape(n_dp * chains, 6 * depth)
    pair_all = totals[:, 6 * chains :].reshape(n_dp, all_heads, channels)
    facts_rows = facts_all.reshape(n_dp * chains, -1)
    cond_wide = condition.shape[1]
    cond_all = facts_rows[:, :cond_wide]
    onehot_all = facts_rows[:, cond_wide : cond_wide + classes]
    grad_ada = jnp.dot(cond_all.T, own_columns(mod_all, 1), precision=highest)
    grad_cond = jnp.dot(mod_all, own_columns(ada_weight, 0).astype(f32).T, precision=highest)
    grad_table = jnp.dot(onehot_all.T, grad_cond, precision=highest)
    grad_pair_weight = jnp.sum(own_columns(pair_all, 2), axis=0)
    sum_in, sum_out, sum_ff_in, sum_ff_out, result, grad_inputs = pl.pallas_call(
        unpack_kernel,
        out_shape=(
            sds((4, own_count, block), f32),
            sds((own_count, block), f32),
            sds((2, own_count, hidden_width), f32),
            sds((own_count, hidden_width), f32),
            sds(own, bf16),
            sds(own, bf16),
        ),
        in_specs=[VMEM_SPEC] * 4,
        out_specs=(VMEM_SPEC,) * 6,
        name="unpack",
    )(attn_own, ff_own, result, grad_inputs)
    return (
        result,
        grad_inputs,
        grad_pair,
        sum_in,
        sum_out.T,
        sum_ff_in,
        sum_ff_out.T,
        grad_ada,
        grad_table,
        grad_pair_weight,
    )


def solution(mesh):
    return jax.shard_map(
        local,
        mesh=mesh,
        in_specs=(
            P("dp", "tp", None),
            P("dp", "tp", None, None),
            P("dp"),
            P("dp"),
            P("dp"),
            P(),
            P(),
            P(),
            P(None, None, "tp"),
            P("tp", None),
            P(None, None, "tp"),
            P("tp", None),
            P("dp", "tp", None),
        ),
        out_specs=(
            P("dp", "tp", None),
            P("dp", "tp", None),
            P("dp", "tp", None, None),
            P(None, "dp", "tp"),
            P("tp", "dp"),
            P(None, "dp", "tp"),
            P("tp", "dp"),
            P(None, "dp"),
            P(None, "dp"),
            P(None, "dp"),
        ),
        check_vma=False,
    )
```
